128 devices in a mesh: col: 16 (over z, y), row: 8 (over x, core).
Axes of the slice: x: 4, y: 4, z: 4, core: 2. Of those that a mesh axis runs over, the one named last changes fastest.
Arguments:
- inter_mask: int32 [32768, 8192], P('row', 'col')
- emb_user: bfloat16 [32768, 64], P(('row', 'col'))
- emb_item: bfloat16 [8192, 64], P(('col', 'row'))
- triples: int32 [2048, 3], replicated
Outputs:
- output 1: bfloat16 [32768, 64], P(('row', 'col'))
- output 2: bfloat16 [8192, 64], P(('col', 'row'))
- output 3: float32 [2048], replicated
All inputs are finite; a program needn't handle non-finite values.
Results may differ from the reference program's by a relative error of at most 0.0065013.
Values are sent between devices in bfloat16 or wider.
A program may use at most 1 GiB of HBM per device.

```python
import jax
import jax.numpy as jnp
from jax import lax

EMB = 64
LAYERS = 3
USERS = 32768
ITEMS = 8192
BATCH = 2048
ACT_MAX = 8
DENS_DIV = 256


def draw_mask(base_key):
    key_user, key_item, key_edge = jax.random.split(base_key, 3)
    user_act = jax.random.randint(key_user, (USERS, 1), 1, ACT_MAX + 1)
    item_pop = jax.random.randint(key_item, (1, ITEMS), 1, ACT_MAX + 1)
    edge_draw = jax.random.randint(key_edge, (USERS, ITEMS), 0, DENS_DIV)
    return (edge_draw < user_act * item_pop).astype(jnp.int32)


def draw_triples(base_key):
    key_user, key_pos, key_neg = jax.random.split(base_key, 3)
    user_ids = jax.random.randint(key_user, (BATCH,), 0, USERS)
    pos_ids = jax.random.randint(key_pos, (BATCH,), 0, ITEMS)
    neg_ids = jax.random.randint(key_neg, (BATCH,), 0, ITEMS)
    return jnp.stack([user_ids, pos_ids, neg_ids], axis=1).astype(jnp.int32)


def setup_inputs(seed: int = 0) -> dict:
    sub_keys = jax.random.split(jax.random.key(seed), 8)
    user_mean = jax.random.normal(sub_keys[1], (1, EMB), jnp.float32)
    user_noise = jax.random.normal(sub_keys[2], (USERS, EMB), jnp.float32)
    user_walk = jnp.cumsum(jax.random.normal(sub_keys[6], (USERS, EMB), jnp.float32), axis=0) * (USERS ** -0.5)
    item_mean = jax.random.normal(sub_keys[3], (1, EMB), jnp.float32)
    item_noise = jax.random.normal(sub_keys[4], (ITEMS, EMB), jnp.float32)
    item_walk = jnp.cumsum(jax.random.normal(sub_keys[7], (ITEMS, EMB), jnp.float32), axis=0) * (ITEMS ** -0.5)
    return {
        "inter_mask": draw_mask(sub_keys[0]),
        "emb_user": (0.5 * (user_mean + user_noise + user_walk)).astype(jnp.bfloat16),
        "emb_item": (0.5 * (item_mean + item_noise + item_walk)).astype(jnp.bfloat16),
        "triples": draw_triples(sub_keys[5]),
    }


def reference(inter_mask, emb_user, emb_item, triples):
    deg_user = jnp.maximum(jnp.sum(inter_mask, axis=1), 1).astype(jnp.float32)
    deg_item = jnp.maximum(jnp.sum(inter_mask, axis=0), 1).astype(jnp.float32)
    adj_norm = (inter_mask.astype(jnp.float32) * lax.rsqrt(deg_user)[:, None] * lax.rsqrt(deg_item)[None, :]).astype(jnp.bfloat16)

    def layer_step(carry, unused):
        cur_user, cur_item, total_user, total_item = carry
        next_user = jnp.dot(adj_norm, cur_item, preferred_element_type=jnp.float32).astype(jnp.bfloat16)
        next_item = jnp.dot(adj_norm.T, cur_user, preferred_element_type=jnp.float32).astype(jnp.bfloat16)
        new_carry = (next_user, next_item, total_user + next_user.astype(jnp.float32), total_item + next_item.astype(jnp.float32))
        return new_carry, None

    start_carry = (emb_user, emb_item, emb_user.astype(jnp.float32), emb_item.astype(jnp.float32))
    final_carry, unused_out = lax.scan(layer_step, start_carry, None, length=LAYERS)
    out_user = (final_carry[2] / (LAYERS + 1)).astype(jnp.bfloat16)
    out_item = (final_carry[3] / (LAYERS + 1)).astype(jnp.bfloat16)
    vec_user = out_user[triples[:, 0]].astype(jnp.float32)
    vec_pos = out_item[triples[:, 1]].astype(jnp.float32)
    vec_neg = out_item[triples[:, 2]].astype(jnp.float32)
    margin = jnp.sum(vec_user * vec_pos, axis=1) - jnp.sum(vec_user * vec_neg, axis=1)
    bpr_loss = jax.nn.softplus(-margin)
    return out_user, out_item, bpr_loss
```

```python
import functools

import jax
import jax.numpy as jnp
from jax import lax
from jax.experimental import pallas as pl
from jax.experimental.pallas import tpu as pltpu
from jax.sharding import PartitionSpec as P

LAYERS = 3
SIDE = 4
F32 = jnp.float32
BF16 = jnp.bfloat16
NN = (((1,), (0,)), ((), ()))
NT = (((1,), (1,)), ((), ()))
TN = (((0,), (0,)), ((), ()))


def mm(lhs, rhs, dims=NN):
    return lax.dot_general(lhs, rhs, dims, preferred_element_type=F32)


def identity(size):
    at_row = lax.broadcasted_iota(jnp.int32, (size, size), 0)
    at_col = lax.broadcasted_iota(jnp.int32, (size, size), 1)
    return jnp.where(at_row == at_col, 1.0, 0.0).astype(BF16)


def kernel(
    rows, mask_hbm, eu_ref, ei_ref, tri_ref, ou_ref, oi_ref, loss_ref,
    mask_buf, adj, ua, ub, pa, pb, ra, rb, sa, sb, qa, qb, utot,
    i_nat, i_pan, pi, ri, itot, du_own, du_y, du_ysum, du_z, di_own, di_got,
    picks, sc_own, sc_row, sc_rsum, sc_y, sc_ysum, sc_z, oi_nat,
    load_sem, send_sem, recv_sem,
):
    r = lax.axis_index("row")
    c = lax.axis_index("col")
    z, y = lax.div(c, SIDE), lax.rem(c, SIDE)
    half = ua.shape[-2]
    emb = 2 * half
    ublk = ua.shape[-1]
    chunks = SIDE * SIDE
    iblk = adj.shape[-1]
    isub = i_nat.shape[1]
    tiles = sc_own.shape[0]
    tw = sc_own.shape[1]

    def plus(base, k, n):
        return lax.rem(base + k, n)

    def y_dev(k):
        return {"col": z * SIDE + plus(y, k, SIDE)}

    def z_dev(k):
        return {"col": plus(z, k, SIDE) * SIDE + y}

    def r_dev(k):
        return {"row": plus(r, k, rows)}

    sides = (2, 1, 3)
    ring = tuple(range(1, rows))
    count = [0]
    sent = []

    def sems(n):
        first = count[0]
        count[0] += n
        return first

    def copy(src, dst, sem, dev):
        return pltpu.make_async_remote_copy(
            src_ref=src, dst_ref=dst, send_sem=send_sem.at[sem], recv_sem=recv_sem.at[sem],
            device_id=dev, device_id_type=pl.DeviceIdType.MESH)

    def push(sem, src, dst, dev):
        one = copy(src, dst, sem, dev)
        one.start()
        sent.append(one)

    def arrive(sem, dst, dev):
        copy(dst, dst, sem, dev).wait_recv()

    loads = [pltpu.make_async_copy(mask_hbm.at[pl.ds(j * ublk, ublk)], mask_buf.at[j], load_sem.at[j]) for j in range(chunks)]
    for one in loads:
        one.start()

    barrier = pltpu.get_barrier_semaphore()
    for k in (1, 2, 3):
        pl.semaphore_signal(barrier, inc=1, device_id=y_dev(k), device_id_type=pl.DeviceIdType.MESH)
        pl.semaphore_signal(barrier, inc=1, device_id=z_dev(k), device_id_type=pl.DeviceIdType.MESH)
    for k in ring:
        pl.semaphore_signal(barrier, inc=1, device_id=r_dev(k), device_id_type=pl.DeviceIdType.MESH)

    eye = identity(emb)
    user0 = mm(eye, eu_ref[...], NT)
    utot[...] = user0
    user0 = user0.astype(BF16)
    ua[0, y, z] = user0[:half]
    ub[0, z, y] = user0[half:]
    i_nat[r] = ei_ref[...]
    pl.semaphore_wait(barrier, 6 + len(ring))

    ug = [sems(4 * SIDE) for _ in range(LAYERS + 1)]

    def user_gather_1(l):
        for k in sides:
            push(ug[l] + k, ua.at[l, y, z], ua.at[l, y, z], z_dev(k))
            push(ug[l] + SIDE + k, ub.at[l, z, y], ub.at[l, z, y], y_dev(k))

    def user_gather_2(l):
        for k in (1, 3, 2):
            arrive(ug[l] + k, ua.at[l, y, plus(z, SIDE - k, SIDE)], z_dev(SIDE - k))
            arrive(ug[l] + SIDE + k, ub.at[l, z, plus(y, SIDE - k, SIDE)], y_dev(SIDE - k))
        for k in sides:
            push(ug[l] + 2 * SIDE + k, ua.at[l, y], ua.at[l, y], y_dev(k))
            push(ug[l] + 3 * SIDE + k, ub.at[l, z], ub.at[l, z], z_dev(k))

    def user_gather_end(l):
        for k in (1, 3, 2):
            arrive(ug[l] + 2 * SIDE + k, ua.at[l, plus(y, SIDE - k, SIDE)], y_dev(SIDE - k))
            arrive(ug[l] + 3 * SIDE + k, ub.at[l, plus(z, SIDE - k, SIDE)], z_dev(SIDE - k))

    us = [sems(4 * SIDE) for _ in range(LAYERS)]

    def user_product(l, panel):
        def step(j, carry):
            part = mm(panel, adj[j], NT)
            jz, jy = lax.div(j, SIDE), lax.rem(j, SIDE)
            pa[l, jy, jz] = part[:half]
            pb[l, jz, jy] = part[half:]
            return carry
        lax.fori_loop(0, chunks, step, 0, unroll=4)
        for k in sides:
            push(us[l] + k, pa.at[l, plus(y, k, SIDE)], ra.at[l, k - 1], y_dev(k))
            push(us[l] + SIDE + k, pb.at[l, plus(z, k, SIDE)], rb.at[l, k - 1], z_dev(k))

    def user_sum_1(l):
        for k in (1, 3, 2):
            arrive(us[l] + k, ra.at[l, k - 1], y_dev(SIDE - k))
            arrive(us[l] + SIDE + k, rb.at[l, k - 1], z_dev(SIDE - k))
        for j in range(SIDE):
            sa[l, j] = pa[l, y, j] + ra[l, 0, j] + ra[l, 1, j] + ra[l, 2, j]
            sb[l, j] = pb[l, z, j] + rb[l, 0, j] + rb[l, 1, j] + rb[l, 2, j]
        for k in sides:
            push(us[l] + 2 * SIDE + k, sa.at[l, plus(z, k, SIDE)], qa.at[l, k - 1], z_dev(k))
            push(us[l] + 3 * SIDE + k, sb.at[l, plus(y, k, SIDE)], qb.at[l, k - 1], y_dev(k))

    def user_sum_2(l):
        for k in (1, 3, 2):
            arrive(us[l] + 2 * SIDE + k, qa.at[l, k - 1], z_dev(SIDE - k))
            arrive(us[l] + 3 * SIDE + k, qb.at[l, k - 1], y_dev(SIDE - k))
        next_a = (sa[l, z] + qa[l, 0] + qa[l, 1] + qa[l, 2]).astype(BF16)
        next_b = (sb[l, y] + qb[l, 0] + qb[l, 1] + qb[l, 2]).astype(BF16)
        utot[pl.ds(0, half)] += next_a.astype(F32)
        utot[pl.ds(half, half)] += next_b.astype(F32)
        return next_a, next_b

    def user_keep(l, next_a, next_b):
        ua[l, y, z] = next_a
        ub[l, z, y] = next_b

    ig = [sems(rows) for _ in range(LAYERS + 1)]
    isum = [sems(rows) for _ in range(LAYERS)]

    def item_product(l):
        def step(j, acc):
            jz, jy = lax.div(j, SIDE), lax.rem(j, SIDE)
            lhs = jnp.concatenate([ua[l, jy, jz], ub[l, jz, jy]], axis=0)
            return acc + mm(lhs, adj[j])
        acc = lax.fori_loop(0, chunks, step, jnp.zeros((emb, iblk), F32), unroll=4)
        pi[l] = acc.reshape(pi.shape[1:])
        for k in ring:
            push(isum[l] + k, pi.at[l, plus(r, k, rows)], ri.at[l, k - 1], r_dev(k))

    def item_gather(l, mine):
        i_pan[l, r] = mine
        for k in ring:
            push(ig[l] + k, i_pan.at[l, r], i_pan.at[l, r], r_dev(k))

    def item_sum(l):
        for k in ring:
            arrive(isum[l] + k, ri.at[l, k - 1], r_dev(rows - k))
        acc = pi[l, r]
        for k in ring:
            acc = acc + ri[l, k - 1]
        mine = acc.astype(BF16).astype(F32)
        itot[...] += mine
        return mine

    def item_panel(l):
        for k in ring:
            arrive(ig[l] + k, i_pan.at[l, plus(r, rows - k, rows)], r_dev(rows - k))
        return i_pan[l].reshape(emb, iblk).astype(BF16)

    user_gather_1(0)
    for k in ring:
        push(ig[0] + k, i_nat.at[r], i_nat.at[r], r_dev(k))

    du_s, dz_s, di_s = sems(SIDE), sems(SIDE), sems(rows)
    ones = jnp.ones((8, iblk), BF16)
    di_acc = jnp.zeros((8, iblk), jnp.int32)
    for j in range(chunks):
        loads[j].wait()
        blk = mask_buf[j]
        di_acc = di_acc + jnp.sum(blk.reshape(ublk // 8, 8, iblk), axis=0)
        blk = blk.astype(F32).astype(BF16)
        adj[j] = blk
        du_own[pl.ds(j, 1), :] = mm(ones, blk, NT)[:1]
    di_own[...] = di_acc.astype(F32)
    for k in sides:
        push(du_s + k, du_own, du_y.at[k - 1], y_dev(k))
    for k in ring:
        push(di_s + k, di_own, di_got.at[k - 1], r_dev(k))
    user_gather_2(0)
    for k in ring:
        arrive(ig[0] + k, i_nat.at[plus(r, rows - k, rows)], r_dev(rows - k))
    item0 = mm(eye, i_nat[...].reshape(iblk, emb), NT)
    i_pan[0] = item0.reshape(i_pan.shape[1:])
    itot[...] = i_pan[0, r]
    item0 = item0.astype(BF16)
    for k in (1, 3, 2):
        arrive(du_s + k, du_y.at[k - 1], y_dev(SIDE - k))
    du_ysum[...] = du_own[...] + du_y[0] + du_y[1] + du_y[2]
    for k in sides:
        push(dz_s + k, du_ysum, du_z.at[k - 1], z_dev(k))
    for k in ring:
        arrive(di_s + k, di_got.at[k - 1], r_dev(rows - k))
    deg_i = di_own[...]
    for k in ring:
        deg_i = deg_i + di_got[k - 1]
    deg_i = jnp.sum(deg_i, axis=0, keepdims=True)
    scale_i = lax.rsqrt(jnp.maximum(deg_i, 1.0))
    for k in (1, 3, 2):
        arrive(dz_s + k, du_z.at[k - 1], z_dev(SIDE - k))
    deg_u = du_ysum[...] + du_z[0] + du_z[1] + du_z[2]
    scale_u = lax.rsqrt(jnp.maximum(deg_u, 1.0)).T
    for j in range(chunks):
        adj[j] = (adj[j].astype(F32) * scale_u[:, j:j + 1] * scale_i).astype(BF16)

    user_product(0, item0)
    user_gather_end(0)
    item_product(0)
    item_gather(1, item_sum(0))
    user_sum_1(0)
    user_product(1, item_panel(1))
    user_keep(1, *user_sum_2(0))
    user_gather_1(1)
    user_sum_1(1)
    user_gather_2(1)
    user_keep(2, *user_sum_2(1))
    user_gather_1(2)
    user_gather_end(1)
    item_product(1)
    user_gather_2(2)
    item_gather(2, item_sum(1))
    user_product(2, item_panel(2))
    user_gather_end(2)
    item_product(2)
    item_sum(2)
    item_gather(3, (itot[...] / (LAYERS + 1)).astype(BF16).astype(F32))
    user_sum_1(2)

    out_it = item_panel(3)
    oi_nat[...] = mm(out_it, eye, TN).reshape(oi_nat.shape)
    oi_ref[...] = oi_nat[r].astype(BF16)
    lane = ublk
    at_row = lax.broadcasted_iota(jnp.int32, (lane, tw), 0)

    def pick_items(which, t):
        local = tri_ref[which, pl.ds(t, 1), :] - c * iblk
        got = jnp.zeros((emb, tw), F32)
        for h in range(iblk // lane):
            hit = jnp.where(local - h * lane == at_row, 1.0, 0.0).astype(BF16)
            got = got + mm(out_it[:, h * lane:(h + 1) * lane], hit)
        return got

    for t in range(tiles):
        picks[0, t] = pick_items(1, t)
        picks[1, t] = pick_items(2, t)

    user_sum_2(2)
    out_ut = (utot[...] / (LAYERS + 1)).astype(BF16)
    ua[3, y, z] = out_ut[:half]
    ub[3, z, y] = out_ut[half:]
    user_gather_1(3)
    ou_ref[...] = mm(out_ut, eye, TN).astype(BF16)
    user_gather_2(3)
    user_gather_end(3)

    stack_a = ua[3].reshape(chunks * half, ublk)
    stack_b = ub[3].reshape(chunks * half, ublk)
    for t in range(tiles):
        local = tri_ref[0, pl.ds(t, 1), :] - r * (chunks * ublk)
        blk_id = lax.div(local, ublk)
        blk_id = jnp.where(local < 0, -1, blk_id)
        hit = jnp.where(local - blk_id * ublk == at_row, 1.0, 0.0).astype(BF16)
        got_a = mm(stack_a, hit)
        got_b = mm(stack_b, hit)
        vec_a = jnp.zeros((half, tw), F32)
        vec_b = jnp.zeros((half, tw), F32)
        for jz in range(SIDE):
            for jy in range(SIDE):
                here = blk_id == jz * SIDE + jy
                ja = (jy * SIDE + jz) * half
                jb = (jz * SIDE + jy) * half
                vec_a = vec_a + jnp.where(here, got_a[ja:ja + half], 0.0)
                vec_b = vec_b + jnp.where(here, got_b[jb:jb + half], 0.0)
        vec = jnp.concatenate([vec_a, vec_b], axis=0)
        pos = jnp.sum(vec * picks[0, t], axis=0, keepdims=True)
        neg = jnp.sum(vec * picks[1, t], axis=0, keepdims=True)
        sc_own[pl.ds(t, 1), :] = pos - neg

    s_r, s_y, s_z = sems(rows), sems(SIDE), sems(SIDE)
    for k in ring:
        push(s_r + k, sc_own, sc_row.at[k - 1], r_dev(k))
    for k in ring:
        arrive(s_r + k, sc_row.at[k - 1], r_dev(rows - k))
    acc = sc_own[...]
    for k in ring:
        acc = acc + sc_row[k - 1]
    sc_rsum[...] = acc
    for k in sides:
        push(s_y + k, sc_rsum, sc_y.at[k - 1], y_dev(k))
    for k in sides:
        arrive(s_y + k, sc_y.at[k - 1], y_dev(SIDE - k))
    sc_ysum[...] = sc_rsum[...] + (sc_y[0] + sc_y[1] + sc_y[2])
    for k in sides:
        push(s_z + k, sc_ysum, sc_z.at[k - 1], z_dev(k))
    for k in sides:
        arrive(s_z + k, sc_z.at[k - 1], z_dev(SIDE - k))
    neg_x = -(sc_ysum[...] + (sc_z[0] + sc_z[1] + sc_z[2]))
    loss_ref[...] = jnp.maximum(neg_x, 0.0) + jnp.log1p(jnp.exp(-jnp.abs(neg_x)))
    for one in sent:
        one.wait_send()
    assert count[0] <= send_sem.shape[0]


def solution(mesh):
    rows = mesh.shape["row"]
    cols = mesh.shape["col"]

    def device_body(mask_blk, user_shard, item_shard, triples):
        ublk, emb = user_shard.shape
        isub = item_shard.shape[0]
        iblk = mask_blk.shape[1]
        batch = triples.shape[0]
        half = emb // 2
        width = emb // rows
        tw = 256
        tiles = batch // tw
        tri = triples.T.reshape(3, tiles, tw)
        n_sem = (2 * LAYERS + 1) * 16 + rows * (2 * LAYERS + 1) + 2 * SIDE + rows + rows + 2 * SIDE
        vmem = pltpu.VMEM
        out_user, out_item, loss = pl.pallas_call(
            functools.partial(kernel, rows),
            name="lightgcn",
            out_shape=(
                jax.ShapeDtypeStruct((ublk, emb), BF16),
                jax.ShapeDtypeStruct((isub, emb), BF16),
                jax.ShapeDtypeStruct((tiles, tw), F32),
            ),
            in_specs=[pl.BlockSpec(memory_space=pl.ANY)] + [pl.BlockSpec(memory_space=vmem)] * 3,
            out_specs=tuple([pl.BlockSpec(memory_space=vmem)] * 3),
            scratch_shapes=[
                vmem((cols, ublk, iblk), jnp.int32),
                vmem((cols, ublk, iblk), BF16),
                vmem((LAYERS + 1, SIDE, SIDE, half, ublk), BF16),
                vmem((LAYERS + 1, SIDE, SIDE, half, ublk), BF16),
                vmem((LAYERS, SIDE, SIDE, half, ublk), F32),
                vmem((LAYERS, SIDE, SIDE, half, ublk), F32),
                vmem((LAYERS, 3, SIDE, half, ublk), F32),
                vmem((LAYERS, 3, SIDE, half, ublk), F32),
                vmem((LAYERS, SIDE, half, ublk), F32),
                vmem((LAYERS, SIDE, half, ublk), F32),
                vmem((LAYERS, 3, half, ublk), F32),
                vmem((LAYERS, 3, half, ublk), F32),
                vmem((emb, ublk), F32),
                vmem((rows, isub, emb), BF16),
                vmem((LAYERS + 1, rows, width, iblk), F32),
                vmem((LAYERS, rows, width, iblk), F32),
                vmem((LAYERS, rows - 1, width, iblk), F32),
                vmem((width, iblk), F32),
                vmem((cols, ublk), F32),
                vmem((3, cols, ublk), F32),
                vmem((cols, ublk), F32),
                vmem((3, cols, ublk), F32),
                vmem((8, iblk), F32),
                vmem((rows - 1, 8, iblk), F32),
                vmem((2, tiles, emb, tw), F32),
                vmem((tiles, tw), F32),
                vmem((rows - 1, tiles, tw), F32),
                vmem((tiles, tw), F32),
                vmem((3, tiles, tw), F32),
                vmem((tiles, tw), F32),
                vmem((3, tiles, tw), F32),
                vmem((rows, isub, emb), F32),
                pltpu.SemaphoreType.DMA((cols,)),
                pltpu.SemaphoreType.DMA((n_sem,)),
                pltpu.SemaphoreType.DMA((n_sem,)),
            ],
            compiler_params=pltpu.CompilerParams(collective_id=0, has_side_effects=True),
        )(mask_blk, user_shard, item_shard, tri)
        return out_user, out_item, loss.reshape(batch)

    return jax.shard_map(
        device_body,
        mesh=mesh,
        in_specs=(P("row", "col"), P(("row", "col"), None), P(("col", "row"), None), P()),
        out_specs=(P(("row", "col"), None), P(("col", "row"), None), P()),
        check_vma=False,
    )
```

```python
import functools

import jax
import jax.numpy as jnp
from jax import lax
from jax.experimental import pallas as pl
from jax.experimental.pallas import tpu as pltpu
from jax.sharding import PartitionSpec as P

LAYERS = 3
SIDE = 4
F32 = jnp.float32
BF16 = jnp.bfloat16
NN = (((1,), (0,)), ((), ()))
NT = (((1,), (1,)), ((), ()))
TN = (((0,), (0,)), ((), ()))


def mm(lhs, rhs, dims=NN):
    return lax.dot_general(lhs, rhs, dims, preferred_element_type=F32)


def identity(size):
    at_row = lax.broadcasted_iota(jnp.int32, (size, size), 0)
    at_col = lax.broadcasted_iota(jnp.int32, (size, size), 1)
    return jnp.where(at_row == at_col, 1.0, 0.0).astype(BF16)


def kernel(
    rows, mask_hbm, eu_ref, ei_ref, tri_ref, ou_ref, oi_ref, loss_ref,
    mask_buf, adj, ua, ub, pa, pb, ra, rb, sa, sb, qa, qb, utot,
    i_nat, i_pan, pi, ri, itot, du_own, du_y, du_ysum, du_z, di_own, di_got,
    picks, sc_own, sc_row, sc_sum, sc_col, oi_nat,
    load_sem, send_sem, recv_sem,
):
    r = lax.axis_index("row")
    c = lax.axis_index("col")
    z, y = lax.div(c, SIDE), lax.rem(c, SIDE)
    half = ua.shape[-2]
    emb = 2 * half
    ublk = ua.shape[-1]
    chunks = SIDE * SIDE
    iblk = adj.shape[-1]
    isub = i_nat.shape[1]
    tiles, tw = picks.shape[1], picks.shape[3]

    def plus(base, k, n):
        return lax.rem(base + k, n)

    def y_dev(k):
        return {"col": z * SIDE + plus(y, k, SIDE)}

    def z_dev(k):
        return {"col": plus(z, k, SIDE) * SIDE + y}

    def r_dev(k):
        return {"row": plus(r, k, rows)}

    def c_dev(k):
        return {"col": plus(c, k, chunks)}

    sides = (2, 1, 3)
    plane = tuple(range(1, chunks))
    ring = tuple(range(1, rows))
    count = [0]
    sent = []

    def sems(n):
        first = count[0]
        count[0] += n
        return first

    def copy(src, dst, sem, dev):
        return pltpu.make_async_remote_copy(
            src_ref=src, dst_ref=dst, send_sem=send_sem.at[sem], recv_sem=recv_sem.at[sem],
            device_id=dev, device_id_type=pl.DeviceIdType.MESH)

    def push(sem, src, dst, dev):
        one = copy(src, dst, sem, dev)
        one.start()
        sent.append(one)

    def arrive(sem, dst, dev):
        copy(dst, dst, sem, dev).wait_recv()

    loads = [pltpu.make_async_copy(mask_hbm.at[pl.ds(j * ublk, ublk)], mask_buf.at[j], load_sem.at[j]) for j in range(chunks)]
    for one in loads:
        one.start()

    barrier = pltpu.get_barrier_semaphore()
    for k in plane:
        pl.semaphore_signal(barrier, inc=1, device_id=c_dev(k), device_id_type=pl.DeviceIdType.MESH)
    for k in ring:
        pl.semaphore_signal(barrier, inc=1, device_id=r_dev(k), device_id_type=pl.DeviceIdType.MESH)

    eye = identity(emb)
    user0 = eu_ref[...]
    utot[...] = user0.astype(F32)
    ua[0, y, z] = user0[:half]
    ub[0, z, y] = user0[half:]
    i_nat[r] = ei_ref[...]
    pl.semaphore_wait(barrier, len(plane) + len(ring))

    ug = [sems(10 * SIDE) for _ in range(LAYERS + 1)]

    def user_gather_start(l):
        for k in sides:
            push(ug[l] + k, ua.at[l, y, z], ua.at[l, y, z], z_dev(k))
            push(ug[l] + 4 + k, ub.at[l, z, y], ub.at[l, z, y], y_dev(k))
        for k in sides:
            push(ug[l] + 8 + k, ua.at[l, y, z], ua.at[l, y, z], y_dev(k))
            push(ug[l] + 12 + k, ub.at[l, z, y], ub.at[l, z, y], z_dev(k))

    def user_gather_fwd(l):
        for q in (1, 3, 2):
            at_z, at_y = plus(z, SIDE - q, SIDE), plus(y, SIDE - q, SIDE)
            arrive(ug[l] + q, ua.at[l, y, at_z], z_dev(SIDE - q))
            arrive(ug[l] + 4 + q, ub.at[l, z, at_y], y_dev(SIDE - q))
            for k in sides:
                push(ug[l] + 8 + 8 * q + k, ua.at[l, y, at_z], ua.at[l, y, at_z], y_dev(k))
                push(ug[l] + 12 + 8 * q + k, ub.at[l, z, at_y], ub.at[l, z, at_y], z_dev(k))

    def user_gather_end(l):
        for q in (0, 1, 3, 2):
            for k in (1, 3, 2):
                at_z, at_y = plus(z, SIDE - q, SIDE), plus(y, SIDE - q, SIDE)
                from_z, from_y = plus(z, SIDE - k, SIDE), plus(y, SIDE - k, SIDE)
                arrive(ug[l] + 8 + 8 * q + k, ua.at[l, from_y, at_z], y_dev(SIDE - k))
                arrive(ug[l] + 12 + 8 * q + k, ub.at[l, from_z, at_y], z_dev(SIDE - k))

    us = [sems(8 * SIDE) for _ in range(LAYERS)]
    groups = ((2, 2), (1, 1), (0, 1))

    def user_product(l, panel):
        def step(j, carry):
            part = mm(panel, adj[j], NT)
            jz, jy = lax.div(j, SIDE), lax.rem(j, SIDE)
            pa[l, jy, plus(jz + SIDE, -z, SIDE)] = part[:half]
            pb[l, jz, plus(jy + SIDE, -y, SIDE)] = part[half:]
            return carry
        lax.fori_loop(0, chunks, step, 0, unroll=4)
        for g, (lo, n) in enumerate(groups):
            for k in sides:
                part = pl.ds(lo, n)
                push(us[l] + 8 * g + k, pa.at[l, plus(y, k, SIDE), part], ra.at[l, k - 1, part], y_dev(k))
                push(us[l] + 8 * g + 4 + k, pb.at[l, plus(z, k, SIDE), part], rb.at[l, k - 1, part], z_dev(k))

    def user_sum_1(l):
        for g, (lo, n) in enumerate(groups):
            part = pl.ds(lo, n)
            for k in (1, 3, 2):
                arrive(us[l] + 8 * g + k, ra.at[l, k - 1, part], y_dev(SIDE - k))
                arrive(us[l] + 8 * g + 4 + k, rb.at[l, k - 1, part], z_dev(SIDE - k))
            for j in range(lo, lo + n):
                sa[l, j] = pa[l, y, j] + ra[l, 0, j] + ra[l, 1, j] + ra[l, 2, j]
                sb[l, j] = pb[l, z, j] + rb[l, 0, j] + rb[l, 1, j] + rb[l, 2, j]
            for k in range(lo, lo + n):
                if k:
                    push(us[l] + 24 + k, sa.at[l, k], qa.at[l, k - 1], z_dev(k))
                    push(us[l] + 28 + k, sb.at[l, k], qb.at[l, k - 1], y_dev(k))

    def user_sum_2(l):
        for k in (2, 3, 1):
            arrive(us[l] + 24 + k, qa.at[l, k - 1], z_dev(SIDE - k))
            arrive(us[l] + 28 + k, qb.at[l, k - 1], y_dev(SIDE - k))
        next_a = (sa[l, 0] + qa[l, 0] + qa[l, 1] + qa[l, 2]).astype(BF16)
        next_b = (sb[l, 0] + qb[l, 0] + qb[l, 1] + qb[l, 2]).astype(BF16)
        utot[pl.ds(0, half)] += next_a.astype(F32)
        utot[pl.ds(half, half)] += next_b.astype(F32)
        return next_a, next_b

    def user_keep(l, next_a, next_b):
        ua[l, y, z] = next_a
        ub[l, z, y] = next_b

    ig = [sems(rows) for _ in range(LAYERS + 1)]
    isum = [sems(rows) for _ in range(LAYERS)]

    def item_product(l):
        def step(j, acc):
            jz, jy = lax.div(j, SIDE), lax.rem(j, SIDE)
            lhs = jnp.concatenate([ua[l, jy, jz], ub[l, jz, jy]], axis=0)
            return acc + mm(lhs, adj[j])
        acc = lax.fori_loop(0, chunks, step, jnp.zeros((emb, iblk), F32), unroll=4)
        pi[l] = acc.reshape(pi.shape[1:])
        for k in ring:
            push(isum[l] + k, pi.at[l, plus(r, k, rows)], ri.at[l, k - 1], r_dev(k))

    def item_gather(l, mine):
        i_pan[l, r] = mine
        for k in ring:
            push(ig[l] + k, i_pan.at[l, r], i_pan.at[l, r], r_dev(k))

    def item_sum(l):
        for k in ring:
            arrive(isum[l] + k, ri.at[l, k - 1], r_dev(rows - k))
        acc = pi[l, r]
        for k in ring:
            acc = acc + ri[l, k - 1]
        mine = acc.astype(BF16).astype(F32)
        itot[...] += mine
        return mine

    def item_panel(l):
        for k in ring:
            arrive(ig[l] + k, i_pan.at[l, plus(r, rows - k, rows)], r_dev(rows - k))
        return i_pan[l].reshape(emb, iblk).astype(BF16)

    user_gather_start(0)
    for k in ring:
        push(ig[0] + k, i_nat.at[r], i_nat.at[r], r_dev(k))

    du_s, dz_s, di_s = sems(SIDE), sems(SIDE), sems(rows)
    ones = jnp.ones((8, iblk), BF16)
    di_acc = jnp.zeros((8, iblk), jnp.int32)
    for j in range(chunks):
        loads[j].wait()
        blk = mask_buf[j]
        di_acc = di_acc + jnp.sum(blk.reshape(ublk // 8, 8, iblk), axis=0)
        blk = blk.astype(F32).astype(BF16)
        adj[j] = blk
        du_own[pl.ds(j, 1), :] = mm(ones, blk, NT)[:1]
    di_own[...] = di_acc.astype(F32)
    for k in sides:
        push(du_s + k, du_own, du_y.at[k - 1], y_dev(k))
    for k in ring:
        push(di_s + k, di_own, di_got.at[k - 1], r_dev(k))
    user_gather_fwd(0)
    for k in ring:
        arrive(ig[0] + k, i_nat.at[plus(r, rows - k, rows)], r_dev(rows - k))
    item0 = mm(eye, i_nat[...].reshape(iblk, emb), NT)
    i_pan[0] = item0.reshape(i_pan.shape[1:])
    itot[...] = i_pan[0, r]
    item0 = item0.astype(BF16)
    for k in (1, 3, 2):
        arrive(du_s + k, du_y.at[k - 1], y_dev(SIDE - k))
    du_ysum[...] = du_own[...] + du_y[0] + du_y[1] + du_y[2]
    for k in sides:
        push(dz_s + k, du_ysum, du_z.at[k - 1], z_dev(k))
    for k in ring:
        arrive(di_s + k, di_got.at[k - 1], r_dev(rows - k))
    deg_i = di_own[...]
    for k in ring:
        deg_i = deg_i + di_got[k - 1]
    deg_i = jnp.sum(deg_i, axis=0, keepdims=True)
    scale_i = lax.rsqrt(jnp.maximum(deg_i, 1.0))
    for k in (1, 3, 2):
        arrive(dz_s + k, du_z.at[k - 1], z_dev(SIDE - k))
    deg_u = du_ysum[...] + du_z[0] + du_z[1] + du_z[2]
    scale_u = lax.rsqrt(jnp.maximum(deg_u, 1.0)).T
    for j in range(chunks):
        adj[j] = adj[j] * (scale_u[:, j:j + 1] * scale_i).astype(BF16)

    user_product(0, item0)
    user_gather_end(0)
    item_product(0)
    item_gather(1, item_sum(0))
    user_sum_1(0)
    user_keep(1, *user_sum_2(0))
    user_gather_start(1)
    user_gather_fwd(1)
    user_product(1, item_panel(1))
    user_gather_end(1)
    item_product(1)
    item_gather(2, item_sum(1))
    user_sum_1(1)
    user_keep(2, *user_sum_2(1))
    user_gather_start(2)
    user_product(2, item_panel(2))
    user_gather_fwd(2)
    user_sum_1(2)
    user_gather_end(2)
    item_product(2)
    user_sum_2(2)
    out_ut = (utot[...] / (LAYERS + 1)).astype(BF16)
    user_keep(3, out_ut[:half], out_ut[half:])
    user_gather_start(3)
    item_sum(2)
    item_gather(3, (itot[...] / (LAYERS + 1)).astype(BF16).astype(F32))
    ou_ref[...] = out_ut
    user_gather_fwd(3)

    out_it = item_panel(3)
    oi_nat[...] = mm(out_it, eye, TN).reshape(oi_nat.shape)
    oi_ref[...] = oi_nat[r].astype(BF16)
    lane = ublk
    at_row = lax.broadcasted_iota(jnp.int32, (lane, tw), 0)

    def pick_items(which, t):
        local = tri_ref[which:which + 1, t * tw:(t + 1) * tw] - c * iblk
        got = jnp.zeros((emb, tw), F32)
        for h in range(iblk // lane):
            hit = jnp.where(local - h * lane == at_row, 1.0, 0.0).astype(BF16)
            got = got + mm(out_it[:, h * lane:(h + 1) * lane], hit)
        return got

    for t in range(tiles):
        picks[0, t] = pick_items(1, t)
        picks[1, t] = pick_items(2, t)

    user_gather_end(3)
    stack_a = ua[3].reshape(chunks * half, ublk)
    stack_b = ub[3].reshape(chunks * half, ublk)
    for t in range(tiles):
        local = tri_ref[0:1, t * tw:(t + 1) * tw] - r * (chunks * ublk)
        blk_id = lax.div(local, ublk)
        blk_id = jnp.where(local < 0, -1, blk_id)
        hit = jnp.where(local - blk_id * ublk == at_row, 1.0, 0.0).astype(BF16)
        got_a = mm(stack_a, hit)
        got_b = mm(stack_b, hit)
        vec_a = jnp.zeros((half, tw), F32)
        vec_b = jnp.zeros((half, tw), F32)
        for jz in range(SIDE):
            for jy in range(SIDE):
                here = blk_id == jz * SIDE + jy
                ja = (jy * SIDE + jz) * half
                jb = (jz * SIDE + jy) * half
                vec_a = vec_a + jnp.where(here, got_a[ja:ja + half], 0.0)
                vec_b = vec_b + jnp.where(here, got_b[jb:jb + half], 0.0)
        vec = jnp.concatenate([vec_a, vec_b], axis=0)
        pos = jnp.sum(vec * picks[0, t], axis=0, keepdims=True)
        neg = jnp.sum(vec * picks[1, t], axis=0, keepdims=True)
        for h in range(tw // 128):
            sc_own[pl.ds(t * (tw // 128) + h, 1), :] = (pos - neg)[:, h * 128:(h + 1) * 128]

    s_r, s_c = sems(rows), sems(chunks)
    for k in ring:
        push(s_r + k, sc_own, sc_row.at[k - 1], r_dev(k))
    for k in ring:
        arrive(s_r + k, sc_row.at[k - 1], r_dev(rows - k))
    acc = sc_own[...]
    for k in ring:
        acc = acc + sc_row[k - 1]
    sc_sum[...] = acc
    for k in plane:
        push(s_c + k, sc_sum, sc_col.at[k - 1], c_dev(k))
    for k in plane:
        arrive(s_c + k, sc_col.at[k - 1], c_dev(chunks - k))
    for k in plane:
        acc = acc + sc_col[k - 1]
    neg_x = -acc
    loss_ref[...] = jnp.maximum(neg_x, 0.0) + jnp.log1p(jnp.exp(-jnp.abs(neg_x)))
    for one in sent:
        one.wait_send()
    assert count[0] <= send_sem.shape[0]


def emit(ou_in, oi_in, loss_in, ou_ref, oi_ref, loss_ref):
    ou_ref[...] = ou_in[...]
    oi_ref[...] = oi_in[...]
    loss_ref[...] = loss_in[...]


def solution(mesh):
    rows = mesh.shape["row"]
    cols = mesh.shape["col"]

    def device_body(mask_blk, user_shard, item_shard, triples):
        ublk, emb = user_shard.shape
        isub = item_shard.shape[0]
        iblk = mask_blk.shape[1]
        batch = triples.shape[0]
        half = emb // 2
        width = emb // rows
        tw = 256
        tiles = batch // tw
        n_sem = 40 * (LAYERS + 1) + 32 * LAYERS + rows * (2 * LAYERS + 1) + 2 * SIDE + rows + rows + cols
        vmem = pltpu.VMEM
        out_user, out_item, loss = pl.pallas_call(
            functools.partial(kernel, rows),
            name="lightgcn",
            out_shape=(
                jax.ShapeDtypeStruct((emb, ublk), BF16),
                jax.ShapeDtypeStruct((isub, emb), BF16),
                jax.ShapeDtypeStruct((batch // 128, 128), F32),
            ),
            in_specs=[pl.BlockSpec(memory_space=pl.ANY)] + [pl.BlockSpec(memory_space=vmem)] * 3,
            out_specs=tuple([pl.BlockSpec(memory_space=vmem)] * 3),
            scratch_shapes=[
                vmem((cols, ublk, iblk), jnp.int32),
                vmem((cols, ublk, iblk), BF16),
                vmem((LAYERS + 1, SIDE, SIDE, half, ublk), BF16),
                vmem((LAYERS + 1, SIDE, SIDE, half, ublk), BF16),
                vmem((LAYERS, SIDE, SIDE, half, ublk), F32),
                vmem((LAYERS, SIDE, SIDE, half, ublk), F32),
                vmem((LAYERS, 3, SIDE, half, ublk), F32),
                vmem((LAYERS, 3, SIDE, half, ublk), F32),
                vmem((LAYERS, SIDE, half, ublk), F32),
                vmem((LAYERS, SIDE, half, ublk), F32),
                vmem((LAYERS, 3, half, ublk), F32),
                vmem((LAYERS, 3, half, ublk), F32),
                vmem((emb, ublk), F32),
                vmem((rows, isub, emb), BF16),
                vmem((LAYERS + 1, rows, width, iblk), F32),
                vmem((LAYERS, rows, width, iblk), F32),
                vmem((LAYERS, rows - 1, width, iblk), F32),
                vmem((width, iblk), F32),
                vmem((cols, ublk), F32),
                vmem((3, cols, ublk), F32),
                vmem((cols, ublk), F32),
                vmem((3, cols, ublk), F32),
                vmem((8, iblk), F32),
                vmem((rows - 1, 8, iblk), F32),
                vmem((2, tiles, emb, tw), F32),
                vmem((batch // 128, 128), F32),
                vmem((rows - 1, batch // 128, 128), F32),
                vmem((batch // 128, 128), F32),
                vmem((cols - 1, batch // 128, 128), F32),
                vmem((rows, isub, emb), F32),
                pltpu.SemaphoreType.DMA((cols,)),
                pltpu.SemaphoreType.DMA((n_sem,)),
                pltpu.SemaphoreType.DMA((n_sem,)),
            ],
            compiler_params=pltpu.CompilerParams(collective_id=0, has_side_effects=True),
        )(mask_blk, user_shard.T, item_shard, triples.T)
        out_user, out_item, loss = pl.pallas_call(
            emit,
            name="emit",
            out_shape=(
                jax.ShapeDtypeStruct((emb, ublk), BF16),
                jax.ShapeDtypeStruct((isub, emb), BF16),
                jax.ShapeDtypeStruct((batch // 128, 128), F32),
            ),
        )(out_user, out_item, loss)
        return out_user.T, out_item, loss.reshape(batch)

    return jax.shard_map(
        device_body,
        mesh=mesh,
        in_specs=(P("row", "col"), P(("row", "col"), None), P(("col", "row"), None), P()),
        out_specs=(P(("row", "col"), None), P(("col", "row"), None), P()),
        check_vma=False,
    )
```

```python
import functools
import math

import jax
import jax.numpy as jnp
from jax import lax
from jax.experimental import pallas as pl
from jax.experimental.pallas import tpu as pltpu
from jax.sharding import PartitionSpec as P

LAYERS = 3
SIDE = 4
F32 = jnp.float32
BF16 = jnp.bfloat16
NN = (((1,), (0,)), ((), ()))
NT = (((1,), (1,)), ((), ()))
TN = (((0,), (0,)), ((), ()))


def mm(lhs, rhs, dims=NN):
    return lax.dot_general(lhs, rhs, dims, preferred_element_type=F32)


def identity(size):
    at_row = lax.broadcasted_iota(jnp.int32, (size, size), 0)
    at_col = lax.broadcasted_iota(jnp.int32, (size, size), 1)
    return jnp.where(at_row == at_col, 1.0, 0.0).astype(BF16)


def kernel(
    rows, mask_hbm, eu_ref, ei_ref, tri_ref, ou_ref, oi_ref, loss_ref,
    mask_buf, adj, ua, ub, pa, pb, ra, rb, sa, sb, qa, qb, utot,
    i_nat, i_pan, pi, ri, itot, du_own, du_y, du_ysum, du_z, di_own, di_got,
    picks, sc_own, sc_row, sc_sum, sc_col, oi_nat,
    load_sem, send_sem, recv_sem,
):
    r = lax.axis_index("row")
    c = lax.axis_index("col")
    z, y = lax.div(c, SIDE), lax.rem(c, SIDE)
    half = ua.shape[-2]
    emb = 2 * half
    ublk = ua.shape[-1]
    chunks = SIDE * SIDE
    iblk = adj.shape[-1]
    isub = i_nat.shape[1]
    tiles, tw = picks.shape[1], picks.shape[3]

    def plus(base, k, n):
        return lax.rem(base + k, n)

    def y_dev(k):
        return {"col": z * SIDE + plus(y, k, SIDE)}

    def z_dev(k):
        return {"col": plus(z, k, SIDE) * SIDE + y}

    def r_dev(k):
        return {"row": plus(r, k, rows)}

    def c_dev(k):
        return {"col": plus(c, k, chunks)}

    sides = (2, 1, 3)
    plane = tuple(range(1, chunks))
    ring = tuple(range(1, rows))
    count = [0]
    sent = []

    def sems(n):
        first = count[0]
        count[0] += n
        return first

    def copy(src, dst, sem, dev, out=0):
        return pltpu.make_async_remote_copy(
            src_ref=src, dst_ref=dst, send_sem=send_sem.at[out], recv_sem=recv_sem.at[sem],
            device_id=dev, device_id_type=pl.DeviceIdType.MESH)

    def push(sem, src, dst, dev):
        copy(src, dst, sem, dev).start()
        sent.append(math.prod(src.shape) * src.dtype.itemsize)

    def arrive(sem, whole):
        copy(whole, whole, sem, {"row": r}).wait_recv()

    loads = [pltpu.make_async_copy(mask_hbm.at[pl.ds(j * ublk, ublk)], mask_buf.at[j], load_sem.at[j]) for j in range(chunks)]
    for one in loads:
        one.start()

    barrier = pltpu.get_barrier_semaphore()
    for k in plane:
        pl.semaphore_signal(barrier, inc=1, device_id=c_dev(k), device_id_type=pl.DeviceIdType.MESH)
    for k in ring:
        pl.semaphore_signal(barrier, inc=1, device_id=r_dev(k), device_id_type=pl.DeviceIdType.MESH)

    eye = identity(emb)
    user0 = eu_ref[...]
    utot[...] = user0.astype(F32)
    ua[0, y, z] = user0[:half]
    ub[0, z, y] = user0[half:]
    i_nat[r] = ei_ref[...]
    pl.semaphore_wait(barrier, len(plane) + len(ring))

    ug = [sems(10) for _ in range(LAYERS + 1)]

    def user_gather_start(l):
        for k in sides:
            push(ug[l] + k, ua.at[l, y, z], ua.at[l, y, z], z_dev(k))
            push(ug[l] + 4 + k, ub.at[l, z, y], ub.at[l, z, y], y_dev(k))
        for k in sides:
            push(ug[l] + 8, ua.at[l, y, z], ua.at[l, y, z], y_dev(k))
            push(ug[l] + 9, ub.at[l, z, y], ub.at[l, z, y], z_dev(k))

    def user_gather_fwd(l):
        for q in (1, 3, 2):
            at_z, at_y = plus(z, SIDE - q, SIDE), plus(y, SIDE - q, SIDE)
            arrive(ug[l] + q, ua.at[l, y, at_z])
            for k in sides:
                push(ug[l] + 8, ua.at[l, y, at_z], ua.at[l, y, at_z], y_dev(k))
            arrive(ug[l] + 4 + q, ub.at[l, z, at_y])
            for k in sides:
                push(ug[l] + 9, ub.at[l, z, at_y], ub.at[l, z, at_y], z_dev(k))

    def user_gather_end(l):
        arrive(ug[l] + 8, ua.at[l, pl.ds(0, SIDE - 1)])
        arrive(ug[l] + 9, ub.at[l, pl.ds(0, SIDE - 1)])

    us = [sems(8) for _ in range(LAYERS)]
    groups = ((2, 2), (1, 1), (0, 1))

    def user_product(l, panel):
        def step(j, carry):
            part = mm(panel, adj[j], NT)
            jz, jy = lax.div(j, SIDE), lax.rem(j, SIDE)
            pa[l, jy, plus(jz + SIDE, -z, SIDE)] = part[:half]
            pb[l, jz, plus(jy + SIDE, -y, SIDE)] = part[half:]
            return carry
        lax.fori_loop(0, chunks, step, 0, unroll=4)
        for g, (lo, n) in enumerate(groups):
            for k in sides:
                part = pl.ds(lo, n)
                push(us[l] + g, pa.at[l, plus(y, k, SIDE), part], ra.at[l, k - 1, part], y_dev(k))
                push(us[l] + 4 + g, pb.at[l, plus(z, k, SIDE), part], rb.at[l, k - 1, part], z_dev(k))

    def user_sum_1(l):
        for g, (lo, n) in enumerate(groups):
            part = pl.ds(lo, n)
            arrive(us[l] + g, ra.at[l, :, part])
            arrive(us[l] + 4 + g, rb.at[l, :, part])
            for j in range(lo, lo + n):
                sa[l, j] = pa[l, y, j] + ra[l, 0, j] + ra[l, 1, j] + ra[l, 2, j]
                sb[l, j] = pb[l, z, j] + rb[l, 0, j] + rb[l, 1, j] + rb[l, 2, j]
            for k in range(lo, lo + n):
                if k:
                    push(us[l] + 3, sa.at[l, k], qa.at[l, k - 1], z_dev(k))
                    push(us[l] + 7, sb.at[l, k], qb.at[l, k - 1], y_dev(k))

    def user_sum_2(l):
        arrive(us[l] + 3, qa.at[l])
        arrive(us[l] + 7, qb.at[l])
        next_a = (sa[l, 0] + qa[l, 0] + qa[l, 1] + qa[l, 2]).astype(BF16)
        next_b = (sb[l, 0] + qb[l, 0] + qb[l, 1] + qb[l, 2]).astype(BF16)
        utot[pl.ds(0, half)] += next_a.astype(F32)
        utot[pl.ds(half, half)] += next_b.astype(F32)
        return next_a, next_b

    def user_keep(l, next_a, next_b):
        ua[l, y, z] = next_a
        ub[l, z, y] = next_b

    ig = [sems(1) for _ in range(LAYERS + 1)]
    isum = [sems(1) for _ in range(LAYERS)]

    def item_product(l):
        def step(j, acc):
            jz, jy = lax.div(j, SIDE), lax.rem(j, SIDE)
            lhs = jnp.concatenate([ua[l, jy, jz], ub[l, jz, jy]], axis=0)
            return acc + mm(lhs, adj[j])
        acc = lax.fori_loop(0, chunks, step, jnp.zeros((emb, iblk), F32), unroll=4)
        pi[l] = acc.reshape(pi.shape[1:])
        for k in ring:
            push(isum[l], pi.at[l, plus(r, k, rows)], ri.at[l, k - 1], r_dev(k))

    def item_gather(l, mine):
        i_pan[l, r] = mine
        for k in ring:
            push(ig[l], i_pan.at[l, r], i_pan.at[l, r], r_dev(k))

    def item_sum(l):
        arrive(isum[l], ri.at[l])
        acc = pi[l, r]
        for k in ring:
            acc = acc + ri[l, k - 1]
        mine = acc.astype(BF16).astype(F32)
        itot[...] += mine
        return mine

    def item_panel(l):
        arrive(ig[l], i_pan.at[l, pl.ds(0, rows - 1)])
        return i_pan[l].reshape(emb, iblk).astype(BF16)

    user_gather_start(0)
    for k in ring:
        copy(i_nat.at[r], i_nat.at[r], ig[0], r_dev(k), 1).start()

    du_s, dz_s, di_s = sems(1), sems(1), sems(1)
    ones = jnp.ones((8, iblk), BF16)
    di_acc = jnp.zeros((8, iblk), jnp.int32)
    for j in range(chunks):
        loads[j].wait()
        blk = mask_buf[j]
        di_acc = di_acc + jnp.sum(blk.reshape(ublk // 8, 8, iblk), axis=0)
        blk = blk.astype(F32).astype(BF16)
        adj[j] = blk
        du_own[pl.ds(j, 1), :] = mm(ones, blk, NT)[:1]
    di_own[...] = di_acc.astype(F32)
    for k in sides:
        push(du_s, du_own, du_y.at[k - 1], y_dev(k))
    for k in ring:
        push(di_s, di_own, di_got.at[k - 1], r_dev(k))
    user_gather_fwd(0)
    arrive(ig[0], i_nat.at[pl.ds(0, rows - 1)])
    item0 = mm(eye, i_nat[...].reshape(iblk, emb), NT)
    i_pan[0] = item0.reshape(i_pan.shape[1:])
    itot[...] = i_pan[0, r]
    item0 = item0.astype(BF16)
    arrive(du_s, du_y)
    du_ysum[...] = du_own[...] + du_y[0] + du_y[1] + du_y[2]
    for k in sides:
        push(dz_s, du_ysum, du_z.at[k - 1], z_dev(k))
    arrive(di_s, di_got)
    deg_i = di_own[...]
    for k in ring:
        deg_i = deg_i + di_got[k - 1]
    deg_i = jnp.sum(deg_i, axis=0, keepdims=True)
    scale_i = lax.rsqrt(jnp.maximum(deg_i, 1.0))
    arrive(dz_s, du_z)
    deg_u = du_ysum[...] + du_z[0] + du_z[1] + du_z[2]
    scale_u = lax.rsqrt(jnp.maximum(deg_u, 1.0)).T
    for j in range(chunks):
        adj[j] = adj[j] * (scale_u[:, j:j + 1] * scale_i).astype(BF16)

    user_product(0, item0)
    user_gather_end(0)
    item_product(0)
    item_gather(1, item_sum(0))
    user_sum_1(0)
    user_keep(1, *user_sum_2(0))
    user_gather_start(1)
    user_gather_fwd(1)
    user_product(1, item_panel(1))
    user_gather_end(1)
    item_product(1)
    item_gather(2, item_sum(1))
    user_sum_1(1)
    user_keep(2, *user_sum_2(1))
    user_gather_start(2)
    user_product(2, item_panel(2))
    user_gather_fwd(2)
    user_sum_1(2)
    user_gather_end(2)
    item_product(2)
    user_sum_2(2)
    out_ut = (utot[...] / (LAYERS + 1)).astype(BF16)
    user_keep(3, out_ut[:half], out_ut[half:])
    user_gather_start(3)
    item_sum(2)
    item_gather(3, (itot[...] / (LAYERS + 1)).astype(BF16).astype(F32))
    ou_ref[...] = out_ut
    user_gather_fwd(3)

    out_it = item_panel(3)
    oi_nat[...] = mm(out_it, eye, TN).reshape(oi_nat.shape)
    oi_ref[...] = oi_nat[r].astype(BF16)
    lane = ublk
    at_row = lax.broadcasted_iota(jnp.int32, (lane, tw), 0)

    def pick_items(which, t):
        local = tri_ref[which:which + 1, t * tw:(t + 1) * tw] - c * iblk
        got = jnp.zeros((emb, tw), F32)
        for h in range(iblk // lane):
            hit = jnp.where(local - h * lane == at_row, 1.0, 0.0).astype(BF16)
            got = got + mm(out_it[:, h * lane:(h + 1) * lane], hit)
        return got

    for t in range(tiles):
        picks[0, t] = pick_items(1, t)
        picks[1, t] = pick_items(2, t)

    user_gather_end(3)
    stack_a = ua[3].reshape(chunks * half, ublk)
    stack_b = ub[3].reshape(chunks * half, ublk)
    for t in range(tiles):
        local = tri_ref[0:1, t * tw:(t + 1) * tw] - r * (chunks * ublk)
        blk_id = lax.div(local, ublk)
        blk_id = jnp.where(local < 0, -1, blk_id)
        hit = jnp.where(local - blk_id * ublk == at_row, 1.0, 0.0).astype(BF16)
        got_a = mm(stack_a, hit)
        got_b = mm(stack_b, hit)
        vec_a = jnp.zeros((half, tw), F32)
        vec_b = jnp.zeros((half, tw), F32)
        for jz in range(SIDE):
            for jy in range(SIDE):
                here = blk_id == jz * SIDE + jy
                ja = (jy * SIDE + jz) * half
                jb = (jz * SIDE + jy) * half
                vec_a = vec_a + jnp.where(here, got_a[ja:ja + half], 0.0)
                vec_b = vec_b + jnp.where(here, got_b[jb:jb + half], 0.0)
        vec = jnp.concatenate([vec_a, vec_b], axis=0)
        pos = jnp.sum(vec * picks[0, t], axis=0, keepdims=True)
        neg = jnp.sum(vec * picks[1, t], axis=0, keepdims=True)
        for h in range(tw // 128):
            sc_own[pl.ds(t * (tw // 128) + h, 1), :] = (pos - neg)[:, h * 128:(h + 1) * 128]

    s_r, s_c = sems(1), sems(1)
    for k in ring:
        push(s_r, sc_own, sc_row.at[k - 1], r_dev(k))
    arrive(s_r, sc_row)
    acc = sc_own[...]
    for k in ring:
        acc = acc + sc_row[k - 1]
    sc_sum[...] = acc
    for k in plane:
        push(s_c, sc_sum, sc_col.at[k - 1], c_dev(k))
    arrive(s_c, sc_col)
    for k in plane:
        acc = acc + sc_col[k - 1]
    neg_x = -acc
    loss_ref[...] = jnp.maximum(neg_x, 0.0) + jnp.log1p(jnp.exp(-jnp.abs(neg_x)))
    span = mask_buf.reshape(chunks * ublk, iblk)
    whole = span.at[pl.ds(0, sum(sent) // (4 * iblk))]
    copy(whole, whole, 0, {"row": r}).wait_send()
    whole = i_nat.at[pl.ds(0, rows - 1)]
    copy(whole, whole, 0, {"row": r}, 1).wait_send()
    assert count[0] == recv_sem.shape[0]
    assert sum(sent) % (32 * iblk) == 0


def emit(ou_in, oi_in, loss_in, ou_ref, oi_ref, loss_ref):
    ou_ref[...] = ou_in[...]
    oi_ref[...] = oi_in[...]
    loss_ref[...] = loss_in[...]


def solution(mesh):
    rows = mesh.shape["row"]
    cols = mesh.shape["col"]

    def device_body(mask_blk, user_shard, item_shard, triples):
        ublk, emb = user_shard.shape
        isub = item_shard.shape[0]
        iblk = mask_blk.shape[1]
        batch = triples.shape[0]
        half = emb // 2
        width = emb // rows
        tw = 256
        tiles = batch // tw
        n_sem = 10 * (LAYERS + 1) + 8 * LAYERS + 2 * LAYERS + 1 + 5
        vmem = pltpu.VMEM
        out_user, out_item, loss = pl.pallas_call(
            functools.partial(kernel, rows),
            name="lightgcn",
            out_shape=(
                jax.ShapeDtypeStruct((emb, ublk), BF16),
                jax.ShapeDtypeStruct((isub, emb), BF16),
                jax.ShapeDtypeStruct((batch // 128, 128), F32),
            ),
            in_specs=[pl.BlockSpec(memory_space=pl.ANY)] + [pl.BlockSpec(memory_space=vmem)] * 3,
            out_specs=tuple([pl.BlockSpec(memory_space=vmem)] * 3),
            scratch_shapes=[
                vmem((cols, ublk, iblk), jnp.int32),
                vmem((cols, ublk, iblk), BF16),
                vmem((LAYERS + 1, SIDE, SIDE, half, ublk), BF16),
                vmem((LAYERS + 1, SIDE, SIDE, half, ublk), BF16),
                vmem((LAYERS, SIDE, SIDE, half, ublk), F32),
                vmem((LAYERS, SIDE, SIDE, half, ublk), F32),
                vmem((LAYERS, 3, SIDE, half, ublk), F32),
                vmem((LAYERS, 3, SIDE, half, ublk), F32),
                vmem((LAYERS, SIDE, half, ublk), F32),
                vmem((LAYERS, SIDE, half, ublk), F32),
                vmem((LAYERS, 3, half, ublk), F32),
                vmem((LAYERS, 3, half, ublk), F32),
                vmem((emb, ublk), F32),
                vmem((rows, isub, emb), BF16),
                vmem((LAYERS + 1, rows, width, iblk), F32),
                vmem((LAYERS, rows, width, iblk), F32),
                vmem((LAYERS, rows - 1, width, iblk), F32),
                vmem((width, iblk), F32),
                vmem((cols, ublk), F32),
                vmem((3, cols, ublk), F32),
                vmem((cols, ublk), F32),
                vmem((3, cols, ublk), F32),
                vmem((8, iblk), F32),
                vmem((rows - 1, 8, iblk), F32),
                vmem((2, tiles, emb, tw), F32),
                vmem((batch // 128, 128), F32),
                vmem((rows - 1, batch // 128, 128), F32),
                vmem((batch // 128, 128), F32),
                vmem((cols - 1, batch // 128, 128), F32),
                vmem((rows, isub, emb), F32),
                pltpu.SemaphoreType.DMA((cols,)),
                pltpu.SemaphoreType.DMA((2,)),
                pltpu.SemaphoreType.DMA((n_sem,)),
            ],
            compiler_params=pltpu.CompilerParams(collective_id=0, has_side_effects=True),
        )(mask_blk, user_shard.T, item_shard, triples.T)
        out_user, out_item, loss = pl.pallas_call(
            emit,
            name="emit",
            out_shape=(
                jax.ShapeDtypeStruct((emb, ublk), BF16),
                jax.ShapeDtypeStruct((isub, emb), BF16),
                jax.ShapeDtypeStruct((batch // 128, 128), F32),
            ),
        )(out_user, out_item, loss)
        return out_user.T, out_item, loss.reshape(batch)

    return jax.shard_map(
        device_body,
        mesh=mesh,
        in_specs=(P("row", "col"), P(("row", "col"), None), P(("col", "row"), None), P()),
        out_specs=(P(("row", "col"), None), P(("col", "row"), None), P()),
        check_vma=False,
    )
```

```python
import functools
import math

import jax
import jax.numpy as jnp
from jax import lax
from jax.experimental import pallas as pl
from jax.experimental.pallas import tpu as pltpu
from jax.sharding import PartitionSpec as P

LAYERS = 3
SIDE = 4
F32 = jnp.float32
BF16 = jnp.bfloat16
NN = (((1,), (0,)), ((), ()))
NT = (((1,), (1,)), ((), ()))
TN = (((0,), (0,)), ((), ()))


def mm(lhs, rhs, dims=NN):
    return lax.dot_general(lhs, rhs, dims, preferred_element_type=F32)


def identity(size):
    at_row = lax.broadcasted_iota(jnp.int32, (size, size), 0)
    at_col = lax.broadcasted_iota(jnp.int32, (size, size), 1)
    return jnp.where(at_row == at_col, 1.0, 0.0).astype(BF16)


def kernel(
    rows, mask_hbm, eu_ref, ei_ref, tri_ref, ou_ref, oi_ref, loss_ref,
    mask_buf, adj, ua, ub, pa, pb, ra, rb, sa, sb, qa, qb, utot,
    i_nat, i_pan, pi, ri, itot, du_own, du_y, du_ysum, du_z, du_inv, di_own, di_got,
    picks, sc_own, sc_row, sc_sum, sc_col, oi_nat,
    load_sem, send_sem, recv_sem,
):
    r = lax.axis_index("row")
    c = lax.axis_index("col")
    z, y = lax.div(c, SIDE), lax.rem(c, SIDE)
    half = ua.shape[-2]
    emb = 2 * half
    ublk = ua.shape[-1]
    chunks = SIDE * SIDE
    iblk = adj.shape[-1]
    isub = i_nat.shape[1]
    tiles, tw = picks.shape[1], picks.shape[3]

    def plus(base, k, n):
        return lax.rem(base + k, n)

    def y_dev(k):
        return {"col": z * SIDE + plus(y, k, SIDE)}

    def z_dev(k):
        return {"col": plus(z, k, SIDE) * SIDE + y}

    def r_dev(k):
        return {"row": plus(r, k, rows)}

    def c_dev(k):
        return {"col": plus(c, k, chunks)}

    sides = (2, 1, 3)
    plane = tuple(range(1, chunks))
    ring = tuple(range(1, rows))
    count = [0]
    sent = []

    def sems(n):
        first = count[0]
        count[0] += n
        return first

    def copy(src, dst, sem, dev, out=0):
        return pltpu.make_async_remote_copy(
            src_ref=src, dst_ref=dst, send_sem=send_sem.at[out], recv_sem=recv_sem.at[sem],
            device_id=dev, device_id_type=pl.DeviceIdType.MESH)

    def push(sem, src, dst, dev):
        copy(src, dst, sem, dev).start()
        sent.append(math.prod(src.shape) * src.dtype.itemsize)

    def arrive(sem, whole):
        copy(whole, whole, sem, {"row": r}).wait_recv()

    loads = [pltpu.make_async_copy(mask_hbm.at[pl.ds(j * ublk, ublk)], mask_buf.at[j], load_sem.at[j]) for j in range(chunks)]
    for one in loads:
        one.start()

    barrier = pltpu.get_barrier_semaphore()
    for k in plane:
        pl.semaphore_signal(barrier, inc=1, device_id=c_dev(k), device_id_type=pl.DeviceIdType.MESH)
    for k in ring:
        pl.semaphore_signal(barrier, inc=1, device_id=r_dev(k), device_id_type=pl.DeviceIdType.MESH)

    eye = identity(emb)
    user0 = eu_ref[...]
    utot[...] = user0.astype(F32)
    ua[0, y, z] = user0[:half]
    ub[0, z, y] = user0[half:]
    i_nat[r] = ei_ref[...]
    ug = [sems(10) for _ in range(LAYERS + 1)]

    def user_gather_start(l):
        for k in sides:
            push(ug[l] + k, ua.at[l, y, z], ua.at[l, y, z], z_dev(k))
            push(ug[l] + 4 + k, ub.at[l, z, y], ub.at[l, z, y], y_dev(k))
        for k in sides:
            push(ug[l] + 8, ua.at[l, y, z], ua.at[l, y, z], y_dev(k))
            push(ug[l] + 9, ub.at[l, z, y], ub.at[l, z, y], z_dev(k))

    def user_gather_fwd(l):
        for q in (1, 3, 2):
            at_z, at_y = plus(z, SIDE - q, SIDE), plus(y, SIDE - q, SIDE)
            arrive(ug[l] + q, ua.at[l, y, at_z])
            for k in sides:
                push(ug[l] + 8, ua.at[l, y, at_z], ua.at[l, y, at_z], y_dev(k))
            arrive(ug[l] + 4 + q, ub.at[l, z, at_y])
            for k in sides:
                push(ug[l] + 9, ub.at[l, z, at_y], ub.at[l, z, at_y], z_dev(k))

    def user_gather_end(l):
        arrive(ug[l] + 8, ua.at[l, pl.ds(0, SIDE - 1)])
        arrive(ug[l] + 9, ub.at[l, pl.ds(0, SIDE - 1)])

    us = [sems(8) for _ in range(LAYERS)]
    groups = ((2, 2), (1, 1), (0, 1))
    order = (
        ((2, 2), (2, 3), (3, 2), (3, 3), (2, 1), (3, 1), (1, 2), (1, 3)),
        ((1, 1),),
        ((0, 1), (0, 2), (0, 3), (1, 0), (2, 0), (3, 0)),
        ((0, 0),),
    )

    def user_product(l, panel, build=None):
        for g, (lo, n) in enumerate(groups + ((0, 0),)):
            for dz, dy in order[g]:
                jz, jy = plus(z, dz, SIDE), plus(y, dy, SIDE)
                j = jz * SIDE + jy
                blk = adj[j] if build is None else build(j)
                part = mm(panel, blk, NT)
                pa[l, jy, dz] = part[:half]
                pb[l, jz, dy] = part[half:]
            if n:
                part = pl.ds(lo, n)
                for k in sides:
                    push(us[l] + g, pa.at[l, plus(y, k, SIDE), part], ra.at[l, k - 1, part], y_dev(k))
                    push(us[l] + 4 + g, pb.at[l, plus(z, k, SIDE), part], rb.at[l, k - 1, part], z_dev(k))

    def user_sum_1(l):
        for g, (lo, n) in enumerate(groups):
            part = pl.ds(lo, n)
            arrive(us[l] + g, ra.at[l, :, part])
            arrive(us[l] + 4 + g, rb.at[l, :, part])
            for j in range(lo, lo + n):
                sa[l, j] = pa[l, y, j] + ra[l, 0, j] + ra[l, 1, j] + ra[l, 2, j]
                sb[l, j] = pb[l, z, j] + rb[l, 0, j] + rb[l, 1, j] + rb[l, 2, j]
            for k in range(lo, lo + n):
                if k:
                    push(us[l] + 3, sa.at[l, k], qa.at[l, k - 1], z_dev(k))
                    push(us[l] + 7, sb.at[l, k], qb.at[l, k - 1], y_dev(k))

    def user_sum_2(l):
        arrive(us[l] + 3, qa.at[l])
        arrive(us[l] + 7, qb.at[l])
        next_a = (sa[l, 0] + qa[l, 0] + qa[l, 1] + qa[l, 2]).astype(BF16)
        next_b = (sb[l, 0] + qb[l, 0] + qb[l, 1] + qb[l, 2]).astype(BF16)
        utot[pl.ds(0, half)] += next_a.astype(F32)
        utot[pl.ds(half, half)] += next_b.astype(F32)
        return next_a, next_b

    def user_keep(l, next_a, next_b):
        ua[l, y, z] = next_a
        ub[l, z, y] = next_b

    ig = [sems(1) for _ in range(LAYERS + 1)]
    isum = [sems(1) for _ in range(LAYERS)]

    def item_product(l):
        def step(j, acc):
            jz, jy = lax.div(j, SIDE), lax.rem(j, SIDE)
            lhs = jnp.concatenate([ua[l, jy, jz], ub[l, jz, jy]], axis=0)
            return acc + mm(lhs, adj[j])
        acc = lax.fori_loop(0, chunks, step, jnp.zeros((emb, iblk), F32), unroll=4)
        pi[l] = acc.reshape(pi.shape[1:])
        for k in ring:
            push(isum[l], pi.at[l, plus(r, k, rows)], ri.at[l, k - 1], r_dev(k))

    def item_gather(l, mine):
        i_pan[l, r] = mine
        for k in ring:
            push(ig[l], i_pan.at[l, r], i_pan.at[l, r], r_dev(k))

    def item_sum(l):
        arrive(isum[l], ri.at[l])
        acc = pi[l, r]
        for k in ring:
            acc = acc + ri[l, k - 1]
        mine = acc.astype(BF16).astype(F32)
        itot[...] += mine
        return mine

    def item_panel(l):
        arrive(ig[l], i_pan.at[l, pl.ds(0, rows - 1)])
        return i_pan[l].reshape(emb, iblk).astype(BF16)

    du_s, dz_s, di_s = sems(1), sems(1), sems(1)
    ones = jnp.ones((8, iblk), BF16)
    di_acc = jnp.zeros((8, iblk), jnp.int32)
    for j in range(chunks):
        loads[j].wait()
        blk = mask_buf[j]
        di_acc = di_acc + jnp.sum(blk.reshape(ublk // 8, 8, iblk), axis=0)
        blk = blk.astype(F32).astype(BF16)
        adj[j] = blk
        du_own[pl.ds(j, 1), :] = mm(ones, blk, NT)[:1]
    di_own[...] = di_acc.astype(F32)
    pl.semaphore_wait(barrier, len(plane) + len(ring))
    for k in sides:
        push(du_s, du_own, du_y.at[k - 1], y_dev(k))
    for k in ring:
        push(di_s, di_own, di_got.at[k - 1], r_dev(k))
    user_gather_start(0)
    for k in ring:
        copy(i_nat.at[r], i_nat.at[r], ig[0], r_dev(k), 1).start()
    arrive(du_s, du_y)
    du_ysum[...] = du_own[...] + du_y[0] + du_y[1] + du_y[2]
    for k in sides:
        push(dz_s, du_ysum, du_z.at[k - 1], z_dev(k))
    arrive(ig[0], i_nat.at[pl.ds(0, rows - 1)])
    item0 = mm(eye, i_nat[...].reshape(iblk, emb), NT)
    i_pan[0] = item0.reshape(i_pan.shape[1:])
    itot[...] = i_pan[0, r]
    item0 = item0.astype(BF16)
    user_gather_fwd(0)
    arrive(di_s, di_got)
    deg_i = di_own[...]
    for k in ring:
        deg_i = deg_i + di_got[k - 1]
    deg_i = jnp.sum(deg_i, axis=0, keepdims=True)
    scale_i = lax.rsqrt(jnp.maximum(deg_i, 1.0))
    arrive(dz_s, du_z)
    deg_u = du_ysum[...] + du_z[0] + du_z[1] + du_z[2]
    du_inv[...] = lax.rsqrt(jnp.maximum(deg_u, 1.0))

    def build(j):
        scale_u = jnp.broadcast_to(du_inv[pl.ds(j, 1), :], (8, ublk)).T[:, :1]
        blk = adj[j] * (scale_u * scale_i).astype(BF16)
        adj[j] = blk
        return blk

    user_product(0, item0, build)
    user_gather_end(0)
    item_product(0)
    item_gather(1, item_sum(0))
    user_sum_1(0)
    user_keep(1, *user_sum_2(0))
    user_gather_start(1)
    user_gather_fwd(1)
    user_product(1, item_panel(1))
    user_gather_end(1)
    item_product(1)
    item_gather(2, item_sum(1))
    user_sum_1(1)
    user_keep(2, *user_sum_2(1))
    user_gather_start(2)
    user_product(2, item_panel(2))
    user_gather_fwd(2)
    user_sum_1(2)
    user_gather_end(2)
    item_product(2)
    user_sum_2(2)
    out_ut = (utot[...] / (LAYERS + 1)).astype(BF16)
    user_keep(3, out_ut[:half], out_ut[half:])
    user_gather_start(3)
    item_sum(2)
    item_gather(3, (itot[...] / (LAYERS + 1)).astype(BF16).astype(F32))
    ou_ref[...] = out_ut
    user_gather_fwd(3)

    out_it = item_panel(3)
    oi_nat[...] = mm(out_it, eye, TN).reshape(oi_nat.shape)
    oi_ref[...] = oi_nat[r].astype(BF16)
    lane = ublk
    at_row = lax.broadcasted_iota(jnp.int32, (lane, tw), 0)

    def pick_items(which, t):
        local = tri_ref[which:which + 1, t * tw:(t + 1) * tw] - c * iblk
        got = jnp.zeros((emb, tw), F32)
        for h in range(iblk // lane):
            hit = jnp.where(local - h * lane == at_row, 1.0, 0.0).astype(BF16)
            got = got + mm(out_it[:, h * lane:(h + 1) * lane], hit)
        return got

    for t in range(tiles):
        picks[0, t] = pick_items(1, t)
        picks[1, t] = pick_items(2, t)

    user_gather_end(3)
    stack_a = ua[3].reshape(chunks * half, ublk)
    stack_b = ub[3].reshape(chunks * half, ublk)
    for t in range(tiles):
        local = tri_ref[0:1, t * tw:(t + 1) * tw] - r * (chunks * ublk)
        blk_id = lax.div(local, ublk)
        blk_id = jnp.where(local < 0, -1, blk_id)
        hit = jnp.where(local - blk_id * ublk == at_row, 1.0, 0.0).astype(BF16)
        got_a = mm(stack_a, hit)
        got_b = mm(stack_b, hit)
        vec_a = jnp.zeros((half, tw), F32)
        vec_b = jnp.zeros((half, tw), F32)
        for jz in range(SIDE):
            for jy in range(SIDE):
                here = blk_id == jz * SIDE + jy
                ja = (jy * SIDE + jz) * half
                jb = (jz * SIDE + jy) * half
                vec_a = vec_a + jnp.where(here, got_a[ja:ja + half], 0.0)
                vec_b = vec_b + jnp.where(here, got_b[jb:jb + half], 0.0)
        vec = jnp.concatenate([vec_a, vec_b], axis=0)
        pos = jnp.sum(vec * picks[0, t], axis=0, keepdims=True)
        neg = jnp.sum(vec * picks[1, t], axis=0, keepdims=True)
        for h in range(tw // 128):
            sc_own[pl.ds(t * (tw // 128) + h, 1), :] = (pos - neg)[:, h * 128:(h + 1) * 128]

    s_r, s_c = sems(1), sems(1)
    for k in ring:
        push(s_r, sc_own, sc_row.at[k - 1], r_dev(k))
    arrive(s_r, sc_row)
    acc = sc_own[...]
    for k in ring:
        acc = acc + sc_row[k - 1]
    sc_sum[...] = acc
    for k in plane:
        push(s_c, sc_sum, sc_col.at[k - 1], c_dev(k))
    arrive(s_c, sc_col)
    for k in plane:
        acc = acc + sc_col[k - 1]
    neg_x = -acc
    loss_ref[...] = jnp.maximum(neg_x, 0.0) + jnp.log1p(jnp.exp(-jnp.abs(neg_x)))
    span = mask_buf.reshape(chunks * ublk, iblk)
    whole = span.at[pl.ds(0, sum(sent) // (4 * iblk))]
    copy(whole, whole, 0, {"row": r}).wait_send()
    whole = i_nat.at[pl.ds(0, rows - 1)]
    copy(whole, whole, 0, {"row": r}, 1).wait_send()
    assert count[0] == recv_sem.shape[0]
    assert sum(sent) % (32 * iblk) == 0


def emit(ou_in, oi_in, loss_in, ou_ref, oi_ref, loss_ref):
    ou_ref[...] = ou_in[...]
    oi_ref[...] = oi_in[...]
    loss_ref[...] = loss_in[...]


def solution(mesh):
    rows = mesh.shape["row"]
    cols = mesh.shape["col"]

    def device_body(mask_blk, user_shard, item_shard, triples):
        ublk, emb = user_shard.shape
        isub = item_shard.shape[0]
        iblk = mask_blk.shape[1]
        batch = triples.shape[0]
        half = emb // 2
        width = emb // rows
        tw = 256
        tiles = batch // tw
        n_sem = 10 * (LAYERS + 1) + 8 * LAYERS + 2 * LAYERS + 1 + 5
        vmem = pltpu.VMEM
        out_user, out_item, loss = pl.pallas_call(
            functools.partial(kernel, rows),
            name="lightgcn",
            out_shape=(
                jax.ShapeDtypeStruct((emb, ublk), BF16),
                jax.ShapeDtypeStruct((isub, emb), BF16),
                jax.ShapeDtypeStruct((batch // 128, 128), F32),
            ),
            in_specs=[pl.BlockSpec(memory_space=pl.ANY)] + [pl.BlockSpec(memory_space=vmem)] * 3,
            out_specs=tuple([pl.BlockSpec(memory_space=vmem)] * 3),
            scratch_shapes=[
                vmem((cols, ublk, iblk), jnp.int32),
                vmem((cols, ublk, iblk), BF16),
                vmem((LAYERS + 1, SIDE, SIDE, half, ublk), BF16),
                vmem((LAYERS + 1, SIDE, SIDE, half, ublk), BF16),
                vmem((LAYERS, SIDE, SIDE, half, ublk), F32),
                vmem((LAYERS, SIDE, SIDE, half, ublk), F32),
                vmem((LAYERS, 3, SIDE, half, ublk), F32),
                vmem((LAYERS, 3, SIDE, half, ublk), F32),
                vmem((LAYERS, SIDE, half, ublk), F32),
                vmem((LAYERS, SIDE, half, ublk), F32),
                vmem((LAYERS, 3, half, ublk), F32),
                vmem((LAYERS, 3, half, ublk), F32),
                vmem((emb, ublk), F32),
                vmem((rows, isub, emb), BF16),
                vmem((LAYERS + 1, rows, width, iblk), F32),
                vmem((LAYERS, rows, width, iblk), F32),
                vmem((LAYERS, rows - 1, width, iblk), F32),
                vmem((width, iblk), F32),
                vmem((cols, ublk), F32),
                vmem((3, cols, ublk), F32),
                vmem((cols, ublk), F32),
                vmem((3, cols, ublk), F32),
                vmem((cols, ublk), F32),
                vmem((8, iblk), F32),
                vmem((rows - 1, 8, iblk), F32),
                vmem((2, tiles, emb, tw), F32),
                vmem((batch // 128, 128), F32),
                vmem((rows - 1, batch // 128, 128), F32),
                vmem((batch // 128, 128), F32),
                vmem((cols - 1, batch // 128, 128), F32),
                vmem((rows, isub, emb), F32),
                pltpu.SemaphoreType.DMA((cols,)),
                pltpu.SemaphoreType.DMA((2,)),
                pltpu.SemaphoreType.DMA((n_sem,)),
            ],
            compiler_params=pltpu.CompilerParams(collective_id=0, has_side_effects=True),
        )(mask_blk, user_shard.T, item_shard, triples.T)
        out_user, out_item, loss = pl.pallas_call(
            emit,
            name="emit",
            out_shape=(
                jax.ShapeDtypeStruct((emb, ublk), BF16),
                jax.ShapeDtypeStruct((isub, emb), BF16),
                jax.ShapeDtypeStruct((batch // 128, 128), F32),
            ),
        )(out_user, out_item, loss)
        return out_user.T, out_item, loss.reshape(batch)

    return jax.shard_map(
        device_body,
        mesh=mesh,
        in_specs=(P("row", "col"), P(("row", "col"), None), P(("col", "row"), None), P()),
        out_specs=(P(("row", "col"), None), P(("col", "row"), None), P()),
        check_vma=False,
    )
```

```python
import functools
import math

import jax
import jax.numpy as jnp
from jax import lax
from jax.experimental import pallas as pl
from jax.experimental.pallas import tpu as pltpu
from jax.sharding import PartitionSpec as P

LAYERS = 3
SIDE = 4
USER_SPAN = 128
F32 = jnp.float32
BF16 = jnp.bfloat16
NN = (((1,), (0,)), ((), ()))
NT = (((1,), (1,)), ((), ()))
TN = (((0,), (0,)), ((), ()))


def mm(lhs, rhs, dims=NN):
    return lax.dot_general(lhs, rhs, dims, preferred_element_type=F32)


def identity(size):
    at_row = lax.broadcasted_iota(jnp.int32, (size, size), 0)
    at_col = lax.broadcasted_iota(jnp.int32, (size, size), 1)
    return jnp.where(at_row == at_col, 1.0, 0.0).astype(BF16)


def kernel(
    rows, mask_hbm, eu_ref, ei_ref, tri_ref, ou_ref, oi_ref, loss_ref,
    mask_buf, adj, ua, ub, pa, pb, ra, rb, sa, sb, qa, qb, utot,
    i_nat, i_pan, pi, ri, itot, du_own, du_y, du_ysum, du_z, du_inv, di_own, di_got,
    oi_nat, oh, apick, ihit, ppa, ppb, pra, prb, psa, psb, pqa, pqb, upick,
    vx, vxr, px, pxr, mrow, lcol,
    load_sem, send_sem, recv_sem,
):
    r = lax.axis_index("row")
    c = lax.axis_index("col")
    z, y = lax.div(c, SIDE), lax.rem(c, SIDE)
    half = ua.shape[-2]
    emb = 2 * half
    ublk = ua.shape[-1]
    chunks = SIDE * SIDE
    iblk = adj.shape[-1]
    isub = i_nat.shape[1]
    tiles, tw = apick.shape[:2]

    def plus(base, k, n):
        return lax.rem(base + k, n)

    def y_dev(k):
        return {"col": z * SIDE + plus(y, k, SIDE)}

    def z_dev(k):
        return {"col": plus(z, k, SIDE) * SIDE + y}

    def r_dev(k):
        return {"row": plus(r, k, rows)}

    def c_dev(k):
        return {"col": plus(c, k, chunks)}

    sides = (2, 1, 3)
    plane = tuple(range(1, chunks))
    ring = tuple(range(1, rows))
    count = [0]
    sent, sent_small = [], []

    def sems(n):
        first = count[0]
        count[0] += n
        return first

    def copy(src, dst, sem, dev, out=0):
        return pltpu.make_async_remote_copy(
            src_ref=src, dst_ref=dst, send_sem=send_sem.at[out], recv_sem=recv_sem.at[sem],
            device_id=dev, device_id_type=pl.DeviceIdType.MESH)

    def push(sem, src, dst, dev):
        size = math.prod(src.shape) * src.dtype.itemsize
        big = size % (32 * iblk) == 0
        copy(src, dst, sem, dev, 0 if big else 2).start()
        (sent if big else sent_small).append(size)

    def arrive(sem, whole):
        copy(whole, whole, sem, {"row": r}).wait_recv()

    loads = [pltpu.make_async_copy(mask_hbm.at[pl.ds(j * ublk, ublk)], mask_buf.at[j], load_sem.at[j]) for j in range(chunks)]
    for one in loads:
        one.start()

    barrier = pltpu.get_barrier_semaphore()
    for k in plane:
        pl.semaphore_signal(barrier, inc=1, device_id=c_dev(k), device_id_type=pl.DeviceIdType.MESH)
    for k in ring:
        pl.semaphore_signal(barrier, inc=1, device_id=r_dev(k), device_id_type=pl.DeviceIdType.MESH)

    eye = identity(emb)
    user0 = eu_ref[...]
    utot[...] = user0.astype(F32)
    ua[0, y, z] = user0[:half]
    ub[0, z, y] = user0[half:]
    i_nat[r] = ei_ref[...]
    ug = [sems(10) for _ in range(LAYERS)]

    def user_gather_start(l):
        for k in sides:
            push(ug[l] + k, ua.at[l, y, z], ua.at[l, y, z], z_dev(k))
            push(ug[l] + 4 + k, ub.at[l, z, y], ub.at[l, z, y], y_dev(k))
        for k in sides:
            push(ug[l] + 8, ua.at[l, y, z], ua.at[l, y, z], y_dev(k))
            push(ug[l] + 9, ub.at[l, z, y], ub.at[l, z, y], z_dev(k))

    def user_gather_fwd(l):
        for q in (1, 3, 2):
            at_z, at_y = plus(z, SIDE - q, SIDE), plus(y, SIDE - q, SIDE)
            arrive(ug[l] + q, ua.at[l, y, at_z])
            for k in sides:
                push(ug[l] + 8, ua.at[l, y, at_z], ua.at[l, y, at_z], y_dev(k))
            arrive(ug[l] + 4 + q, ub.at[l, z, at_y])
            for k in sides:
                push(ug[l] + 9, ub.at[l, z, at_y], ub.at[l, z, at_y], z_dev(k))

    def user_gather_end(l):
        arrive(ug[l] + 8, ua.at[l, pl.ds(0, SIDE - 1)])
        arrive(ug[l] + 9, ub.at[l, pl.ds(0, SIDE - 1)])

    us = [sems(8) for _ in range(LAYERS + 1)]
    groups = ((2, 2), (1, 1), (0, 1))
    order = (
        ((2, 2), (2, 3), (3, 2), (3, 3), (2, 1), (3, 1), (1, 2), (1, 3)),
        ((1, 1),),
        ((0, 1), (0, 2), (0, 3), (1, 0), (2, 0), (3, 0)),
        ((0, 0),),
    )

    def layer_bufs(l):
        return us[l], [ref.at[l] for ref in (pa, pb, ra, rb, sa, sb, qa, qb)]

    pick_bufs = us[LAYERS], [ppa, ppb, pra, prb, psa, psb, pqa, pqb]

    def sum_send(bufs, g):
        sem, (own_a, own_b, got_a, got_b) = bufs[0], bufs[1][:4]
        part = pl.ds(*groups[g])
        for k in sides:
            push(sem + g, own_a.at[plus(y, k, SIDE), part], got_a.at[k - 1, part], y_dev(k))
            push(sem + 4 + g, own_b.at[plus(z, k, SIDE), part], got_b.at[k - 1, part], z_dev(k))

    def sum_1(bufs):
        sem, (own_a, own_b, got_a, got_b, mid_a, mid_b, end_a, end_b) = bufs
        for g, (lo, n) in enumerate(groups):
            part = pl.ds(lo, n)
            arrive(sem + g, got_a.at[:, part])
            arrive(sem + 4 + g, got_b.at[:, part])
            for j in range(lo, lo + n):
                mid_a[j] = own_a[y, j] + got_a[0, j] + got_a[1, j] + got_a[2, j]
                mid_b[j] = own_b[z, j] + got_b[0, j] + got_b[1, j] + got_b[2, j]
            for k in range(lo, lo + n):
                if k:
                    push(sem + 3, mid_a.at[k], end_a.at[k - 1], z_dev(k))
                    push(sem + 7, mid_b.at[k], end_b.at[k - 1], y_dev(k))

    def sum_2(bufs):
        sem, (mid_a, mid_b, end_a, end_b) = bufs[0], bufs[1][4:]
        arrive(sem + 3, end_a)
        arrive(sem + 7, end_b)
        next_a = (mid_a[0] + end_a[0] + end_a[1] + end_a[2]).astype(BF16)
        next_b = (mid_b[0] + end_b[0] + end_b[1] + end_b[2]).astype(BF16)
        return next_a, next_b

    def user_product(l, panel, build=None):
        for g in range(len(order)):
            for dz, dy in order[g]:
                jz, jy = plus(z, dz, SIDE), plus(y, dy, SIDE)
                j = jz * SIDE + jy
                blk = adj[j] if build is None else build(j)
                part = mm(panel, blk, NT)
                pa[l, jy, dz] = part[:half]
                pb[l, jz, dy] = part[half:]
            if g < len(groups):
                sum_send(layer_bufs(l), g)

    def user_sum_1(l):
        sum_1(layer_bufs(l))

    def user_sum_2(l):
        next_a, next_b = sum_2(layer_bufs(l))
        utot[pl.ds(0, half)] += next_a.astype(F32)
        utot[pl.ds(half, half)] += next_b.astype(F32)
        return next_a, next_b

    def user_keep(l, next_a, next_b):
        ua[l, y, z] = next_a
        ub[l, z, y] = next_b

    ig = [sems(1) for _ in range(LAYERS + 1)]
    isum = [sems(1) for _ in range(LAYERS)]

    def item_product(l):
        def step(j, acc):
            jz, jy = lax.div(j, SIDE), lax.rem(j, SIDE)
            lhs = jnp.concatenate([ua[l, jy, jz], ub[l, jz, jy]], axis=0)
            return acc + mm(lhs, adj[j])
        acc = lax.fori_loop(0, chunks, step, jnp.zeros((emb, iblk), F32), unroll=4)
        pi[l] = acc.reshape(pi.shape[1:])
        for k in ring:
            push(isum[l], pi.at[l, plus(r, k, rows)], ri.at[l, k - 1], r_dev(k))

    def item_gather(l, mine):
        i_pan[l, r] = mine
        for k in ring:
            push(ig[l], i_pan.at[l, r], i_pan.at[l, r], r_dev(k))

    def item_sum(l):
        arrive(isum[l], ri.at[l])
        acc = pi[l, r]
        for k in ring:
            acc = acc + ri[l, k - 1]
        mine = acc.astype(BF16).astype(F32)
        itot[...] += mine
        return mine

    def item_panel(l):
        arrive(ig[l], i_pan.at[l, pl.ds(0, rows - 1)])
        return i_pan[l].reshape(emb, iblk).astype(BF16)

    def pick_rows(t):
        ids = (tri_ref[0:1, t * tw:(t + 1) * tw] - r * (chunks * ublk)).astype(F32)
        ids = jnp.broadcast_to(ids, (8, tw)).T[:, :1]
        lane = lax.broadcasted_iota(jnp.int32, (tw, ublk), 1).astype(F32)
        for j in range(chunks):
            oh[:, j * ublk:(j + 1) * ublk] = jnp.where(ids - j * ublk == lane, 1.0, 0.0).astype(BF16)
        rows_got = mm(oh[...], adj[...].reshape(chunks * ublk, iblk))
        apick[t] = rows_got.astype(BF16)

    def pick_product(panel):
        for t in range(tiles):
            part = mm(panel, apick[t], NT)
            for h in range(tw // 128):
                jz, jy = divmod(t * (tw // 128) + h, SIDE)
                cut = part[:, h * 128:(h + 1) * 128]
                ppa[jy, plus(jz + SIDE, -z, SIDE)] = cut[:half]
                ppb[jz, plus(jy + SIDE, -y, SIDE)] = cut[half:]
        for g in range(len(groups)):
            sum_send(pick_bufs, g)

    def pick_users(l):
        local = tri_ref[0:1, pl.ds(pl.multiple_of(c * 128, 128), 128)] - r * (chunks * ublk)
        blk_id = jnp.where(local < 0, -1, lax.div(local, ublk))
        at_row = lax.broadcasted_iota(jnp.int32, (ublk, 128), 0)
        hit = jnp.where(local - blk_id * ublk == at_row, 1.0, 0.0).astype(BF16)
        got_a = mm(ua[l].reshape(chunks * half, ublk), hit)
        got_b = mm(ub[l].reshape(chunks * half, ublk), hit)
        vec_a = jnp.zeros((half, 128), F32)
        vec_b = jnp.zeros((half, 128), F32)
        for jz in range(SIDE):
            for jy in range(SIDE):
                here = blk_id == jz * SIDE + jy
                ja = (jy * SIDE + jz) * half
                jb = (jz * SIDE + jy) * half
                vec_a = vec_a + jnp.where(here, got_a[ja:ja + half], 0.0)
                vec_b = vec_b + jnp.where(here, got_b[jb:jb + half], 0.0)
        if l:
            vec_a = upick[pl.ds(0, half)] + vec_a
            vec_b = upick[pl.ds(half, half)] + vec_b
        upick[pl.ds(0, half)] = vec_a
        upick[pl.ds(half, half)] = vec_b

    def item_hits():
        at_row = lax.broadcasted_iota(jnp.int32, (ublk, tw), 0)
        for which in (1, 2):
            for t in range(tiles):
                local = tri_ref[which:which + 1, t * tw:(t + 1) * tw] - c * iblk
                hit = lax.rem(local + USER_SPAN * ublk, ublk) == at_row
                ihit[which - 1, t] = jnp.where(hit, 1.0, 0.0).astype(BF16)

    def pick_items(mine):
        lhs = jnp.concatenate([mine[:, h * ublk:(h + 1) * ublk] for h in range(iblk // ublk)], axis=0).astype(BF16)
        width = mine.shape[0]
        for which in (1, 2):
            for t in range(tiles):
                local = tri_ref[which:which + 1, t * tw:(t + 1) * tw] - c * iblk
                got = mm(lhs, ihit[which - 1, t])
                vec = jnp.zeros((width, tw), F32)
                for h in range(iblk // ublk):
                    here = (local >= h * ublk) & (local < (h + 1) * ublk)
                    vec = vec + jnp.where(here, got[h * width:(h + 1) * width], 0.0)
                for h in range(tw // 128):
                    px[t * (tw // 128) + h, which - 1] = vec[:, h * 128:(h + 1) * 128]

    du_s, dz_s, di_s = sems(1), sems(1), sems(1)
    ones = jnp.ones((8, iblk), BF16)
    di_acc = jnp.zeros((8, iblk), jnp.int32)
    for j in range(chunks):
        loads[j].wait()
        blk = mask_buf[j]
        di_acc = di_acc + jnp.sum(blk.reshape(ublk // 8, 8, iblk), axis=0)
        blk = blk.astype(F32).astype(BF16)
        adj[j] = blk
        du_own[pl.ds(j, 1), :] = mm(ones, blk, NT)[:1]
    di_own[...] = di_acc.astype(F32)
    pl.semaphore_wait(barrier, len(plane) + len(ring))
    for k in sides:
        push(du_s, du_own, du_y.at[k - 1], y_dev(k))
    for k in ring:
        push(di_s, di_own, di_got.at[k - 1], r_dev(k))
    user_gather_start(0)
    for k in ring:
        copy(i_nat.at[r], i_nat.at[r], ig[0], r_dev(k), 1).start()
    arrive(du_s, du_y)
    du_ysum[...] = du_own[...] + du_y[0] + du_y[1] + du_y[2]
    for k in sides:
        push(dz_s, du_ysum, du_z.at[k - 1], z_dev(k))
    arrive(ig[0], i_nat.at[pl.ds(0, rows - 1)])
    item0 = mm(eye, i_nat[...].reshape(iblk, emb), NT)
    i_pan[0] = item0.reshape(i_pan.shape[1:])
    itot[...] = i_pan[0, r]
    item0 = item0.astype(BF16)
    user_gather_fwd(0)
    arrive(di_s, di_got)
    deg_i = di_own[...]
    for k in ring:
        deg_i = deg_i + di_got[k - 1]
    deg_i = jnp.sum(deg_i, axis=0, keepdims=True)
    scale_i = lax.rsqrt(jnp.maximum(deg_i, 1.0))
    arrive(dz_s, du_z)
    deg_u = du_ysum[...] + du_z[0] + du_z[1] + du_z[2]
    du_inv[...] = lax.rsqrt(jnp.maximum(deg_u, 1.0))

    def build(j):
        scale_u = jnp.broadcast_to(du_inv[pl.ds(j, 1), :], (8, ublk)).T[:, :1]
        blk = adj[j] * (scale_u * scale_i).astype(BF16)
        adj[j] = blk
        return blk

    s_u, s_i, s_m, s_l = sems(1), sems(1), sems(1), sems(1)
    user_product(0, item0, build)
    user_gather_end(0)
    item_product(0)
    pick_rows(0)
    pick_rows(1)
    pick_rows(2)
    item_gather(1, item_sum(0))
    user_sum_1(0)
    user_keep(1, *user_sum_2(0))
    user_gather_start(1)
    pick_rows(3)
    pick_rows(4)
    user_gather_fwd(1)
    user_product(1, item_panel(1))
    pick_rows(5)
    pick_rows(6)
    pick_rows(7)
    user_gather_end(1)
    item_product(1)
    item_hits()
    pick_users(0)
    pick_users(1)
    item_gather(2, item_sum(1))
    user_sum_1(1)
    user_keep(2, *user_sum_2(1))
    user_gather_start(2)
    panel2 = item_panel(2)
    pick_product(panel2)
    user_gather_fwd(2)
    sum_1(pick_bufs)
    user_product(2, panel2)
    user_gather_end(2)
    item_product(2)
    pick_users(2)

    vec_a, vec_b = sum_2(pick_bufs)
    vec_a = ((upick[pl.ds(0, half)] + vec_a.astype(F32)) / (LAYERS + 1)).astype(BF16).astype(F32)
    vec_b = ((upick[pl.ds(half, half)] + vec_b.astype(F32)) / (LAYERS + 1)).astype(BF16).astype(F32)
    vx[...] = jnp.concatenate([vec_a, vec_b], axis=0).reshape(vx.shape)
    for k in ring:
        push(s_u, vx.at[plus(r, k, rows)], vxr.at[k - 1], r_dev(k))

    item_sum(2)
    out_slice = (itot[...] / (LAYERS + 1)).astype(BF16).astype(F32)
    pick_items(out_slice)
    for k in plane:
        push(s_i, px.at[plus(c, k, chunks)], pxr.at[k - 1], c_dev(k))
    item_gather(3, out_slice)
    arrive(s_u, vxr)
    vec_u = vx[r]
    for k in ring:
        vec_u = vec_u + vxr[k - 1]
    user_sum_1(2)
    arrive(s_i, pxr)
    vec_p, vec_n = px[c, 0], px[c, 1]
    for k in plane:
        vec_p = vec_p + pxr[k - 1, 0]
        vec_n = vec_n + pxr[k - 1, 1]
    part = jnp.sum(vec_u * vec_p, axis=0, keepdims=True) - jnp.sum(vec_u * vec_n, axis=0, keepdims=True)
    mrow[r] = jnp.broadcast_to(part, mrow.shape[1:])
    for k in ring:
        push(s_m, mrow.at[r], mrow.at[r], r_dev(k))
    user_sum_2(2)
    ou_ref[...] = (utot[...] / (LAYERS + 1)).astype(BF16)
    arrive(s_m, mrow.at[pl.ds(0, rows - 1)])
    acc = mrow[0]
    for k in range(1, rows):
        acc = acc + mrow[k]
    neg_x = -acc
    lcol[c] = jnp.maximum(neg_x, 0.0) + jnp.log1p(jnp.exp(-jnp.abs(neg_x)))
    for k in plane:
        push(s_l, lcol.at[c], lcol.at[c], c_dev(k))
    out_it = item_panel(3)
    oi_nat[...] = mm(out_it, eye, TN).reshape(oi_nat.shape)
    oi_ref[...] = oi_nat[r].astype(BF16)
    arrive(s_l, lcol.at[pl.ds(0, chunks - 1)])
    loss_ref[...] = lcol[:, 0]

    span = mask_buf.reshape(chunks * ublk, iblk)
    whole = span.at[pl.ds(0, sum(sent) // (4 * iblk))]
    copy(whole, whole, 0, {"row": r}).wait_send()
    whole = span.at[pl.ds(0, sum(sent_small) // 512), pl.ds(0, 128)]
    copy(whole, whole, 0, {"row": r}, 2).wait_send()
    whole = i_nat.at[pl.ds(0, rows - 1)]
    copy(whole, whole, 0, {"row": r}, 1).wait_send()
    assert count[0] == recv_sem.shape[0]
    assert sum(sent_small) % 4096 == 0


def emit(ou_in, oi_in, loss_in, ou_ref, oi_ref, loss_ref):
    ou_ref[...] = ou_in[...]
    oi_ref[...] = oi_in[...]
    loss_ref[...] = loss_in[...]


def solution(mesh):
    rows = mesh.shape["row"]
    cols = mesh.shape["col"]

    def device_body(mask_blk, user_shard, item_shard, triples):
        ublk, emb = user_shard.shape
        isub = item_shard.shape[0]
        iblk = mask_blk.shape[1]
        batch = triples.shape[0]
        half = emb // 2
        width = emb // rows
        tw = 256
        tiles = batch // tw
        n_sem = 10 * LAYERS + 8 * (LAYERS + 1) + 2 * LAYERS + 1 + 3 + 4
        vmem = pltpu.VMEM
        out_user, out_item, loss = pl.pallas_call(
            functools.partial(kernel, rows),
            name="lightgcn",
            out_shape=(
                jax.ShapeDtypeStruct((emb, ublk), BF16),
                jax.ShapeDtypeStruct((isub, emb), BF16),
                jax.ShapeDtypeStruct((batch // 128, 128), F32),
            ),
            in_specs=[pl.BlockSpec(memory_space=pl.ANY)] + [pl.BlockSpec(memory_space=vmem)] * 3,
            out_specs=tuple([pl.BlockSpec(memory_space=vmem)] * 3),
            scratch_shapes=[
                vmem((cols, ublk, iblk), jnp.int32),
                vmem((cols, ublk, iblk), BF16),
                vmem((LAYERS, SIDE, SIDE, half, ublk), BF16),
                vmem((LAYERS, SIDE, SIDE, half, ublk), BF16),
                vmem((LAYERS, SIDE, SIDE, half, ublk), F32),
                vmem((LAYERS, SIDE, SIDE, half, ublk), F32),
                vmem((LAYERS, 3, SIDE, half, ublk), F32),
                vmem((LAYERS, 3, SIDE, half, ublk), F32),
                vmem((LAYERS, SIDE, half, ublk), F32),
                vmem((LAYERS, SIDE, half, ublk), F32),
                vmem((LAYERS, 3, half, ublk), F32),
                vmem((LAYERS, 3, half, ublk), F32),
                vmem((emb, ublk), F32),
                vmem((rows, isub, emb), BF16),
                vmem((LAYERS + 1, rows, width, iblk), F32),
                vmem((LAYERS, rows, width, iblk), F32),
                vmem((LAYERS, rows - 1, width, iblk), F32),
                vmem((width, iblk), F32),
                vmem((cols, ublk), F32),
                vmem((3, cols, ublk), F32),
                vmem((cols, ublk), F32),
                vmem((3, cols, ublk), F32),
                vmem((cols, ublk), F32),
                vmem((8, iblk), F32),
                vmem((rows - 1, 8, iblk), F32),
                vmem((rows, isub, emb), F32),
                vmem((tw, cols * ublk), BF16),
                vmem((tiles, tw, iblk), BF16),
                vmem((2, tiles, ublk, tw), BF16),
                vmem((SIDE, SIDE, half, 128), F32),
                vmem((SIDE, SIDE, half, 128), F32),
                vmem((3, SIDE, half, 128), F32),
                vmem((3, SIDE, half, 128), F32),
                vmem((SIDE, half, 128), F32),
                vmem((SIDE, half, 128), F32),
                vmem((3, half, 128), F32),
                vmem((3, half, 128), F32),
                vmem((emb, 128), F32),
                vmem((rows, width, 128), F32),
                vmem((rows - 1, width, 128), F32),
                vmem((cols, 2, width, 128), F32),
                vmem((cols - 1, 2, width, 128), F32),
                vmem((rows, 8, 128), F32),
                vmem((cols, 8, 128), F32),
                pltpu.SemaphoreType.DMA((cols,)),
                pltpu.SemaphoreType.DMA((3,)),
                pltpu.SemaphoreType.DMA((n_sem,)),
            ],
            compiler_params=pltpu.CompilerParams(collective_id=0, has_side_effects=True),
        )(mask_blk, user_shard.T, item_shard, triples.T)
        out_user, out_item, loss = pl.pallas_call(
            emit,
            name="emit",
            out_shape=(
                jax.ShapeDtypeStruct((emb, ublk), BF16),
                jax.ShapeDtypeStruct((isub, emb), BF16),
                jax.ShapeDtypeStruct((batch // 128, 128), F32),
            ),
        )(out_user, out_item, loss)
        return out_user.T, out_item, loss.reshape(batch)

    return jax.shard_map(
        device_body,
        mesh=mesh,
        in_specs=(P("row", "col"), P(("row", "col"), None), P(("col", "row"), None), P()),
        out_specs=(P(("row", "col"), None), P(("col", "row"), None), P()),
        check_vma=False,
    )
```

```python
import functools
import math

import jax
import jax.numpy as jnp
from jax import lax
from jax.experimental import pallas as pl
from jax.experimental.pallas import tpu as pltpu
from jax.sharding import PartitionSpec as P

LAYERS = 3
SIDE = 4
USER_SPAN = 128
F32 = jnp.float32
BF16 = jnp.bfloat16
NN = (((1,), (0,)), ((), ()))
NT = (((1,), (1,)), ((), ()))
TN = (((0,), (0,)), ((), ()))


def mm(lhs, rhs, dims=NN):
    return lax.dot_general(lhs, rhs, dims, preferred_element_type=F32)


def identity(size):
    at_row = lax.broadcasted_iota(jnp.int32, (size, size), 0)
    at_col = lax.broadcasted_iota(jnp.int32, (size, size), 1)
    return jnp.where(at_row == at_col, 1.0, 0.0).astype(BF16)


def kernel(
    rows, mask_hbm, eu_ref, ei_ref, tri_ref, ou_ref, oi_ref, loss_ref,
    mask_buf, adj, ua, ub, pa, pb, ra, rb, sa, sb, qa, qb, utot,
    i_nat, i_pan, pi, ri, itot, du_own, du_y, du_ysum, du_z, du_inv, di_own, di_got,
    oi_nat, oh, apick, ihit, ppa, ppb, pra, prb, psa, psb, pqa, pqb, upick,
    vx, vxr, px, pxr, tiny,
    load_sem, send_sem, recv_sem,
):
    r = lax.axis_index("row")
    c = lax.axis_index("col")
    z, y = lax.div(c, SIDE), lax.rem(c, SIDE)
    half = ua.shape[-2]
    emb = 2 * half
    ublk = ua.shape[-1]
    chunks = SIDE * SIDE
    iblk = adj.shape[-1]
    isub = i_nat.shape[1]
    tiles, tw = apick.shape[:2]

    def plus(base, k, n):
        return lax.rem(base + k, n)

    def y_dev(k):
        return {"col": z * SIDE + plus(y, k, SIDE)}

    def z_dev(k):
        return {"col": plus(z, k, SIDE) * SIDE + y}

    def r_dev(k):
        return {"row": plus(r, k, rows)}

    def c_dev(k):
        return {"col": plus(c, k, chunks)}

    sides = (2, 1, 3)
    plane = tuple(range(1, chunks))
    ring = tuple(range(1, rows))
    count = [0]
    sent = [], [], []

    def sems(n):
        first = count[0]
        count[0] += n
        return first

    def copy(src, dst, sem, dev, out=0):
        return pltpu.make_async_remote_copy(
            src_ref=src, dst_ref=dst, send_sem=send_sem.at[out], recv_sem=recv_sem.at[sem],
            device_id=dev, device_id_type=pl.DeviceIdType.MESH)

    def push(sem, src, dst, dev):
        size = math.prod(src.shape) * src.dtype.itemsize
        kind = 0 if size % (32 * iblk) == 0 else 1 if size % 4096 == 0 else 2
        copy(src, dst, sem, dev, kind).start()
        sent[kind].append(size)

    def arrive(sem, whole):
        copy(whole, whole, sem, {"row": r}).wait_recv()

    loads = [pltpu.make_async_copy(mask_hbm.at[pl.ds(j * ublk, ublk)], mask_buf.at[j], load_sem.at[j]) for j in range(chunks)]
    for one in loads:
        one.start()

    barrier = pltpu.get_barrier_semaphore()
    for k in plane:
        pl.semaphore_signal(barrier, inc=1, device_id=c_dev(k), device_id_type=pl.DeviceIdType.MESH)
    for k in ring:
        pl.semaphore_signal(barrier, inc=1, device_id=r_dev(k), device_id_type=pl.DeviceIdType.MESH)

    eye = identity(emb)
    user0 = eu_ref[...]
    utot[...] = user0.astype(F32)
    ua[0, y, z] = user0[:half]
    ub[0, z, y] = user0[half:]
    i_nat[r] = ei_ref[...]
    ug = [sems(10) for _ in range(LAYERS)]

    def user_gather_start(l):
        for k in sides:
            push(ug[l] + k, ua.at[l, y, z], ua.at[l, y, z], z_dev(k))
            push(ug[l] + 4 + k, ub.at[l, z, y], ub.at[l, z, y], y_dev(k))
        for k in sides:
            push(ug[l] + 8, ua.at[l, y, z], ua.at[l, y, z], y_dev(k))
            push(ug[l] + 9, ub.at[l, z, y], ub.at[l, z, y], z_dev(k))

    def user_gather_fwd(l):
        for q in (1, 3, 2):
            at_z, at_y = plus(z, SIDE - q, SIDE), plus(y, SIDE - q, SIDE)
            arrive(ug[l] + q, ua.at[l, y, at_z])
            for k in sides:
                push(ug[l] + 8, ua.at[l, y, at_z], ua.at[l, y, at_z], y_dev(k))
            arrive(ug[l] + 4 + q, ub.at[l, z, at_y])
            for k in sides:
                push(ug[l] + 9, ub.at[l, z, at_y], ub.at[l, z, at_y], z_dev(k))

    def user_gather_end(l):
        arrive(ug[l] + 8, ua.at[l, pl.ds(0, SIDE - 1)])
        arrive(ug[l] + 9, ub.at[l, pl.ds(0, SIDE - 1)])

    us = [sems(8) for _ in range(LAYERS + 1)]
    groups = ((2, 2), (1, 1), (0, 1))
    order = (
        ((2, 2), (2, 3), (3, 2), (3, 3), (2, 1), (3, 1), (1, 2), (1, 3)),
        ((1, 1),),
        ((0, 1), (0, 2), (0, 3), (1, 0), (2, 0), (3, 0)),
        ((0, 0),),
    )

    def layer_bufs(l):
        return us[l], [ref.at[l] for ref in (pa, pb, ra, rb, sa, sb, qa, qb)]

    pick_bufs = us[LAYERS], [ppa, ppb, pra, prb, psa, psb, pqa, pqb]

    def sum_send(bufs, g):
        sem, (own_a, own_b, got_a, got_b) = bufs[0], bufs[1][:4]
        part = pl.ds(*groups[g])
        for k in sides:
            push(sem + g, own_a.at[plus(y, k, SIDE), part], got_a.at[k - 1, part], y_dev(k))
            push(sem + 4 + g, own_b.at[plus(z, k, SIDE), part], got_b.at[k - 1, part], z_dev(k))

    def sum_1(bufs):
        sem, (own_a, own_b, got_a, got_b, mid_a, mid_b, end_a, end_b) = bufs
        for g, (lo, n) in enumerate(groups):
            part = pl.ds(lo, n)
            arrive(sem + g, got_a.at[:, part])
            arrive(sem + 4 + g, got_b.at[:, part])
            for j in range(lo, lo + n):
                mid_a[j] = own_a[y, j] + got_a[0, j] + got_a[1, j] + got_a[2, j]
                mid_b[j] = own_b[z, j] + got_b[0, j] + got_b[1, j] + got_b[2, j]
            for k in range(lo, lo + n):
                if k:
                    push(sem + 3, mid_a.at[k], end_a.at[k - 1], z_dev(k))
                    push(sem + 7, mid_b.at[k], end_b.at[k - 1], y_dev(k))

    def sum_2(bufs):
        sem, (mid_a, mid_b, end_a, end_b) = bufs[0], bufs[1][4:]
        arrive(sem + 3, end_a)
        arrive(sem + 7, end_b)
        next_a = (mid_a[0] + end_a[0] + end_a[1] + end_a[2]).astype(BF16)
        next_b = (mid_b[0] + end_b[0] + end_b[1] + end_b[2]).astype(BF16)
        return next_a, next_b

    def user_product(l, panel, g, build=None):
        for dz, dy in order[g]:
            jz, jy = plus(z, dz, SIDE), plus(y, dy, SIDE)
            j = jz * SIDE + jy
            blk = adj[j] if build is None else build(j)
            part = mm(panel, blk, NT)
            pa[l, jy, dz] = part[:half]
            pb[l, jz, dy] = part[half:]

    def user_sum_send(l, g):
        sum_send(layer_bufs(l), g)

    def user_sum_1(l):
        sum_1(layer_bufs(l))

    def user_sum_2(l):
        next_a, next_b = sum_2(layer_bufs(l))
        utot[pl.ds(0, half)] += next_a.astype(F32)
        utot[pl.ds(half, half)] += next_b.astype(F32)
        return next_a, next_b

    def user_keep(l, next_a, next_b):
        ua[l, y, z] = next_a
        ub[l, z, y] = next_b

    ig = [sems(1) for _ in range(LAYERS + 1)]
    isum = [sems(1) for _ in range(LAYERS)]

    def item_product(l):
        def step(j, acc):
            jz, jy = lax.div(j, SIDE), lax.rem(j, SIDE)
            lhs = jnp.concatenate([ua[l, jy, jz], ub[l, jz, jy]], axis=0)
            return acc + mm(lhs, adj[j])
        acc = lax.fori_loop(0, chunks, step, jnp.zeros((emb, iblk), F32), unroll=4)
        pi[l] = acc.reshape(pi.shape[1:])
        for k in ring:
            push(isum[l], pi.at[l, plus(r, k, rows)], ri.at[l, k - 1], r_dev(k))

    def item_gather(l, mine):
        i_pan[l, r] = mine
        for k in ring:
            push(ig[l], i_pan.at[l, r], i_pan.at[l, r], r_dev(k))

    def item_sum(l):
        arrive(isum[l], ri.at[l])
        acc = pi[l, r]
        for k in ring:
            acc = acc + ri[l, k - 1]
        mine = acc.astype(BF16).astype(F32)
        itot[...] += mine
        return mine

    def item_panel(l):
        arrive(ig[l], i_pan.at[l, pl.ds(0, rows - 1)])
        return i_pan[l].reshape(emb, iblk).astype(BF16)

    def pick_rows(t):
        ids = (tri_ref[0:1, t * tw:(t + 1) * tw] - r * (chunks * ublk)).astype(F32)
        ids = jnp.broadcast_to(ids, (8, tw)).T[:, :1]
        lane = lax.broadcasted_iota(jnp.int32, (tw, ublk), 1).astype(F32)
        for j in range(chunks):
            oh[:, j * ublk:(j + 1) * ublk] = jnp.where(ids - j * ublk == lane, 1.0, 0.0).astype(BF16)
        rows_got = mm(oh[...], adj[...].reshape(chunks * ublk, iblk))
        apick[t] = rows_got.astype(BF16)

    def pick_product(panel):
        for t in range(tiles):
            part = mm(panel, apick[t], NT)
            for h in range(tw // 128):
                jz, jy = divmod(t * (tw // 128) + h, SIDE)
                cut = part[:, h * 128:(h + 1) * 128]
                ppa[jy, plus(jz + SIDE, -z, SIDE)] = cut[:half]
                ppb[jz, plus(jy + SIDE, -y, SIDE)] = cut[half:]
        for g in range(len(groups)):
            sum_send(pick_bufs, g)

    def pick_users(l):
        local = tri_ref[0:1, pl.ds(pl.multiple_of(c * 128, 128), 128)] - r * (chunks * ublk)
        blk_id = jnp.where(local < 0, -1, lax.div(local, ublk))
        at_row = lax.broadcasted_iota(jnp.int32, (ublk, 128), 0)
        hit = jnp.where(local - blk_id * ublk == at_row, 1.0, 0.0).astype(BF16)
        got_a = mm(ua[l].reshape(chunks * half, ublk), hit)
        got_b = mm(ub[l].reshape(chunks * half, ublk), hit)
        vec_a = jnp.zeros((half, 128), F32)
        vec_b = jnp.zeros((half, 128), F32)
        for jz in range(SIDE):
            for jy in range(SIDE):
                here = blk_id == jz * SIDE + jy
                ja = (jy * SIDE + jz) * half
                jb = (jz * SIDE + jy) * half
                vec_a = vec_a + jnp.where(here, got_a[ja:ja + half], 0.0)
                vec_b = vec_b + jnp.where(here, got_b[jb:jb + half], 0.0)
        if l:
            vec_a = upick[pl.ds(0, half)] + vec_a
            vec_b = upick[pl.ds(half, half)] + vec_b
        upick[pl.ds(0, half)] = vec_a
        upick[pl.ds(half, half)] = vec_b

    def item_hits():
        at_row = lax.broadcasted_iota(jnp.int32, (ublk, tw), 0)
        for which in (1, 2):
            for t in range(tiles):
                local = tri_ref[which:which + 1, t * tw:(t + 1) * tw] - c * iblk
                hit = lax.rem(local + USER_SPAN * ublk, ublk) == at_row
                ihit[which - 1, t] = jnp.where(hit, 1.0, 0.0).astype(BF16)

    def pick_items(mine):
        lhs = jnp.concatenate([mine[:, h * ublk:(h + 1) * ublk] for h in range(iblk // ublk)], axis=0).astype(BF16)
        width = mine.shape[0]
        for which in (1, 2):
            for t in range(tiles):
                local = tri_ref[which:which + 1, t * tw:(t + 1) * tw] - c * iblk
                got = mm(lhs, ihit[which - 1, t])
                vec = jnp.zeros((width, tw), F32)
                for h in range(iblk // ublk):
                    here = (local >= h * ublk) & (local < (h + 1) * ublk)
                    vec = vec + jnp.where(here, got[h * width:(h + 1) * width], 0.0)
                for h in range(tw // 128):
                    px[t * (tw // 128) + h, which - 1] = vec[:, h * 128:(h + 1) * 128]

    du_s, dz_s, di_s = sems(1), sems(1), sems(1)
    ones = jnp.ones((8, iblk), BF16)
    di_acc = jnp.zeros((8, iblk), jnp.int32)
    for j in range(chunks):
        loads[j].wait()
        blk = mask_buf[j]
        di_acc = di_acc + jnp.sum(blk.reshape(ublk // 8, 8, iblk), axis=0)
        blk = blk.astype(F32).astype(BF16)
        adj[j] = blk
        du_own[pl.ds(j, 1), :] = mm(ones, blk, NT)[:1]
    di_own[...] = di_acc.astype(F32)
    pl.semaphore_wait(barrier, len(plane) + len(ring))
    for k in sides:
        push(du_s, du_own, du_y.at[k - 1], y_dev(k))
    for k in ring:
        push(di_s, di_own, di_got.at[k - 1], r_dev(k))
    user_gather_start(0)
    for k in ring:
        copy(i_nat.at[r], i_nat.at[r], ig[0], r_dev(k), 3).start()
    arrive(du_s, du_y)
    du_ysum[...] = du_own[...] + du_y[0] + du_y[1] + du_y[2]
    for k in sides:
        push(dz_s, du_ysum, du_z.at[k - 1], z_dev(k))
    arrive(ig[0], i_nat.at[pl.ds(0, rows - 1)])
    item0 = mm(eye, i_nat[...].reshape(iblk, emb), NT)
    i_pan[0] = item0.reshape(i_pan.shape[1:])
    itot[...] = i_pan[0, r]
    item0 = item0.astype(BF16)
    user_gather_fwd(0)
    arrive(di_s, di_got)
    deg_i = di_own[...]
    for k in ring:
        deg_i = deg_i + di_got[k - 1]
    deg_i = jnp.sum(deg_i, axis=0, keepdims=True)
    scale_i = lax.rsqrt(jnp.maximum(deg_i, 1.0))
    arrive(dz_s, du_z)
    deg_u = du_ysum[...] + du_z[0] + du_z[1] + du_z[2]
    du_inv[...] = lax.rsqrt(jnp.maximum(deg_u, 1.0))

    def build(j):
        scale_u = jnp.broadcast_to(du_inv[pl.ds(j, 1), :], (8, ublk)).T[:, :1]
        blk = adj[j] * (scale_u * scale_i).astype(BF16)
        adj[j] = blk
        return blk

    s_u, s_i, s_m, s_l = sems(1), sems(1), sems(1), sems(1)
    user_product(0, item0, 0, build)
    user_sum_send(0, 0)
    user_product(0, item0, 1, build)
    user_sum_send(0, 1)
    user_product(0, item0, 2, build)
    user_sum_send(0, 2)
    user_product(0, item0, 3, build)
    user_gather_end(0)
    item_product(0)
    pick_rows(0)
    mine = item_sum(0)
    item_gather(1, mine)
    pick_rows(1)
    user_sum_1(0)
    panel1 = item_panel(1)
    user_product(1, panel1, 0)
    user_sum_send(1, 0)
    user_product(1, panel1, 1)
    user_product(1, panel1, 2)
    user_product(1, panel1, 3)
    user_keep(1, *user_sum_2(0))
    user_gather_start(1)
    user_sum_send(1, 1)
    pick_rows(2)
    user_gather_fwd(1)
    user_sum_send(1, 2)
    pick_rows(3)
    pick_rows(4)
    pick_rows(5)
    user_sum_1(1)
    user_gather_end(1)
    item_product(1)
    item_hits()
    pick_users(0)
    pick_users(1)
    user_keep(2, *user_sum_2(1))
    user_gather_start(2)
    mine = item_sum(1)
    item_gather(2, mine)
    user_gather_fwd(2)
    pick_rows(6)
    pick_rows(7)
    panel2 = item_panel(2)
    pick_product(panel2)
    user_gather_end(2)
    item_product(2)
    pick_users(2)
    sum_1(pick_bufs)
    item_sum(2)
    out_slice = (itot[...] / (LAYERS + 1)).astype(BF16).astype(F32)
    pick_items(out_slice)
    for k in plane:
        push(s_i, px.at[plus(c, k, chunks)], pxr.at[k - 1], c_dev(k))
    vec_a, vec_b = sum_2(pick_bufs)
    vec_a = ((upick[pl.ds(0, half)] + vec_a.astype(F32)) / (LAYERS + 1)).astype(BF16).astype(F32)
    vec_b = ((upick[pl.ds(half, half)] + vec_b.astype(F32)) / (LAYERS + 1)).astype(BF16).astype(F32)
    vx[...] = jnp.concatenate([vec_a, vec_b], axis=0).reshape(vx.shape)
    for k in ring:
        push(s_u, vx.at[plus(r, k, rows)], vxr.at[k - 1], r_dev(k))
    user_product(2, panel2, 0)
    user_sum_send(2, 0)
    user_product(2, panel2, 1)
    user_sum_send(2, 1)
    user_product(2, panel2, 2)
    user_sum_send(2, 2)
    user_product(2, panel2, 3)
    item_gather(3, out_slice)
    arrive(s_u, vxr)
    vec_u = vx[r]
    for k in ring:
        vec_u = vec_u + vxr[k - 1]
    arrive(s_i, pxr)
    vec_p, vec_n = px[c, 0], px[c, 1]
    for k in plane:
        vec_p = vec_p + pxr[k - 1, 0]
        vec_n = vec_n + pxr[k - 1, 1]
    part = jnp.sum(vec_u * vec_p, axis=0, keepdims=True) - jnp.sum(vec_u * vec_n, axis=0, keepdims=True)
    tiny[chunks + r] = part
    for k in ring:
        push(s_m, tiny.at[chunks + r], tiny.at[chunks + r], r_dev(k))
    arrive(s_m, tiny.at[pl.ds(chunks, rows - 1)])
    neg_x = -tiny[chunks]
    for k in range(1, rows):
        neg_x = neg_x - tiny[chunks + k]
    tiny[c] = jnp.maximum(neg_x, 0.0) + jnp.log1p(jnp.exp(-jnp.abs(neg_x)))
    for k in plane:
        push(s_l, tiny.at[c], tiny.at[c], c_dev(k))
    user_sum_1(2)
    user_sum_2(2)
    ou_ref[...] = (utot[...] / (LAYERS + 1)).astype(BF16)
    out_it = item_panel(3)
    oi_nat[...] = mm(out_it, eye, TN).reshape(oi_nat.shape)
    oi_ref[...] = oi_nat[r].astype(BF16)
    arrive(s_l, tiny.at[pl.ds(0, chunks - 1)])
    for k in range(chunks):
        loss_ref[pl.ds(k, 1), :] = tiny[k]

    span = mask_buf.reshape(chunks * ublk, iblk)
    ends = (
        span.at[pl.ds(0, sum(sent[0]) // (4 * iblk))],
        span.at[pl.ds(0, sum(sent[1]) // 512), pl.ds(0, 128)],
        tiny.at[pl.ds(0, sum(sent[2]) // 512)],
        i_nat.at[pl.ds(0, rows - 1)],
    )
    for kind, whole in enumerate(ends):
        copy(whole, whole, 0, {"row": r}, kind).wait_send()
    assert count[0] == recv_sem.shape[0]
    assert all(size % 512 == 0 for size in sent[2])


def emit(ou_in, oi_in, loss_in, ou_ref, oi_ref, loss_ref):
    ou_ref[...] = ou_in[...]
    oi_ref[...] = oi_in[...]
    loss_ref[...] = loss_in[...]


def solution(mesh):
    rows = mesh.shape["row"]
    cols = mesh.shape["col"]

    def device_body(mask_blk, user_shard, item_shard, triples):
        ublk, emb = user_shard.shape
        isub = item_shard.shape[0]
        iblk = mask_blk.shape[1]
        batch = triples.shape[0]
        half = emb // 2
        width = emb // rows
        tw = 256
        tiles = batch // tw
        n_sem = 10 * LAYERS + 8 * (LAYERS + 1) + 2 * LAYERS + 1 + 3 + 4
        vmem = pltpu.VMEM
        out_user, out_item, loss = pl.pallas_call(
            functools.partial(kernel, rows),
            name="lightgcn",
            out_shape=(
                jax.ShapeDtypeStruct((emb, ublk), BF16),
                jax.ShapeDtypeStruct((isub, emb), BF16),
                jax.ShapeDtypeStruct((batch // 128, 128), F32),
            ),
            in_specs=[pl.BlockSpec(memory_space=pl.ANY)] + [pl.BlockSpec(memory_space=vmem)] * 3,
            out_specs=tuple([pl.BlockSpec(memory_space=vmem)] * 3),
            scratch_shapes=[
                vmem((cols, ublk, iblk), jnp.int32),
                vmem((cols, ublk, iblk), BF16),
                vmem((LAYERS, SIDE, SIDE, half, ublk), BF16),
                vmem((LAYERS, SIDE, SIDE, half, ublk), BF16),
                vmem((LAYERS, SIDE, SIDE, half, ublk), F32),
                vmem((LAYERS, SIDE, SIDE, half, ublk), F32),
                vmem((LAYERS, 3, SIDE, half, ublk), F32),
                vmem((LAYERS, 3, SIDE, half, ublk), F32),
                vmem((LAYERS, SIDE, half, ublk), F32),
                vmem((LAYERS, SIDE, half, ublk), F32),
                vmem((LAYERS, 3, half, ublk), F32),
                vmem((LAYERS, 3, half, ublk), F32),
                vmem((emb, ublk), F32),
                vmem((rows, isub, emb), BF16),
                vmem((LAYERS + 1, rows, width, iblk), F32),
                vmem((LAYERS, rows, width, iblk), F32),
                vmem((LAYERS, rows - 1, width, iblk), F32),
                vmem((width, iblk), F32),
                vmem((cols, ublk), F32),
                vmem((3, cols, ublk), F32),
                vmem((cols, ublk), F32),
                vmem((3, cols, ublk), F32),
                vmem((cols, ublk), F32),
                vmem((8, iblk), F32),
                vmem((rows - 1, 8, iblk), F32),
                vmem((rows, isub, emb), F32),
                vmem((tw, cols * ublk), BF16),
                vmem((tiles, tw, iblk), BF16),
                vmem((2, tiles, ublk, tw), BF16),
                vmem((SIDE, SIDE, half, 128), F32),
                vmem((SIDE, SIDE, half, 128), F32),
                vmem((3, SIDE, half, 128), F32),
                vmem((3, SIDE, half, 128), F32),
                vmem((SIDE, half, 128), F32),
                vmem((SIDE, half, 128), F32),
                vmem((3, half, 128), F32),
                vmem((3, half, 128), F32),
                vmem((emb, 128), F32),
                vmem((rows, width, 128), F32),
                vmem((rows - 1, width, 128), F32),
                vmem((cols, 2, width, 128), F32),
                vmem((cols - 1, 2, width, 128), F32),
                vmem((cols + rows, 1, 128), F32),
                pltpu.SemaphoreType.DMA((cols,)),
                pltpu.SemaphoreType.DMA((4,)),
                pltpu.SemaphoreType.DMA((n_sem,)),
            ],
            compiler_params=pltpu.CompilerParams(collective_id=0, has_side_effects=True),
        )(mask_blk, user_shard.T, item_shard, triples.T)
        out_user, out_item, loss = pl.pallas_call(
            emit,
            name="emit",
            out_shape=(
                jax.ShapeDtypeStruct((emb, ublk), BF16),
                jax.ShapeDtypeStruct((isub, emb), BF16),
                jax.ShapeDtypeStruct((batch // 128, 128), F32),
            ),
        )(out_user, out_item, loss)
        return out_user.T, out_item, loss.reshape(batch)

    return jax.shard_map(
        device_body,
        mesh=mesh,
        in_specs=(P("row", "col"), P(("row", "col"), None), P(("col", "row"), None), P()),
        out_specs=(P(("row", "col"), None), P(("col", "row"), None), P()),
        check_vma=False,
    )
```

```python
import functools
import math

import jax
import jax.numpy as jnp
from jax import lax
from jax.experimental import pallas as pl
from jax.experimental.pallas import tpu as pltpu
from jax.sharding import PartitionSpec as P

LAYERS = 3
SIDE = 4
USER_SPAN = 128
AHEAD = 5
F32 = jnp.float32
BF16 = jnp.bfloat16
NN = (((1,), (0,)), ((), ()))
NT = (((1,), (1,)), ((), ()))
TN = (((0,), (0,)), ((), ()))


def mm(lhs, rhs, dims=NN):
    return lax.dot_general(lhs, rhs, dims, preferred_element_type=F32)


def identity(size):
    at_row = lax.broadcasted_iota(jnp.int32, (size, size), 0)
    at_col = lax.broadcasted_iota(jnp.int32, (size, size), 1)
    return jnp.where(at_row == at_col, 1.0, 0.0).astype(BF16)


def kernel(
    rows, mask_hbm, eu_ref, ei_ref, tri_ref, ou_ref, oi_ref, loss_ref,
    mask_buf, adj, ua, ub, pa, pb, ra, rb, sa, sb, qa, qb, utot,
    i_nat, i_pan, pi, ri, itot, du_own, du_y, du_ysum, du_z, du_inv, di_own, di_got,
    oi_nat, oh, apick, ihit, ppa, ppb, pra, prb, psa, psb, pqa, pqb, upick,
    vx, vxr, px, pxr, tiny,
    load_sem, send_sem, recv_sem,
):
    r = lax.axis_index("row")
    c = lax.axis_index("col")
    z, y = lax.div(c, SIDE), lax.rem(c, SIDE)
    half = ua.shape[-2]
    emb = 2 * half
    ublk = ua.shape[-1]
    chunks = SIDE * SIDE
    iblk = adj.shape[-1]
    isub = i_nat.shape[1]
    tiles, tw = apick.shape[:2]

    def plus(base, k, n):
        return lax.rem(base + k, n)

    def y_dev(k):
        return {"col": z * SIDE + plus(y, k, SIDE)}

    def z_dev(k):
        return {"col": plus(z, k, SIDE) * SIDE + y}

    def r_dev(k):
        return {"row": plus(r, k, rows)}

    def c_dev(k):
        return {"col": plus(c, k, chunks)}

    sides = (2, 1, 3)
    plane = tuple(range(1, chunks))
    ring = tuple(range(1, rows))
    count = [0]
    sent = [], [], []

    def sems(n):
        first = count[0]
        count[0] += n
        return first

    def copy(src, dst, sem, dev, out=0):
        return pltpu.make_async_remote_copy(
            src_ref=src, dst_ref=dst, send_sem=send_sem.at[out], recv_sem=recv_sem.at[sem],
            device_id=dev, device_id_type=pl.DeviceIdType.MESH)

    def push(sem, src, dst, dev):
        size = math.prod(src.shape) * src.dtype.itemsize
        kind = 0 if size % (32 * iblk) == 0 else 1 if size % 4096 == 0 else 2
        copy(src, dst, sem, dev, kind).start()
        sent[kind].append(size)

    def arrive(sem, whole):
        copy(whole, whole, sem, {"row": r}).wait_recv()

    loads = [pltpu.make_async_copy(mask_hbm.at[pl.ds(j * ublk, ublk)], mask_buf.at[j], load_sem.at[j]) for j in range(chunks)]
    for one in loads[:AHEAD]:
        one.start()

    barrier = pltpu.get_barrier_semaphore()
    for k in plane:
        pl.semaphore_signal(barrier, inc=1, device_id=c_dev(k), device_id_type=pl.DeviceIdType.MESH)
    for k in ring:
        pl.semaphore_signal(barrier, inc=1, device_id=r_dev(k), device_id_type=pl.DeviceIdType.MESH)

    eye = identity(emb)
    user0 = eu_ref[...]
    utot[...] = user0.astype(F32)
    ua[0, y, z] = user0[:half]
    ub[0, z, y] = user0[half:]
    i_nat[r] = ei_ref[...]
    ug = [sems(10) for _ in range(LAYERS)]

    def user_gather_start(l):
        for k in sides:
            push(ug[l] + k, ua.at[l, y, z], ua.at[l, y, z], z_dev(k))
            push(ug[l] + 4 + k, ub.at[l, z, y], ub.at[l, z, y], y_dev(k))
        for k in sides:
            push(ug[l] + 8, ua.at[l, y, z], ua.at[l, y, z], y_dev(k))
            push(ug[l] + 9, ub.at[l, z, y], ub.at[l, z, y], z_dev(k))

    def user_gather_fwd(l):
        for q in (1, 3, 2):
            at_z, at_y = plus(z, SIDE - q, SIDE), plus(y, SIDE - q, SIDE)
            arrive(ug[l] + q, ua.at[l, y, at_z])
            for k in sides:
                push(ug[l] + 8, ua.at[l, y, at_z], ua.at[l, y, at_z], y_dev(k))
            arrive(ug[l] + 4 + q, ub.at[l, z, at_y])
            for k in sides:
                push(ug[l] + 9, ub.at[l, z, at_y], ub.at[l, z, at_y], z_dev(k))

    def user_gather_end(l):
        arrive(ug[l] + 8, ua.at[l, pl.ds(0, SIDE - 1)])
        arrive(ug[l] + 9, ub.at[l, pl.ds(0, SIDE - 1)])

    us = [sems(8) for _ in range(LAYERS + 1)]
    groups = ((2, 2), (1, 1), (0, 1))
    order = (
        ((2, 2), (2, 3), (3, 2), (3, 3), (2, 1), (3, 1), (1, 2), (1, 3)),
        ((1, 1),),
        ((0, 1), (0, 2), (0, 3), (1, 0), (2, 0), (3, 0)),
        ((0, 0),),
    )

    def layer_bufs(l):
        return us[l], [ref.at[l] for ref in (pa, pb, ra, rb, sa, sb, qa, qb)]

    pick_bufs = us[LAYERS], [ppa, ppb, pra, prb, psa, psb, pqa, pqb]

    def sum_send(bufs, g):
        sem, (own_a, own_b, got_a, got_b) = bufs[0], bufs[1][:4]
        part = pl.ds(*groups[g])
        for k in sides:
            push(sem + g, own_a.at[plus(y, k, SIDE), part], got_a.at[k - 1, part], y_dev(k))
            push(sem + 4 + g, own_b.at[plus(z, k, SIDE), part], got_b.at[k - 1, part], z_dev(k))

    def sum_1(bufs):
        sem, (own_a, own_b, got_a, got_b, mid_a, mid_b, end_a, end_b) = bufs
        for g, (lo, n) in enumerate(groups):
            part = pl.ds(lo, n)
            arrive(sem + g, got_a.at[:, part])
            arrive(sem + 4 + g, got_b.at[:, part])
            for j in range(lo, lo + n):
                mid_a[j] = own_a[y, j] + got_a[0, j] + got_a[1, j] + got_a[2, j]
                mid_b[j] = own_b[z, j] + got_b[0, j] + got_b[1, j] + got_b[2, j]
            for k in range(lo, lo + n):
                if k:
                    push(sem + 3, mid_a.at[k], end_a.at[k - 1], z_dev(k))
                    push(sem + 7, mid_b.at[k], end_b.at[k - 1], y_dev(k))

    def sum_2(bufs):
        sem, (mid_a, mid_b, end_a, end_b) = bufs[0], bufs[1][4:]
        arrive(sem + 3, end_a)
        arrive(sem + 7, end_b)
        next_a = (mid_a[0] + end_a[0] + end_a[1] + end_a[2]).astype(BF16)
        next_b = (mid_b[0] + end_b[0] + end_b[1] + end_b[2]).astype(BF16)
        return next_a, next_b

    def user_product(l, panel, g, build=None):
        for dz, dy in order[g]:
            jz, jy = plus(z, dz, SIDE), plus(y, dy, SIDE)
            j = jz * SIDE + jy
            blk = adj[j] if build is None else build(j)
            part = mm(panel, blk, NT)
            pa[l, jy, dz] = part[:half]
            pb[l, jz, dy] = part[half:]

    def user_sum_send(l, g):
        sum_send(layer_bufs(l), g)

    def user_sum_1(l):
        sum_1(layer_bufs(l))

    def user_sum_2(l):
        next_a, next_b = sum_2(layer_bufs(l))
        utot[pl.ds(0, half)] += next_a.astype(F32)
        utot[pl.ds(half, half)] += next_b.astype(F32)
        return next_a, next_b

    def user_keep(l, next_a, next_b):
        ua[l, y, z] = next_a
        ub[l, z, y] = next_b

    ig = [sems(1) for _ in range(LAYERS + 1)]
    isum = [sems(1) for _ in range(LAYERS)]

    def item_product(l):
        def step(j, acc):
            jz, jy = lax.div(j, SIDE), lax.rem(j, SIDE)
            lhs = jnp.concatenate([ua[l, jy, jz], ub[l, jz, jy]], axis=0)
            return acc + mm(lhs, adj[j])
        acc = lax.fori_loop(0, chunks, step, jnp.zeros((emb, iblk), F32), unroll=4)
        pi[l] = acc.reshape(pi.shape[1:])
        for k in ring:
            push(isum[l], pi.at[l, plus(r, k, rows)], ri.at[l, k - 1], r_dev(k))

    def item_gather(l, mine):
        i_pan[l, r] = mine
        for k in ring:
            push(ig[l], i_pan.at[l, r], i_pan.at[l, r], r_dev(k))

    def item_sum(l):
        arrive(isum[l], ri.at[l])
        acc = pi[l, r]
        for k in ring:
            acc = acc + ri[l, k - 1]
        mine = acc.astype(BF16).astype(F32)
        itot[...] += mine
        return mine

    def item_panel(l):
        arrive(ig[l], i_pan.at[l, pl.ds(0, rows - 1)])
        return i_pan[l].reshape(emb, iblk).astype(BF16)

    def pick_rows(t):
        ids = (tri_ref[0:1, t * tw:(t + 1) * tw] - r * (chunks * ublk)).astype(F32)
        ids = jnp.broadcast_to(ids, (8, tw)).T[:, :1]
        lane = lax.broadcasted_iota(jnp.int32, (tw, ublk), 1).astype(F32)
        for j in range(chunks):
            oh[:, j * ublk:(j + 1) * ublk] = jnp.where(ids - j * ublk == lane, 1.0, 0.0).astype(BF16)
        rows_got = mm(oh[...], adj[...].reshape(chunks * ublk, iblk))
        apick[t] = rows_got.astype(BF16)

    def pick_product(panel):
        for t in range(tiles):
            part = mm(panel, apick[t], NT)
            for h in range(tw // 128):
                jz, jy = divmod(t * (tw // 128) + h, SIDE)
                cut = part[:, h * 128:(h + 1) * 128]
                ppa[jy, plus(jz + SIDE, -z, SIDE)] = cut[:half]
                ppb[jz, plus(jy + SIDE, -y, SIDE)] = cut[half:]
        for g in range(len(groups)):
            sum_send(pick_bufs, g)

    def pick_users(l):
        local = tri_ref[0:1, pl.ds(pl.multiple_of(c * 128, 128), 128)] - r * (chunks * ublk)
        blk_id = jnp.where(local < 0, -1, lax.div(local, ublk))
        at_row = lax.broadcasted_iota(jnp.int32, (ublk, 128), 0)
        hit = jnp.where(local - blk_id * ublk == at_row, 1.0, 0.0).astype(BF16)
        got_a = mm(ua[l].reshape(chunks * half, ublk), hit)
        got_b = mm(ub[l].reshape(chunks * half, ublk), hit)
        vec_a = jnp.zeros((half, 128), F32)
        vec_b = jnp.zeros((half, 128), F32)
        for jz in range(SIDE):
            for jy in range(SIDE):
                here = blk_id == jz * SIDE + jy
                ja = (jy * SIDE + jz) * half
                jb = (jz * SIDE + jy) * half
                vec_a = vec_a + jnp.where(here, got_a[ja:ja + half], 0.0)
                vec_b = vec_b + jnp.where(here, got_b[jb:jb + half], 0.0)
        if l:
            vec_a = upick[pl.ds(0, half)] + vec_a
            vec_b = upick[pl.ds(half, half)] + vec_b
        upick[pl.ds(0, half)] = vec_a
        upick[pl.ds(half, half)] = vec_b

    def item_hits():
        at_row = lax.broadcasted_iota(jnp.int32, (ublk, tw), 0)
        for which in (1, 2):
            for t in range(tiles):
                local = tri_ref[which:which + 1, t * tw:(t + 1) * tw] - c * iblk
                hit = lax.rem(local + USER_SPAN * ublk, ublk) == at_row
                ihit[which - 1, t] = jnp.where(hit, 1.0, 0.0).astype(BF16)

    def pick_items(mine):
        lhs = jnp.concatenate([mine[:, h * ublk:(h + 1) * ublk] for h in range(iblk // ublk)], axis=0).astype(BF16)
        width = mine.shape[0]
        for which in (1, 2):
            for t in range(tiles):
                local = tri_ref[which:which + 1, t * tw:(t + 1) * tw] - c * iblk
                got = mm(lhs, ihit[which - 1, t])
                vec = jnp.zeros((width, tw), F32)
                for h in range(iblk // ublk):
                    here = (local >= h * ublk) & (local < (h + 1) * ublk)
                    vec = vec + jnp.where(here, got[h * width:(h + 1) * width], 0.0)
                for h in range(tw // 128):
                    px[t * (tw // 128) + h, which - 1] = vec[:, h * 128:(h + 1) * 128]

    du_s, dz_s, di_s = sems(1), sems(1), sems(1)
    ones = jnp.ones((8, iblk), BF16)
    di_acc = jnp.zeros((8, iblk), jnp.int32)
    for j in range(chunks):
        loads[j].wait()
        if j + AHEAD < chunks:
            loads[j + AHEAD].start()
        blk = mask_buf[j]
        di_acc = di_acc + jnp.sum(blk.reshape(ublk // 8, 8, iblk), axis=0)
        blk = blk.astype(F32).astype(BF16)
        adj[j] = blk
        du_own[pl.ds(j, 1), :] = mm(ones, blk, NT)[:1]
    di_own[...] = di_acc.astype(F32)
    pl.semaphore_wait(barrier, len(plane) + len(ring))
    for k in sides:
        push(du_s, du_own, du_y.at[k - 1], y_dev(k))
    for k in ring:
        push(di_s, di_own, di_got.at[k - 1], r_dev(k))
    user_gather_start(0)
    for k in ring:
        copy(i_nat.at[r], i_nat.at[r], ig[0], r_dev(k), 3).start()
    arrive(du_s, du_y)
    du_ysum[...] = du_own[...] + du_y[0] + du_y[1] + du_y[2]
    for k in sides:
        push(dz_s, du_ysum, du_z.at[k - 1], z_dev(k))
    arrive(ig[0], i_nat.at[pl.ds(0, rows - 1)])
    item0 = mm(eye, i_nat[...].reshape(iblk, emb), NT)
    i_pan[0] = item0.reshape(i_pan.shape[1:])
    itot[...] = i_pan[0, r]
    item0 = item0.astype(BF16)
    user_gather_fwd(0)
    arrive(di_s, di_got)
    deg_i = di_own[...]
    for k in ring:
        deg_i = deg_i + di_got[k - 1]
    deg_i = jnp.sum(deg_i, axis=0, keepdims=True)
    scale_i = lax.rsqrt(jnp.maximum(deg_i, 1.0))
    arrive(dz_s, du_z)
    deg_u = du_ysum[...] + du_z[0] + du_z[1] + du_z[2]
    du_inv[...] = lax.rsqrt(jnp.maximum(deg_u, 1.0))

    def build(j):
        scale_u = jnp.broadcast_to(du_inv[pl.ds(j, 1), :], (8, ublk)).T[:, :1]
        blk = adj[j] * (scale_u * scale_i).astype(BF16)
        adj[j] = blk
        return blk

    s_u, s_i, s_m, s_l = sems(1), sems(1), sems(1), sems(1)
    user_product(0, item0, 0, build)
    user_sum_send(0, 0)
    user_product(0, item0, 1, build)
    user_sum_send(0, 1)
    user_product(0, item0, 2, build)
    user_sum_send(0, 2)
    user_product(0, item0, 3, build)
    user_gather_end(0)
    item_product(0)
    pick_rows(0)
    mine = item_sum(0)
    item_gather(1, mine)
    pick_rows(1)
    user_sum_1(0)
    panel1 = item_panel(1)
    user_product(1, panel1, 0)
    user_sum_send(1, 0)
    user_product(1, panel1, 1)
    user_product(1, panel1, 2)
    user_product(1, panel1, 3)
    user_keep(1, *user_sum_2(0))
    user_gather_start(1)
    user_sum_send(1, 1)
    pick_rows(2)
    user_gather_fwd(1)
    user_sum_send(1, 2)
    pick_rows(3)
    pick_rows(4)
    pick_rows(5)
    user_sum_1(1)
    user_gather_end(1)
    item_product(1)
    item_hits()
    pick_users(0)
    pick_users(1)
    user_keep(2, *user_sum_2(1))
    user_gather_start(2)
    mine = item_sum(1)
    item_gather(2, mine)
    user_gather_fwd(2)
    pick_rows(6)
    pick_rows(7)
    panel2 = item_panel(2)
    pick_product(panel2)
    user_gather_end(2)
    item_product(2)
    pick_users(2)
    sum_1(pick_bufs)
    item_sum(2)
    out_slice = (itot[...] / (LAYERS + 1)).astype(BF16).astype(F32)
    pick_items(out_slice)
    for k in plane:
        push(s_i, px.at[plus(c, k, chunks)], pxr.at[k - 1], c_dev(k))
    vec_a, vec_b = sum_2(pick_bufs)
    vec_a = ((upick[pl.ds(0, half)] + vec_a.astype(F32)) / (LAYERS + 1)).astype(BF16).astype(F32)
    vec_b = ((upick[pl.ds(half, half)] + vec_b.astype(F32)) / (LAYERS + 1)).astype(BF16).astype(F32)
    vx[...] = jnp.concatenate([vec_a, vec_b], axis=0).reshape(vx.shape)
    for k in ring:
        push(s_u, vx.at[plus(r, k, rows)], vxr.at[k - 1], r_dev(k))
    user_product(2, panel2, 0)
    user_sum_send(2, 0)
    user_product(2, panel2, 1)
    user_sum_send(2, 1)
    user_product(2, panel2, 2)
    user_sum_send(2, 2)
    user_product(2, panel2, 3)
    item_gather(3, out_slice)
    arrive(s_u, vxr)
    vec_u = vx[r]
    for k in ring:
        vec_u = vec_u + vxr[k - 1]
    arrive(s_i, pxr)
    vec_p, vec_n = px[c, 0], px[c, 1]
    for k in plane:
        vec_p = vec_p + pxr[k - 1, 0]
        vec_n = vec_n + pxr[k - 1, 1]
    part = jnp.sum(vec_u * vec_p, axis=0, keepdims=True) - jnp.sum(vec_u * vec_n, axis=0, keepdims=True)
    tiny[chunks + r] = part
    for k in ring:
        push(s_m, tiny.at[chunks + r], tiny.at[chunks + r], r_dev(k))
    arrive(s_m, tiny.at[pl.ds(chunks, rows - 1)])
    neg_x = -tiny[chunks]
    for k in range(1, rows):
        neg_x = neg_x - tiny[chunks + k]
    tiny[c] = jnp.maximum(neg_x, 0.0) + jnp.log1p(jnp.exp(-jnp.abs(neg_x)))
    for k in plane:
        push(s_l, tiny.at[c], tiny.at[c], c_dev(k))
    user_sum_1(2)
    user_sum_2(2)
    ou_ref[...] = (utot[...] / (LAYERS + 1)).astype(BF16)
    out_it = item_panel(3)
    oi_nat[...] = mm(out_it, eye, TN).reshape(oi_nat.shape)
    oi_ref[...] = oi_nat[r].astype(BF16)
    arrive(s_l, tiny.at[pl.ds(0, chunks - 1)])
    for k in range(chunks):
        loss_ref[pl.ds(k, 1), :] = tiny[k]

    span = mask_buf.reshape(chunks * ublk, iblk)
    ends = (
        span.at[pl.ds(0, sum(sent[0]) // (4 * iblk))],
        span.at[pl.ds(0, sum(sent[1]) // 512), pl.ds(0, 128)],
        tiny.at[pl.ds(0, sum(sent[2]) // 512)],
        i_nat.at[pl.ds(0, rows - 1)],
    )
    for kind, whole in enumerate(ends):
        copy(whole, whole, 0, {"row": r}, kind).wait_send()
    assert count[0] == recv_sem.shape[0]
    assert all(size % 512 == 0 for size in sent[2])


def emit(ou_in, oi_in, loss_in, ou_ref, oi_ref, loss_ref):
    ou_ref[...] = ou_in[...]
    oi_ref[...] = oi_in[...]
    loss_ref[...] = loss_in[...]


def solution(mesh):
    rows = mesh.shape["row"]
    cols = mesh.shape["col"]

    def device_body(mask_blk, user_shard, item_shard, triples):
        ublk, emb = user_shard.shape
        isub = item_shard.shape[0]
        iblk = mask_blk.shape[1]
        batch = triples.shape[0]
        half = emb // 2
        width = emb // rows
        tw = 256
        tiles = batch // tw
        n_sem = 10 * LAYERS + 8 * (LAYERS + 1) + 2 * LAYERS + 1 + 3 + 4
        vmem = pltpu.VMEM
        out_user, out_item, loss = pl.pallas_call(
            functools.partial(kernel, rows),
            name="lightgcn",
            out_shape=(
                jax.ShapeDtypeStruct((emb, ublk), BF16),
                jax.ShapeDtypeStruct((isub, emb), BF16),
                jax.ShapeDtypeStruct((batch // 128, 128), F32),
            ),
            in_specs=[pl.BlockSpec(memory_space=pltpu.HBM)] + [pl.BlockSpec(memory_space=vmem)] * 3,
            out_specs=tuple([pl.BlockSpec(memory_space=vmem)] * 3),
            scratch_shapes=[
                vmem((cols, ublk, iblk), jnp.int32),
                vmem((cols, ublk, iblk), BF16),
                vmem((LAYERS, SIDE, SIDE, half, ublk), BF16),
                vmem((LAYERS, SIDE, SIDE, half, ublk), BF16),
                vmem((LAYERS, SIDE, SIDE, half, ublk), F32),
                vmem((LAYERS, SIDE, SIDE, half, ublk), F32),
                vmem((LAYERS, 3, SIDE, half, ublk), F32),
                vmem((LAYERS, 3, SIDE, half, ublk), F32),
                vmem((LAYERS, SIDE, half, ublk), F32),
                vmem((LAYERS, SIDE, half, ublk), F32),
                vmem((LAYERS, 3, half, ublk), F32),
                vmem((LAYERS, 3, half, ublk), F32),
                vmem((emb, ublk), F32),
                vmem((rows, isub, emb), BF16),
                vmem((LAYERS + 1, rows, width, iblk), F32),
                vmem((LAYERS, rows, width, iblk), F32),
                vmem((LAYERS, rows - 1, width, iblk), F32),
                vmem((width, iblk), F32),
                vmem((cols, ublk), F32),
                vmem((3, cols, ublk), F32),
                vmem((cols, ublk), F32),
                vmem((3, cols, ublk), F32),
                vmem((cols, ublk), F32),
                vmem((8, iblk), F32),
                vmem((rows - 1, 8, iblk), F32),
                vmem((rows, isub, emb), F32),
                vmem((tw, cols * ublk), BF16),
                vmem((tiles, tw, iblk), BF16),
                vmem((2, tiles, ublk, tw), BF16),
                vmem((SIDE, SIDE, half, 128), F32),
                vmem((SIDE, SIDE, half, 128), F32),
                vmem((3, SIDE, half, 128), F32),
                vmem((3, SIDE, half, 128), F32),
                vmem((SIDE, half, 128), F32),
                vmem((SIDE, half, 128), F32),
                vmem((3, half, 128), F32),
                vmem((3, half, 128), F32),
                vmem((emb, 128), F32),
                vmem((rows, width, 128), F32),
                vmem((rows - 1, width, 128), F32),
                vmem((cols, 2, width, 128), F32),
                vmem((cols - 1, 2, width, 128), F32),
                vmem((cols + rows, 1, 128), F32),
                pltpu.SemaphoreType.DMA((cols,)),
                pltpu.SemaphoreType.DMA((4,)),
                pltpu.SemaphoreType.DMA((n_sem,)),
            ],
            compiler_params=pltpu.CompilerParams(collective_id=0, has_side_effects=True, vmem_limit_bytes=48 * 2**20),
        )(mask_blk, user_shard.T, item_shard, triples.T)
        out_user, out_item, loss = pl.pallas_call(
            emit,
            name="emit",
            out_shape=(
                jax.ShapeDtypeStruct((emb, ublk), BF16),
                jax.ShapeDtypeStruct((isub, emb), BF16),
                jax.ShapeDtypeStruct((batch // 128, 128), F32),
            ),
            compiler_params=pltpu.CompilerParams(vmem_limit_bytes=2**20),
        )(out_user, out_item, loss)
        return out_user.T, out_item, loss.reshape(batch)

    return jax.shard_map(
        device_body,
        mesh=mesh,
        in_specs=(P("row", "col"), P(("row", "col"), None), P(("col", "row"), None), P()),
        out_specs=(P(("row", "col"), None), P(("col", "row"), None), P()),
        check_vma=False,
    )
```

```python
import functools
import math

import jax
import jax.numpy as jnp
from jax import lax
from jax.experimental import pallas as pl
from jax.experimental.pallas import tpu as pltpu
from jax.sharding import PartitionSpec as P

LAYERS = 3
SIDE = 4
USER_SPAN = 128
AHEAD = 5
F32 = jnp.float32
BF16 = jnp.bfloat16
NN = (((1,), (0,)), ((), ()))
NT = (((1,), (1,)), ((), ()))
TN = (((0,), (0,)), ((), ()))


def mm(lhs, rhs, dims=NN):
    return lax.dot_general(lhs, rhs, dims, preferred_element_type=F32)


def identity(size):
    at_row = lax.broadcasted_iota(jnp.int32, (size, size), 0)
    at_col = lax.broadcasted_iota(jnp.int32, (size, size), 1)
    return jnp.where(at_row == at_col, 1.0, 0.0).astype(BF16)


def kernel(
    rows, mask_hbm, eu_hbm, ei_hbm, tri_hbm, ou_ref, oi_ref, loss_ref,
    mask_buf, adj, ua, ub, pa, pb, ra, rb, sa, sb, qa, qb, utot,
    i_nat, i_pan, pi, ri, itot, du_own, du_y, du_ysum, du_z, du_inv, di_own, di_got,
    oi_nat, oh, apick, ihit, ppa, ppb, pra, prb, psa, psb, pqa, pqb, upick,
    vx, vxr, px, pxr, tiny,
    tri_ref, load_sem, send_sem, recv_sem,
):
    r = lax.axis_index("row")
    c = lax.axis_index("col")
    z, y = lax.div(c, SIDE), lax.rem(c, SIDE)
    half = ua.shape[-2]
    emb = 2 * half
    ublk = ua.shape[-1]
    chunks = SIDE * SIDE
    iblk = adj.shape[-1]
    isub = i_nat.shape[1]
    tiles, tw = apick.shape[:2]

    def plus(base, k, n):
        return lax.rem(base + k, n)

    def y_dev(k):
        return {"col": z * SIDE + plus(y, k, SIDE)}

    def z_dev(k):
        return {"col": plus(z, k, SIDE) * SIDE + y}

    def r_dev(k):
        return {"row": plus(r, k, rows)}

    def c_dev(k):
        return {"col": plus(c, k, chunks)}

    sides = (2, 1, 3)
    plane = tuple(range(1, chunks))
    ring = tuple(range(1, rows))
    count = [0]
    sent = [], [], []

    def sems(n):
        first = count[0]
        count[0] += n
        return first

    def copy(src, dst, sem, dev, out=0):
        return pltpu.make_async_remote_copy(
            src_ref=src, dst_ref=dst, send_sem=send_sem.at[out], recv_sem=recv_sem.at[sem],
            device_id=dev, device_id_type=pl.DeviceIdType.MESH)

    def push(sem, src, dst, dev):
        size = math.prod(src.shape) * src.dtype.itemsize
        kind = 0 if size % (32 * iblk) == 0 else 1 if size % 4096 == 0 else 2
        copy(src, dst, sem, dev, kind).start()
        sent[kind].append(size)

    def arrive(sem, whole):
        copy(whole, whole, sem, {"row": r}).wait_recv()

    loads = [pltpu.make_async_copy(mask_hbm.at[pl.ds(j * ublk, ublk)], mask_buf.at[j], load_sem.at[j]) for j in range(chunks)]
    for one in loads[:AHEAD]:
        one.start()
    smalls = [
        pltpu.make_async_copy(eu_hbm.at[pl.ds(0, half)], ua.at[0, y, z], load_sem.at[chunks]),
        pltpu.make_async_copy(eu_hbm.at[pl.ds(half, half)], ub.at[0, z, y], load_sem.at[chunks + 1]),
        pltpu.make_async_copy(ei_hbm, i_nat.at[r], load_sem.at[chunks + 2]),
        pltpu.make_async_copy(tri_hbm, tri_ref, load_sem.at[chunks + 3]),
    ]
    for one in smalls:
        one.start()

    barrier = pltpu.get_barrier_semaphore()
    for k in sides:
        pl.semaphore_signal(barrier, inc=1, device_id=y_dev(k), device_id_type=pl.DeviceIdType.MESH)
        pl.semaphore_signal(barrier, inc=1, device_id=z_dev(k), device_id_type=pl.DeviceIdType.MESH)
    for k in ring:
        pl.semaphore_signal(barrier, inc=1, device_id=r_dev(k), device_id_type=pl.DeviceIdType.MESH)

    eye = identity(emb)
    ug = [sems(10) for _ in range(LAYERS)]

    def user_gather_start(l):
        for k in sides:
            push(ug[l] + k, ua.at[l, y, z], ua.at[l, y, z], z_dev(k))
            push(ug[l] + 4 + k, ub.at[l, z, y], ub.at[l, z, y], y_dev(k))
        for k in sides:
            push(ug[l] + 8, ua.at[l, y, z], ua.at[l, y, z], y_dev(k))
            push(ug[l] + 9, ub.at[l, z, y], ub.at[l, z, y], z_dev(k))

    def user_gather_fwd(l):
        for q in (1, 3, 2):
            at_z, at_y = plus(z, SIDE - q, SIDE), plus(y, SIDE - q, SIDE)
            arrive(ug[l] + q, ua.at[l, y, at_z])
            for k in sides:
                push(ug[l] + 8, ua.at[l, y, at_z], ua.at[l, y, at_z], y_dev(k))
            arrive(ug[l] + 4 + q, ub.at[l, z, at_y])
            for k in sides:
                push(ug[l] + 9, ub.at[l, z, at_y], ub.at[l, z, at_y], z_dev(k))

    def user_gather_end(l):
        arrive(ug[l] + 8, ua.at[l, pl.ds(0, SIDE - 1)])
        arrive(ug[l] + 9, ub.at[l, pl.ds(0, SIDE - 1)])

    us = [sems(8) for _ in range(LAYERS + 1)]
    groups = ((2, 2), (1, 1), (0, 1))
    order = (
        ((2, 2), (2, 3), (3, 2), (3, 3), (2, 1), (3, 1), (1, 2), (1, 3)),
        ((1, 1),),
        ((0, 1), (0, 2), (0, 3), (1, 0), (2, 0), (3, 0)),
        ((0, 0),),
    )

    def layer_bufs(l):
        return us[l], [ref.at[l] for ref in (pa, pb, ra, rb, sa, sb, qa, qb)]

    pick_bufs = us[LAYERS], [ppa, ppb, pra, prb, psa, psb, pqa, pqb]

    def sum_send(bufs, g):
        sem, (own_a, own_b, got_a, got_b) = bufs[0], bufs[1][:4]
        part = pl.ds(*groups[g])
        for k in sides:
            push(sem + g, own_a.at[plus(y, k, SIDE), part], got_a.at[k - 1, part], y_dev(k))
            push(sem + 4 + g, own_b.at[plus(z, k, SIDE), part], got_b.at[k - 1, part], z_dev(k))

    def sum_1(bufs):
        sem, (own_a, own_b, got_a, got_b, mid_a, mid_b, end_a, end_b) = bufs
        for g, (lo, n) in enumerate(groups):
            part = pl.ds(lo, n)
            arrive(sem + g, got_a.at[:, part])
            arrive(sem + 4 + g, got_b.at[:, part])
            for j in range(lo, lo + n):
                mid_a[j] = own_a[y, j] + got_a[0, j] + got_a[1, j] + got_a[2, j]
                mid_b[j] = own_b[z, j] + got_b[0, j] + got_b[1, j] + got_b[2, j]
            for k in range(lo, lo + n):
                if k:
                    push(sem + 3, mid_a.at[k], end_a.at[k - 1], z_dev(k))
                    push(sem + 7, mid_b.at[k], end_b.at[k - 1], y_dev(k))

    def sum_2(bufs):
        sem, (mid_a, mid_b, end_a, end_b) = bufs[0], bufs[1][4:]
        arrive(sem + 3, end_a)
        arrive(sem + 7, end_b)
        next_a = (mid_a[0] + end_a[0] + end_a[1] + end_a[2]).astype(BF16)
        next_b = (mid_b[0] + end_b[0] + end_b[1] + end_b[2]).astype(BF16)
        return next_a, next_b

    def user_product(l, panel, g, build=None):
        for dz, dy in order[g]:
            jz, jy = plus(z, dz, SIDE), plus(y, dy, SIDE)
            j = jz * SIDE + jy
            blk = adj[j] if build is None else build(j)
            part = mm(panel, blk, NT)
            pa[l, jy, dz] = part[:half]
            pb[l, jz, dy] = part[half:]

    def user_sum_send(l, g):
        sum_send(layer_bufs(l), g)

    def user_sum_1(l):
        sum_1(layer_bufs(l))

    def user_sum_2(l):
        next_a, next_b = sum_2(layer_bufs(l))
        utot[pl.ds(0, half)] += next_a.astype(F32)
        utot[pl.ds(half, half)] += next_b.astype(F32)
        return next_a, next_b

    def user_keep(l, next_a, next_b):
        ua[l, y, z] = next_a
        ub[l, z, y] = next_b

    ig = [sems(1) for _ in range(LAYERS + 1)]
    isum = [sems(1) for _ in range(LAYERS)]

    def item_product(l):
        def step(j, acc):
            jz, jy = lax.div(j, SIDE), lax.rem(j, SIDE)
            lhs = jnp.concatenate([ua[l, jy, jz], ub[l, jz, jy]], axis=0)
            return acc + mm(lhs, adj[j])
        acc = lax.fori_loop(0, chunks, step, jnp.zeros((emb, iblk), F32), unroll=4)
        pi[l] = acc.reshape(pi.shape[1:])
        for k in ring:
            push(isum[l], pi.at[l, plus(r, k, rows)], ri.at[l, k - 1], r_dev(k))

    def item_gather(l, mine):
        i_pan[l, r] = mine
        for k in ring:
            push(ig[l], i_pan.at[l, r], i_pan.at[l, r], r_dev(k))

    def item_sum(l):
        arrive(isum[l], ri.at[l])
        acc = pi[l, r]
        for k in ring:
            acc = acc + ri[l, k - 1]
        mine = acc.astype(BF16).astype(F32)
        itot[...] += mine
        return mine

    def item_panel(l):
        arrive(ig[l], i_pan.at[l, pl.ds(0, rows - 1)])
        return i_pan[l].reshape(emb, iblk).astype(BF16)

    def pick_rows(t):
        ids = (tri_ref[0:1, t * tw:(t + 1) * tw] - r * (chunks * ublk)).astype(F32)
        ids = jnp.broadcast_to(ids, (8, tw)).T[:, :1]
        lane = lax.broadcasted_iota(jnp.int32, (tw, ublk), 1).astype(F32)
        for j in range(chunks):
            oh[:, j * ublk:(j + 1) * ublk] = jnp.where(ids - j * ublk == lane, 1.0, 0.0).astype(BF16)
        rows_got = mm(oh[...], adj[...].reshape(chunks * ublk, iblk))
        apick[t] = rows_got.astype(BF16)

    def pick_product(panel):
        for t in range(tiles):
            part = mm(panel, apick[t], NT)
            for h in range(tw // 128):
                jz, jy = divmod(t * (tw // 128) + h, SIDE)
                cut = part[:, h * 128:(h + 1) * 128]
                ppa[jy, plus(jz + SIDE, -z, SIDE)] = cut[:half]
                ppb[jz, plus(jy + SIDE, -y, SIDE)] = cut[half:]
        for g in range(len(groups)):
            sum_send(pick_bufs, g)

    def pick_users(l):
        local = tri_ref[0:1, pl.ds(pl.multiple_of(c * 128, 128), 128)] - r * (chunks * ublk)
        blk_id = jnp.where(local < 0, -1, lax.div(local, ublk))
        at_row = lax.broadcasted_iota(jnp.int32, (ublk, 128), 0)
        hit = jnp.where(local - blk_id * ublk == at_row, 1.0, 0.0).astype(BF16)
        got_a = mm(ua[l].reshape(chunks * half, ublk), hit)
        got_b = mm(ub[l].reshape(chunks * half, ublk), hit)
        vec_a = jnp.zeros((half, 128), F32)
        vec_b = jnp.zeros((half, 128), F32)
        for jz in range(SIDE):
            for jy in range(SIDE):
                here = blk_id == jz * SIDE + jy
                ja = (jy * SIDE + jz) * half
                jb = (jz * SIDE + jy) * half
                vec_a = vec_a + jnp.where(here, got_a[ja:ja + half], 0.0)
                vec_b = vec_b + jnp.where(here, got_b[jb:jb + half], 0.0)
        if l:
            vec_a = upick[pl.ds(0, half)] + vec_a
            vec_b = upick[pl.ds(half, half)] + vec_b
        upick[pl.ds(0, half)] = vec_a
        upick[pl.ds(half, half)] = vec_b

    def item_hits():
        at_row = lax.broadcasted_iota(jnp.int32, (ublk, tw), 0)
        for which in (1, 2):
            for t in range(tiles):
                local = tri_ref[which:which + 1, t * tw:(t + 1) * tw] - c * iblk
                hit = lax.rem(local + USER_SPAN * ublk, ublk) == at_row
                ihit[which - 1, t] = jnp.where(hit, 1.0, 0.0).astype(BF16)

    def pick_items(mine):
        lhs = jnp.concatenate([mine[:, h * ublk:(h + 1) * ublk] for h in range(iblk // ublk)], axis=0).astype(BF16)
        width = mine.shape[0]
        for which in (1, 2):
            for t in range(tiles):
                local = tri_ref[which:which + 1, t * tw:(t + 1) * tw] - c * iblk
                got = mm(lhs, ihit[which - 1, t])
                vec = jnp.zeros((width, tw), F32)
                for h in range(iblk // ublk):
                    here = (local >= h * ublk) & (local < (h + 1) * ublk)
                    vec = vec + jnp.where(here, got[h * width:(h + 1) * width], 0.0)
                for h in range(tw // 128):
                    px[t * (tw // 128) + h, which - 1] = vec[:, h * 128:(h + 1) * 128]

    du_s, dz_s, di_s = sems(1), sems(1), sems(1)
    ones = jnp.ones((8, iblk), BF16)
    di_acc = jnp.zeros((8, iblk), jnp.int32)
    for j in range(chunks):
        loads[j].wait()
        if j + AHEAD < chunks:
            loads[j + AHEAD].start()
        blk = mask_buf[j]
        di_acc = di_acc + jnp.sum(blk.reshape(ublk // 8, 8, iblk), axis=0)
        blk = blk.astype(F32).astype(BF16)
        adj[j] = blk
        du_own[pl.ds(j, 1), :] = mm(ones, blk, NT)[:1]
    di_own[...] = di_acc.astype(F32)
    for one in smalls:
        one.wait()
    pl.semaphore_wait(barrier, 2 * len(sides) + len(ring))
    for k in sides:
        push(du_s, du_own, du_y.at[k - 1], y_dev(k))
    for k in ring:
        push(di_s, di_own, di_got.at[k - 1], r_dev(k))
    user_gather_start(0)
    utot[pl.ds(0, half)] = ua[0, y, z].astype(F32)
    utot[pl.ds(half, half)] = ub[0, z, y].astype(F32)
    for k in ring:
        copy(i_nat.at[r], i_nat.at[r], ig[0], r_dev(k), 3).start()
    arrive(du_s, du_y)
    du_ysum[...] = du_own[...] + du_y[0] + du_y[1] + du_y[2]
    for k in sides:
        push(dz_s, du_ysum, du_z.at[k - 1], z_dev(k))
    arrive(ig[0], i_nat.at[pl.ds(0, rows - 1)])
    item0 = mm(eye, i_nat[...].reshape(iblk, emb), NT)
    i_pan[0] = item0.reshape(i_pan.shape[1:])
    itot[...] = i_pan[0, r]
    item0 = item0.astype(BF16)
    user_gather_fwd(0)
    arrive(di_s, di_got)
    deg_i = di_own[...]
    for k in ring:
        deg_i = deg_i + di_got[k - 1]
    deg_i = jnp.sum(deg_i, axis=0, keepdims=True)
    scale_i = lax.rsqrt(jnp.maximum(deg_i, 1.0))
    arrive(dz_s, du_z)
    deg_u = du_ysum[...] + du_z[0] + du_z[1] + du_z[2]
    du_inv[...] = lax.rsqrt(jnp.maximum(deg_u, 1.0))

    def build(j):
        scale_u = jnp.broadcast_to(du_inv[pl.ds(j, 1), :], (8, ublk)).T[:, :1]
        blk = adj[j] * (scale_u * scale_i).astype(BF16)
        adj[j] = blk
        return blk

    s_u, s_i, s_m, s_l = sems(1), sems(1), sems(1), sems(1)
    user_product(0, item0, 0, build)
    user_sum_send(0, 0)
    user_product(0, item0, 1, build)
    user_sum_send(0, 1)
    user_product(0, item0, 2, build)
    user_sum_send(0, 2)
    user_product(0, item0, 3, build)
    user_gather_end(0)
    item_product(0)
    pick_rows(0)
    mine = item_sum(0)
    item_gather(1, mine)
    pick_rows(1)
    user_sum_1(0)
    panel1 = item_panel(1)
    user_product(1, panel1, 0)
    user_sum_send(1, 0)
    user_product(1, panel1, 1)
    user_product(1, panel1, 2)
    user_product(1, panel1, 3)
    user_keep(1, *user_sum_2(0))
    user_gather_start(1)
    user_sum_send(1, 1)
    pick_rows(2)
    user_gather_fwd(1)
    user_sum_send(1, 2)
    pick_rows(3)
    pick_rows(4)
    pick_rows(5)
    user_sum_1(1)
    user_gather_end(1)
    item_product(1)
    item_hits()
    pick_users(0)
    pick_users(1)
    user_keep(2, *user_sum_2(1))
    user_gather_start(2)
    mine = item_sum(1)
    item_gather(2, mine)
    user_gather_fwd(2)
    pick_rows(6)
    pick_rows(7)
    panel2 = item_panel(2)
    pick_product(panel2)
    user_gather_end(2)
    item_product(2)
    pick_users(2)
    sum_1(pick_bufs)
    item_sum(2)
    out_slice = (itot[...] / (LAYERS + 1)).astype(BF16).astype(F32)
    pick_items(out_slice)
    for k in plane:
        push(s_i, px.at[plus(c, k, chunks)], pxr.at[k - 1], c_dev(k))
    vec_a, vec_b = sum_2(pick_bufs)
    vec_a = ((upick[pl.ds(0, half)] + vec_a.astype(F32)) / (LAYERS + 1)).astype(BF16).astype(F32)
    vec_b = ((upick[pl.ds(half, half)] + vec_b.astype(F32)) / (LAYERS + 1)).astype(BF16).astype(F32)
    vx[...] = jnp.concatenate([vec_a, vec_b], axis=0).reshape(vx.shape)
    for k in ring:
        push(s_u, vx.at[plus(r, k, rows)], vxr.at[k - 1], r_dev(k))
    user_product(2, panel2, 0)
    user_sum_send(2, 0)
    user_product(2, panel2, 1)
    user_sum_send(2, 1)
    user_product(2, panel2, 2)
    user_sum_send(2, 2)
    user_product(2, panel2, 3)
    item_gather(3, out_slice)
    arrive(s_u, vxr)
    vec_u = vx[r]
    for k in ring:
        vec_u = vec_u + vxr[k - 1]
    arrive(s_i, pxr)
    vec_p, vec_n = px[c, 0], px[c, 1]
    for k in plane:
        vec_p = vec_p + pxr[k - 1, 0]
        vec_n = vec_n + pxr[k - 1, 1]
    part = jnp.sum(vec_u * vec_p, axis=0, keepdims=True) - jnp.sum(vec_u * vec_n, axis=0, keepdims=True)
    tiny[chunks + r] = part
    for k in ring:
        push(s_m, tiny.at[chunks + r], tiny.at[chunks + r], r_dev(k))
    arrive(s_m, tiny.at[pl.ds(chunks, rows - 1)])
    neg_x = -tiny[chunks]
    for k in range(1, rows):
        neg_x = neg_x - tiny[chunks + k]
    tiny[c] = jnp.maximum(neg_x, 0.0) + jnp.log1p(jnp.exp(-jnp.abs(neg_x)))
    for k in plane:
        push(s_l, tiny.at[c], tiny.at[c], c_dev(k))
    user_sum_1(2)
    user_sum_2(2)
    ou_ref[...] = (utot[...] / (LAYERS + 1)).astype(BF16)
    out_it = item_panel(3)
    oi_nat[...] = mm(out_it, eye, TN).reshape(oi_nat.shape)
    oi_ref[...] = oi_nat[r].astype(BF16)
    arrive(s_l, tiny.at[pl.ds(0, chunks - 1)])
    for k in range(chunks):
        loss_ref[pl.ds(k, 1), :] = tiny[k]

    span = mask_buf.reshape(chunks * ublk, iblk)
    ends = (
        span.at[pl.ds(0, sum(sent[0]) // (4 * iblk))],
        span.at[pl.ds(0, sum(sent[1]) // 512), pl.ds(0, 128)],
        tiny.at[pl.ds(0, sum(sent[2]) // 512)],
        i_nat.at[pl.ds(0, rows - 1)],
    )
    for kind, whole in enumerate(ends):
        copy(whole, whole, 0, {"row": r}, kind).wait_send()
    assert count[0] == recv_sem.shape[0]
    assert all(size % 512 == 0 for size in sent[2])


def emit(ou_in, oi_in, loss_in, ou_ref, oi_ref, loss_ref):
    ou_ref[...] = ou_in[...]
    oi_ref[...] = oi_in[...]
    loss_ref[...] = loss_in[...]


def solution(mesh):
    rows = mesh.shape["row"]
    cols = mesh.shape["col"]

    def device_body(mask_blk, user_shard, item_shard, triples):
        ublk, emb = user_shard.shape
        isub = item_shard.shape[0]
        iblk = mask_blk.shape[1]
        batch = triples.shape[0]
        half = emb // 2
        width = emb // rows
        tw = 256
        tiles = batch // tw
        n_sem = 10 * LAYERS + 8 * (LAYERS + 1) + 2 * LAYERS + 1 + 3 + 4
        vmem = pltpu.VMEM
        out_user, out_item, loss = pl.pallas_call(
            functools.partial(kernel, rows),
            name="lightgcn",
            out_shape=(
                jax.ShapeDtypeStruct((emb, ublk), BF16),
                jax.ShapeDtypeStruct((isub, emb), BF16),
                jax.ShapeDtypeStruct((batch // 128, 128), F32),
            ),
            in_specs=[pl.BlockSpec(memory_space=pl.ANY)] * 4,
            out_specs=tuple([pl.BlockSpec(memory_space=vmem)] * 3),
            scratch_shapes=[
                vmem((cols, ublk, iblk), jnp.int32),
                vmem((cols, ublk, iblk), BF16),
                vmem((LAYERS, SIDE, SIDE, half, ublk), BF16),
                vmem((LAYERS, SIDE, SIDE, half, ublk), BF16),
                vmem((LAYERS, SIDE, SIDE, half, ublk), F32),
                vmem((LAYERS, SIDE, SIDE, half, ublk), F32),
                vmem((LAYERS, 3, SIDE, half, ublk), F32),
                vmem((LAYERS, 3, SIDE, half, ublk), F32),
                vmem((LAYERS, SIDE, half, ublk), F32),
                vmem((LAYERS, SIDE, half, ublk), F32),
                vmem((LAYERS, 3, half, ublk), F32),
                vmem((LAYERS, 3, half, ublk), F32),
                vmem((emb, ublk), F32),
                vmem((rows, isub, emb), BF16),
                vmem((LAYERS + 1, rows, width, iblk), F32),
                vmem((LAYERS, rows, width, iblk), F32),
                vmem((LAYERS, rows - 1, width, iblk), F32),
                vmem((width, iblk), F32),
                vmem((cols, ublk), F32),
                vmem((3, cols, ublk), F32),
                vmem((cols, ublk), F32),
                vmem((3, cols, ublk), F32),
                vmem((cols, ublk), F32),
                vmem((8, iblk), F32),
                vmem((rows - 1, 8, iblk), F32),
                vmem((rows, isub, emb), F32),
                vmem((tw, cols * ublk), BF16),
                vmem((tiles, tw, iblk), BF16),
                vmem((2, tiles, ublk, tw), BF16),
                vmem((SIDE, SIDE, half, 128), F32),
                vmem((SIDE, SIDE, half, 128), F32),
                vmem((3, SIDE, half, 128), F32),
                vmem((3, SIDE, half, 128), F32),
                vmem((SIDE, half, 128), F32),
                vmem((SIDE, half, 128), F32),
                vmem((3, half, 128), F32),
                vmem((3, half, 128), F32),
                vmem((emb, 128), F32),
                vmem((rows, width, 128), F32),
                vmem((rows - 1, width, 128), F32),
                vmem((cols, 2, width, 128), F32),
                vmem((cols - 1, 2, width, 128), F32),
                vmem((cols + rows, 1, 128), F32),
                vmem((3, batch), jnp.int32),
                pltpu.SemaphoreType.DMA((cols + 4,)),
                pltpu.SemaphoreType.DMA((4,)),
                pltpu.SemaphoreType.DMA((n_sem,)),
            ],
            compiler_params=pltpu.CompilerParams(collective_id=0, has_side_effects=True),
        )(mask_blk, user_shard.T, item_shard, triples.T)
        out_user, out_item, loss = pl.pallas_call(
            emit,
            name="emit",
            out_shape=(
                jax.ShapeDtypeStruct((emb, ublk), BF16),
                jax.ShapeDtypeStruct((isub, emb), BF16),
                jax.ShapeDtypeStruct((batch // 128, 128), F32),
            ),
        )(out_user, out_item, loss)
        return out_user.T, out_item, loss.reshape(batch)

    return jax.shard_map(
        device_body,
        mesh=mesh,
        in_specs=(P("row", "col"), P(("row", "col"), None), P(("col", "row"), None), P()),
        out_specs=(P(("row", "col"), None), P(("col", "row"), None), P()),
        check_vma=False,
    )
```

```python
import functools
import math

import jax
import jax.numpy as jnp
from jax import lax
from jax.experimental import pallas as pl
from jax.experimental.pallas import tpu as pltpu
from jax.sharding import PartitionSpec as P

LAYERS = 3
SIDE = 4
USER_SPAN = 128
AHEAD = 8
F32 = jnp.float32
BF16 = jnp.bfloat16
NN = (((1,), (0,)), ((), ()))
NT = (((1,), (1,)), ((), ()))
TN = (((0,), (0,)), ((), ()))


def mm(lhs, rhs, dims=NN):
    return lax.dot_general(lhs, rhs, dims, preferred_element_type=F32)


def identity(size):
    at_row = lax.broadcasted_iota(jnp.int32, (size, size), 0)
    at_col = lax.broadcasted_iota(jnp.int32, (size, size), 1)
    return jnp.where(at_row == at_col, 1.0, 0.0).astype(BF16)


def kernel(
    rows, mask_hbm, eu_hbm, ei_hbm, tri_hbm, ou_ref, oi_ref, loss_ref,
    mask_buf, adj, ua, ub, pa, pb, ra, rb, sa, sb, qa, qb, utot,
    i_nat, i_pan, pi, ri, itot, du_own, du_y, du_ysum, du_z, du_inv, di_own, di_got,
    oi_nat, oh, apick, ihit, ppa, ppb, pra, prb, psa, psb, pqa, pqb, upick,
    vx, vxr, px, pxr, tiny,
    tri_ref, load_sem, send_sem, recv_sem,
):
    r = lax.axis_index("row")
    c = lax.axis_index("col")
    z, y = lax.div(c, SIDE), lax.rem(c, SIDE)
    half = ua.shape[-2]
    emb = 2 * half
    ublk = ua.shape[-1]
    chunks = SIDE * SIDE
    iblk = adj.shape[-1]
    isub = i_nat.shape[1]
    tiles, tw = apick.shape[:2]

    def plus(base, k, n):
        return lax.rem(base + k, n)

    def y_dev(k):
        return {"col": z * SIDE + plus(y, k, SIDE)}

    def z_dev(k):
        return {"col": plus(z, k, SIDE) * SIDE + y}

    def r_dev(k):
        return {"row": plus(r, k, rows)}

    def c_dev(k):
        return {"col": plus(c, k, chunks)}

    sides = (2, 1, 3)
    plane = tuple(range(1, chunks))
    ring = tuple(range(1, rows))
    count = [0]
    sent = [], [], []

    def sems(n):
        first = count[0]
        count[0] += n
        return first

    def copy(src, dst, sem, dev, out=0):
        return pltpu.make_async_remote_copy(
            src_ref=src, dst_ref=dst, send_sem=send_sem.at[out], recv_sem=recv_sem.at[sem],
            device_id=dev, device_id_type=pl.DeviceIdType.MESH)

    def push(sem, src, dst, dev):
        size = math.prod(src.shape) * src.dtype.itemsize
        kind = 0 if size % (32 * iblk) == 0 else 1 if size % 4096 == 0 else 2
        copy(src, dst, sem, dev, kind).start()
        sent[kind].append(size)

    def arrive(sem, whole):
        copy(whole, whole, sem, {"row": r}).wait_recv()

    loads = [pltpu.make_async_copy(mask_hbm.at[pl.ds(j * ublk, ublk)], mask_buf.at[j], load_sem.at[j % AHEAD]) for j in range(chunks)]
    for one in loads[:AHEAD]:
        one.start()
    smalls = [
        pltpu.make_async_copy(eu_hbm.at[pl.ds(0, half)], ua.at[0, y, z], load_sem.at[AHEAD]),
        pltpu.make_async_copy(eu_hbm.at[pl.ds(half, half)], ub.at[0, z, y], load_sem.at[AHEAD + 1]),
        pltpu.make_async_copy(ei_hbm, i_nat.at[r], load_sem.at[AHEAD + 2]),
        pltpu.make_async_copy(tri_hbm, tri_ref, load_sem.at[AHEAD + 3]),
    ]
    for one in smalls:
        one.start()

    barrier = pltpu.get_barrier_semaphore()
    for k in sides:
        pl.semaphore_signal(barrier, inc=1, device_id=y_dev(k), device_id_type=pl.DeviceIdType.MESH)
        pl.semaphore_signal(barrier, inc=1, device_id=z_dev(k), device_id_type=pl.DeviceIdType.MESH)
    for k in ring:
        pl.semaphore_signal(barrier, inc=1, device_id=r_dev(k), device_id_type=pl.DeviceIdType.MESH)

    eye = identity(emb)
    ug = [sems(10) for _ in range(LAYERS)]

    def user_gather_start(l):
        for k in sides:
            push(ug[l] + k, ua.at[l, y, z], ua.at[l, y, z], z_dev(k))
            push(ug[l] + 4 + k, ub.at[l, z, y], ub.at[l, z, y], y_dev(k))
        for k in sides:
            push(ug[l] + 8, ua.at[l, y, z], ua.at[l, y, z], y_dev(k))
            push(ug[l] + 9, ub.at[l, z, y], ub.at[l, z, y], z_dev(k))

    def user_gather_fwd(l):
        for q in (1, 3, 2):
            at_z, at_y = plus(z, SIDE - q, SIDE), plus(y, SIDE - q, SIDE)
            arrive(ug[l] + q, ua.at[l, y, at_z])
            for k in sides:
                push(ug[l] + 8, ua.at[l, y, at_z], ua.at[l, y, at_z], y_dev(k))
            arrive(ug[l] + 4 + q, ub.at[l, z, at_y])
            for k in sides:
                push(ug[l] + 9, ub.at[l, z, at_y], ub.at[l, z, at_y], z_dev(k))

    def user_gather_end(l):
        arrive(ug[l] + 8, ua.at[l, pl.ds(0, SIDE - 1)])
        arrive(ug[l] + 9, ub.at[l, pl.ds(0, SIDE - 1)])

    us = [sems(10) for _ in range(LAYERS + 1)]
    groups = ((2, 1), (3, 1), (1, 1), (0, 1))
    order = (
        ((2, 2), (2, 3), (3, 2), (2, 1), (1, 2)),
        ((3, 3), (3, 1), (1, 3)),
        ((1, 1),),
        ((0, 1), (0, 2), (0, 3), (1, 0), (2, 0), (3, 0)),
        ((0, 0),),
    )

    def layer_bufs(l):
        return us[l], [ref.at[l] for ref in (pa, pb, ra, rb, sa, sb, qa, qb)]

    pick_bufs = us[LAYERS], [ppa, ppb, pra, prb, psa, psb, pqa, pqb]

    def sum_send(bufs, g):
        sem, (own_a, own_b, got_a, got_b) = bufs[0], bufs[1][:4]
        part = pl.ds(*groups[g])
        for k in sides:
            push(sem + g, own_a.at[plus(y, k, SIDE), part], got_a.at[k - 1, part], y_dev(k))
            push(sem + 5 + g, own_b.at[plus(z, k, SIDE), part], got_b.at[k - 1, part], z_dev(k))

    def sum_1(bufs):
        sem, (own_a, own_b, got_a, got_b, mid_a, mid_b, end_a, end_b) = bufs
        for g, (lo, n) in enumerate(groups):
            part = pl.ds(lo, n)
            arrive(sem + g, got_a.at[:, part])
            arrive(sem + 5 + g, got_b.at[:, part])
            for j in range(lo, lo + n):
                mid_a[j] = own_a[y, j] + got_a[0, j] + got_a[1, j] + got_a[2, j]
                mid_b[j] = own_b[z, j] + got_b[0, j] + got_b[1, j] + got_b[2, j]
            for k in range(lo, lo + n):
                if k:
                    push(sem + 4, mid_a.at[k], end_a.at[k - 1], z_dev(k))
                    push(sem + 9, mid_b.at[k], end_b.at[k - 1], y_dev(k))

    def sum_2(bufs):
        sem, (mid_a, mid_b, end_a, end_b) = bufs[0], bufs[1][4:]
        arrive(sem + 4, end_a)
        arrive(sem + 9, end_b)
        next_a = (mid_a[0] + end_a[0] + end_a[1] + end_a[2]).astype(BF16)
        next_b = (mid_b[0] + end_b[0] + end_b[1] + end_b[2]).astype(BF16)
        return next_a, next_b

    def user_product(l, panel, g, build=None):
        for dz, dy in order[g]:
            jz, jy = plus(z, dz, SIDE), plus(y, dy, SIDE)
            j = jz * SIDE + jy
            blk = adj[j] if build is None else build(j)
            part = mm(panel, blk, NT)
            pa[l, jy, dz] = part[:half]
            pb[l, jz, dy] = part[half:]

    def user_sum_send(l, g):
        sum_send(layer_bufs(l), g)

    def user_sum_1(l):
        sum_1(layer_bufs(l))

    def user_sum_2(l):
        next_a, next_b = sum_2(layer_bufs(l))
        utot[pl.ds(0, half)] += next_a.astype(F32)
        utot[pl.ds(half, half)] += next_b.astype(F32)
        return next_a, next_b

    def user_keep(l, next_a, next_b):
        ua[l, y, z] = next_a
        ub[l, z, y] = next_b

    ig = [sems(1) for _ in range(LAYERS + 1)]
    isum = [sems(1) for _ in range(LAYERS)]

    def item_product(l):
        def step(j, acc):
            jz, jy = lax.div(j, SIDE), lax.rem(j, SIDE)
            lhs = jnp.concatenate([ua[l, jy, jz], ub[l, jz, jy]], axis=0)
            return acc + mm(lhs, adj[j])
        acc = lax.fori_loop(0, chunks, step, jnp.zeros((emb, iblk), F32), unroll=4)
        pi[l] = acc.reshape(pi.shape[1:])
        for k in ring:
            push(isum[l], pi.at[l, plus(r, k, rows)], ri.at[l, k - 1], r_dev(k))

    def item_gather(l, mine):
        i_pan[l, r] = mine
        for k in ring:
            push(ig[l], i_pan.at[l, r], i_pan.at[l, r], r_dev(k))

    def item_sum(l):
        arrive(isum[l], ri.at[l])
        acc = pi[l, r]
        for k in ring:
            acc = acc + ri[l, k - 1]
        mine = acc.astype(BF16).astype(F32)
        itot[...] += mine
        return mine

    def item_panel(l):
        arrive(ig[l], i_pan.at[l, pl.ds(0, rows - 1)])
        return i_pan[l].reshape(emb, iblk).astype(BF16)

    def pick_rows(t):
        ids = (tri_ref[0:1, t * tw:(t + 1) * tw] - r * (chunks * ublk)).astype(F32)
        ids = jnp.broadcast_to(ids, (8, tw)).T[:, :1]
        lane = lax.broadcasted_iota(jnp.int32, (tw, ublk), 1).astype(F32)
        for j in range(chunks):
            oh[:, j * ublk:(j + 1) * ublk] = jnp.where(ids - j * ublk == lane, 1.0, 0.0).astype(BF16)
        rows_got = mm(oh[...], adj[...].reshape(chunks * ublk, iblk))
        apick[t] = rows_got.astype(BF16)

    def pick_product(panel):
        for t in range(tiles):
            part = mm(panel, apick[t], NT)
            for h in range(tw // 128):
                jz, jy = divmod(t * (tw // 128) + h, SIDE)
                cut = part[:, h * 128:(h + 1) * 128]
                ppa[jy, plus(jz + SIDE, -z, SIDE)] = cut[:half]
                ppb[jz, plus(jy + SIDE, -y, SIDE)] = cut[half:]
        for g in range(len(groups)):
            sum_send(pick_bufs, g)

    def pick_users(l):
        local = tri_ref[0:1, pl.ds(pl.multiple_of(c * 128, 128), 128)] - r * (chunks * ublk)
        blk_id = jnp.where(local < 0, -1, lax.div(local, ublk))
        at_row = lax.broadcasted_iota(jnp.int32, (ublk, 128), 0)
        hit = jnp.where(local - blk_id * ublk == at_row, 1.0, 0.0).astype(BF16)
        got_a = mm(ua[l].reshape(chunks * half, ublk), hit)
        got_b = mm(ub[l].reshape(chunks * half, ublk), hit)
        vec_a = jnp.zeros((half, 128), F32)
        vec_b = jnp.zeros((half, 128), F32)
        for jz in range(SIDE):
            for jy in range(SIDE):
                here = blk_id == jz * SIDE + jy
                ja = (jy * SIDE + jz) * half
                jb = (jz * SIDE + jy) * half
                vec_a = vec_a + jnp.where(here, got_a[ja:ja + half], 0.0)
                vec_b = vec_b + jnp.where(here, got_b[jb:jb + half], 0.0)
        if l:
            vec_a = upick[pl.ds(0, half)] + vec_a
            vec_b = upick[pl.ds(half, half)] + vec_b
        upick[pl.ds(0, half)] = vec_a
        upick[pl.ds(half, half)] = vec_b

    def item_hits():
        at_row = lax.broadcasted_iota(jnp.int32, (ublk, tw), 0)
        for which in (1, 2):
            for t in range(tiles):
                local = tri_ref[which:which + 1, t * tw:(t + 1) * tw] - c * iblk
                hit = lax.rem(local + USER_SPAN * ublk, ublk) == at_row
                ihit[which - 1, t] = jnp.where(hit, 1.0, 0.0).astype(BF16)

    def pick_items(mine):
        lhs = jnp.concatenate([mine[:, h * ublk:(h + 1) * ublk] for h in range(iblk // ublk)], axis=0).astype(BF16)
        width = mine.shape[0]
        for which in (1, 2):
            for t in range(tiles):
                local = tri_ref[which:which + 1, t * tw:(t + 1) * tw] - c * iblk
                got = mm(lhs, ihit[which - 1, t])
                vec = jnp.zeros((width, tw), F32)
                for h in range(iblk // ublk):
                    here = (local >= h * ublk) & (local < (h + 1) * ublk)
                    vec = vec + jnp.where(here, got[h * width:(h + 1) * width], 0.0)
                for h in range(tw // 128):
                    px[t * (tw // 128) + h, which - 1] = vec[:, h * 128:(h + 1) * 128]

    du_s, dz_s, di_s = sems(1), sems(1), sems(1)
    ones = jnp.ones((8, iblk), BF16)
    di_acc = jnp.zeros((8, iblk), jnp.int32)
    for j in range(chunks):
        loads[j].wait()
        if j + AHEAD < chunks:
            loads[j + AHEAD].start()
        blk = mask_buf[j]
        di_acc = di_acc + jnp.sum(blk.reshape(ublk // 8, 8, iblk), axis=0)
        blk = blk.astype(F32).astype(BF16)
        adj[j] = blk
        du_own[pl.ds(j, 1), :] = mm(ones, blk, NT)[:1]
    di_own[...] = di_acc.astype(F32)
    for one in smalls:
        one.wait()
    pl.semaphore_wait(barrier, 2 * len(sides) + len(ring))
    for k in sides:
        push(du_s, du_own, du_y.at[k - 1], y_dev(k))
    for k in ring:
        push(di_s, di_own, di_got.at[k - 1], r_dev(k))
    user_gather_start(0)
    utot[pl.ds(0, half)] = ua[0, y, z].astype(F32)
    utot[pl.ds(half, half)] = ub[0, z, y].astype(F32)
    for k in ring:
        copy(i_nat.at[r], i_nat.at[r], ig[0], r_dev(k), 3).start()
    arrive(du_s, du_y)
    du_ysum[...] = du_own[...] + du_y[0] + du_y[1] + du_y[2]
    for k in sides:
        push(dz_s, du_ysum, du_z.at[k - 1], z_dev(k))
    arrive(ig[0], i_nat.at[pl.ds(0, rows - 1)])
    item0 = mm(eye, i_nat[...].reshape(iblk, emb), NT)
    i_pan[0] = item0.reshape(i_pan.shape[1:])
    itot[...] = i_pan[0, r]
    item0 = item0.astype(BF16)
    user_gather_fwd(0)
    arrive(di_s, di_got)
    deg_i = di_own[...]
    for k in ring:
        deg_i = deg_i + di_got[k - 1]
    deg_i = jnp.sum(deg_i, axis=0, keepdims=True)
    scale_i = lax.rsqrt(jnp.maximum(deg_i, 1.0))
    arrive(dz_s, du_z)
    deg_u = du_ysum[...] + du_z[0] + du_z[1] + du_z[2]
    du_inv[...] = lax.rsqrt(jnp.maximum(deg_u, 1.0))

    def build(j):
        scale_u = jnp.broadcast_to(du_inv[pl.ds(j, 1), :], (8, ublk)).T[:, :1]
        blk = adj[j] * (scale_u * scale_i).astype(BF16)
        adj[j] = blk
        return blk

    s_u, s_i, s_m, s_l = sems(1), sems(1), sems(1), sems(1)
    user_product(0, item0, 0, build)
    user_sum_send(0, 0)
    user_product(0, item0, 1, build)
    user_sum_send(0, 1)
    user_product(0, item0, 2, build)
    user_sum_send(0, 2)
    user_product(0, item0, 3, build)
    user_sum_send(0, 3)
    user_product(0, item0, 4, build)
    user_gather_end(0)
    item_product(0)
    pick_rows(0)
    mine = item_sum(0)
    item_gather(1, mine)
    pick_rows(1)
    user_sum_1(0)
    panel1 = item_panel(1)
    user_product(1, panel1, 0)
    user_sum_send(1, 0)
    user_product(1, panel1, 1)
    user_sum_send(1, 1)
    user_product(1, panel1, 2)
    user_product(1, panel1, 3)
    user_product(1, panel1, 4)
    user_keep(1, *user_sum_2(0))
    user_gather_start(1)
    user_sum_send(1, 2)
    pick_rows(2)
    user_gather_fwd(1)
    user_sum_send(1, 3)
    pick_rows(3)
    pick_rows(4)
    pick_rows(5)
    user_sum_1(1)
    user_gather_end(1)
    item_product(1)
    item_hits()
    pick_users(0)
    pick_users(1)
    user_keep(2, *user_sum_2(1))
    user_gather_start(2)
    mine = item_sum(1)
    item_gather(2, mine)
    user_gather_fwd(2)
    pick_rows(6)
    pick_rows(7)
    panel2 = item_panel(2)
    pick_product(panel2)
    user_gather_end(2)
    item_product(2)
    pick_users(2)
    sum_1(pick_bufs)
    item_sum(2)
    out_slice = (itot[...] / (LAYERS + 1)).astype(BF16).astype(F32)
    pick_items(out_slice)
    for k in plane:
        push(s_i, px.at[plus(c, k, chunks)], pxr.at[k - 1], c_dev(k))
    vec_a, vec_b = sum_2(pick_bufs)
    vec_a = ((upick[pl.ds(0, half)] + vec_a.astype(F32)) / (LAYERS + 1)).astype(BF16).astype(F32)
    vec_b = ((upick[pl.ds(half, half)] + vec_b.astype(F32)) / (LAYERS + 1)).astype(BF16).astype(F32)
    vx[...] = jnp.concatenate([vec_a, vec_b], axis=0).reshape(vx.shape)
    for k in ring:
        push(s_u, vx.at[plus(r, k, rows)], vxr.at[k - 1], r_dev(k))
    user_product(2, panel2, 0)
    user_sum_send(2, 0)
    user_product(2, panel2, 1)
    user_sum_send(2, 1)
    user_product(2, panel2, 2)
    user_sum_send(2, 2)
    user_product(2, panel2, 3)
    user_sum_send(2, 3)
    user_product(2, panel2, 4)
    item_gather(3, out_slice)
    arrive(s_u, vxr)
    vec_u = vx[r]
    for k in ring:
        vec_u = vec_u + vxr[k - 1]
    arrive(s_i, pxr)
    vec_p, vec_n = px[c, 0], px[c, 1]
    for k in plane:
        vec_p = vec_p + pxr[k - 1, 0]
        vec_n = vec_n + pxr[k - 1, 1]
    part = jnp.sum(vec_u * vec_p, axis=0, keepdims=True) - jnp.sum(vec_u * vec_n, axis=0, keepdims=True)
    tiny[chunks + r] = part
    for k in ring:
        push(s_m, tiny.at[chunks + r], tiny.at[chunks + r], r_dev(k))
    arrive(s_m, tiny.at[pl.ds(chunks, rows - 1)])
    neg_x = -tiny[chunks]
    for k in range(1, rows):
        neg_x = neg_x - tiny[chunks + k]
    tiny[c] = jnp.maximum(neg_x, 0.0) + jnp.log1p(jnp.exp(-jnp.abs(neg_x)))
    for k in plane:
        push(s_l, tiny.at[c], tiny.at[c], c_dev(k))
    user_sum_1(2)
    user_sum_2(2)
    ou_ref[...] = (utot[...] / (LAYERS + 1)).astype(BF16)
    out_it = item_panel(3)
    oi_nat[...] = mm(out_it, eye, TN).reshape(oi_nat.shape)
    oi_ref[...] = oi_nat[r].astype(BF16)
    arrive(s_l, tiny.at[pl.ds(0, chunks - 1)])
    for k in range(chunks):
        loss_ref[pl.ds(k, 1), :] = tiny[k]

    span = mask_buf.reshape(chunks * ublk, iblk)
    ends = (
        span.at[pl.ds(0, sum(sent[0]) // (4 * iblk))],
        span.at[pl.ds(0, sum(sent[1]) // 512), pl.ds(0, 128)],
        tiny.at[pl.ds(0, sum(sent[2]) // 512)],
        i_nat.at[pl.ds(0, rows - 1)],
    )
    for kind, whole in enumerate(ends):
        copy(whole, whole, 0, {"row": r}, kind).wait_send()
    assert count[0] == recv_sem.shape[0]
    assert all(size % 512 == 0 for size in sent[2])


def emit(ou_in, oi_in, loss_in, ou_ref, oi_ref, loss_ref):
    ou_ref[...] = ou_in[...]
    oi_ref[...] = oi_in[...]
    loss_ref[...] = loss_in[...]


def solution(mesh):
    rows = mesh.shape["row"]
    cols = mesh.shape["col"]

    def device_body(mask_blk, user_shard, item_shard, triples):
        ublk, emb = user_shard.shape
        isub = item_shard.shape[0]
        iblk = mask_blk.shape[1]
        batch = triples.shape[0]
        half = emb // 2
        width = emb // rows
        tw = 256
        tiles = batch // tw
        n_sem = 10 * LAYERS + 10 * (LAYERS + 1) + 2 * LAYERS + 1 + 3 + 4
        vmem = pltpu.VMEM
        out_user, out_item, loss = pl.pallas_call(
            functools.partial(kernel, rows),
            name="lightgcn",
            out_shape=(
                jax.ShapeDtypeStruct((emb, ublk), BF16),
                jax.ShapeDtypeStruct((isub, emb), BF16),
                jax.ShapeDtypeStruct((batch // 128, 128), F32),
            ),
            in_specs=[pl.BlockSpec(memory_space=pl.ANY)] * 4,
            out_specs=tuple([pl.BlockSpec(memory_space=vmem)] * 3),
            scratch_shapes=[
                vmem((cols, ublk, iblk), jnp.int32),
                vmem((cols, ublk, iblk), BF16),
                vmem((LAYERS, SIDE, SIDE, half, ublk), BF16),
                vmem((LAYERS, SIDE, SIDE, half, ublk), BF16),
                vmem((LAYERS, SIDE, SIDE, half, ublk), F32),
                vmem((LAYERS, SIDE, SIDE, half, ublk), F32),
                vmem((LAYERS, 3, SIDE, half, ublk), F32),
                vmem((LAYERS, 3, SIDE, half, ublk), F32),
                vmem((LAYERS, SIDE, half, ublk), F32),
                vmem((LAYERS, SIDE, half, ublk), F32),
                vmem((LAYERS, 3, half, ublk), F32),
                vmem((LAYERS, 3, half, ublk), F32),
                vmem((emb, ublk), F32),
                vmem((rows, isub, emb), BF16),
                vmem((LAYERS + 1, rows, width, iblk), F32),
                vmem((LAYERS, rows, width, iblk), F32),
                vmem((LAYERS, rows - 1, width, iblk), F32),
                vmem((width, iblk), F32),
                vmem((cols, ublk), F32),
                vmem((3, cols, ublk), F32),
                vmem((cols, ublk), F32),
                vmem((3, cols, ublk), F32),
                vmem((cols, ublk), F32),
                vmem((8, iblk), F32),
                vmem((rows - 1, 8, iblk), F32),
                vmem((rows, isub, emb), F32),
                vmem((tw, cols * ublk), BF16),
                vmem((tiles, tw, iblk), BF16),
                vmem((2, tiles, ublk, tw), BF16),
                vmem((SIDE, SIDE, half, 128), F32),
                vmem((SIDE, SIDE, half, 128), F32),
                vmem((3, SIDE, half, 128), F32),
                vmem((3, SIDE, half, 128), F32),
                vmem((SIDE, half, 128), F32),
                vmem((SIDE, half, 128), F32),
                vmem((3, half, 128), F32),
                vmem((3, half, 128), F32),
                vmem((emb, 128), F32),
                vmem((rows, width, 128), F32),
                vmem((rows - 1, width, 128), F32),
                vmem((cols, 2, width, 128), F32),
                vmem((cols - 1, 2, width, 128), F32),
                vmem((cols + rows, 1, 128), F32),
                vmem((3, batch), jnp.int32),
                pltpu.SemaphoreType.DMA((AHEAD + 4,)),
                pltpu.SemaphoreType.DMA((4,)),
                pltpu.SemaphoreType.DMA((n_sem,)),
            ],
            compiler_params=pltpu.CompilerParams(collective_id=0, has_side_effects=True),
        )(mask_blk, user_shard.T, item_shard, triples.T)
        out_user, out_item, loss = pl.pallas_call(
            emit,
            name="emit",
            out_shape=(
                jax.ShapeDtypeStruct((emb, ublk), BF16),
                jax.ShapeDtypeStruct((isub, emb), BF16),
                jax.ShapeDtypeStruct((batch // 128, 128), F32),
            ),
        )(out_user, out_item, loss)
        return out_user.T, out_item, loss.reshape(batch)

    return jax.shard_map(
        device_body,
        mesh=mesh,
        in_specs=(P("row", "col"), P(("row", "col"), None), P(("col", "row"), None), P()),
        out_specs=(P(("row", "col"), None), P(("col", "row"), None), P()),
        check_vma=False,
    )
```

```python
import functools
import math

import jax
import jax.numpy as jnp
from jax import lax
from jax.experimental import pallas as pl
from jax.experimental.pallas import tpu as pltpu
from jax.sharding import PartitionSpec as P

LAYERS = 3
SIDE = 4
USER_SPAN = 128
AHEAD = 8
F32 = jnp.float32
BF16 = jnp.bfloat16
NN = (((1,), (0,)), ((), ()))
NT = (((1,), (1,)), ((), ()))
TN = (((0,), (0,)), ((), ()))


def mm(lhs, rhs, dims=NN):
    return lax.dot_general(lhs, rhs, dims, preferred_element_type=F32)


def identity(size):
    at_row = lax.broadcasted_iota(jnp.int32, (size, size), 0)
    at_col = lax.broadcasted_iota(jnp.int32, (size, size), 1)
    return jnp.where(at_row == at_col, 1.0, 0.0).astype(BF16)


def kernel(
    rows, mask_hbm, eu_hbm, ei_hbm, tri_hbm, ou_ref, oi_ref, loss_ref,
    mask_buf, adj, ua, ub, pa, pb, ra, rb, sa, sb, qa, qb, utot,
    i_nat, i_pan, pi, ri, itot, du_own, du_y, du_ysum, du_z, du_inv, di_own, di_got,
    oi_nat, oh, apick, ihit, ppa, ppb, pra, prb, psa, psb, pqa, pqb, upick,
    vx, vxr, px, pxr, tiny,
    tri_ref, load_sem, send_sem, recv_sem,
):
    r = lax.axis_index("row")
    c = lax.axis_index("col")
    z, y = lax.div(c, SIDE), lax.rem(c, SIDE)
    half = ua.shape[-2]
    emb = 2 * half
    ublk = ua.shape[-1]
    chunks = SIDE * SIDE
    iblk = adj.shape[-1]
    isub = i_nat.shape[1]
    tiles, tw = apick.shape[:2]

    def plus(base, k, n):
        return lax.rem(base + k, n)

    def y_dev(k):
        return {"col": z * SIDE + plus(y, k, SIDE)}

    def z_dev(k):
        return {"col": plus(z, k, SIDE) * SIDE + y}

    def r_dev(k):
        return {"row": plus(r, k, rows)}

    def c_dev(k):
        return {"col": plus(c, k, chunks)}

    sides = (2, 1, 3)
    plane = tuple(range(1, chunks))
    ring = tuple(range(1, rows))
    far_ring = tuple(sorted(ring, key=lambda k: -min(k, rows - k)))
    far_plane = tuple(sorted(plane, key=lambda k: -min(k % SIDE, SIDE - k % SIDE) - min(k // SIDE, SIDE - k // SIDE)))
    count = [0]
    sent = [], [], []

    def sems(n):
        first = count[0]
        count[0] += n
        return first

    def copy(src, dst, sem, dev, out=0):
        return pltpu.make_async_remote_copy(
            src_ref=src, dst_ref=dst, send_sem=send_sem.at[out], recv_sem=recv_sem.at[sem],
            device_id=dev, device_id_type=pl.DeviceIdType.MESH)

    def push(sem, src, dst, dev):
        size = math.prod(src.shape) * src.dtype.itemsize
        kind = 0 if size % (32 * iblk) == 0 else 1 if size % 4096 == 0 else 2
        copy(src, dst, sem, dev, kind).start()
        sent[kind].append(size)

    def arrive(sem, whole):
        copy(whole, whole, sem, {"row": r}).wait_recv()

    loads = [pltpu.make_async_copy(mask_hbm.at[pl.ds(j * ublk, ublk)], mask_buf.at[j], load_sem.at[j % AHEAD]) for j in range(chunks)]
    for one in loads[:AHEAD]:
        one.start()
    smalls = [
        pltpu.make_async_copy(eu_hbm.at[pl.ds(0, half)], ua.at[0, y, z], load_sem.at[AHEAD]),
        pltpu.make_async_copy(eu_hbm.at[pl.ds(half, half)], ub.at[0, z, y], load_sem.at[AHEAD + 1]),
        pltpu.make_async_copy(ei_hbm, i_nat.at[r], load_sem.at[AHEAD + 2]),
        pltpu.make_async_copy(tri_hbm, tri_ref, load_sem.at[AHEAD + 3]),
    ]
    for one in smalls:
        one.start()

    barrier = pltpu.get_barrier_semaphore()
    for k in sides:
        pl.semaphore_signal(barrier, inc=1, device_id=y_dev(k), device_id_type=pl.DeviceIdType.MESH)
        pl.semaphore_signal(barrier, inc=1, device_id=z_dev(k), device_id_type=pl.DeviceIdType.MESH)
    for k in ring:
        pl.semaphore_signal(barrier, inc=1, device_id=r_dev(k), device_id_type=pl.DeviceIdType.MESH)

    eye = identity(emb)
    ug = [sems(10) for _ in range(LAYERS)]

    def user_gather_start(l):
        for k in sides:
            push(ug[l] + k, ua.at[l, y, z], ua.at[l, y, z], z_dev(k))
            push(ug[l] + 4 + k, ub.at[l, z, y], ub.at[l, z, y], y_dev(k))
        for k in sides:
            push(ug[l] + 8, ua.at[l, y, z], ua.at[l, y, z], y_dev(k))
            push(ug[l] + 9, ub.at[l, z, y], ub.at[l, z, y], z_dev(k))

    def user_gather_fwd(l):
        for q in (1, 3, 2):
            at_z, at_y = plus(z, SIDE - q, SIDE), plus(y, SIDE - q, SIDE)
            arrive(ug[l] + q, ua.at[l, y, at_z])
            for k in sides:
                push(ug[l] + 8, ua.at[l, y, at_z], ua.at[l, y, at_z], y_dev(k))
            arrive(ug[l] + 4 + q, ub.at[l, z, at_y])
            for k in sides:
                push(ug[l] + 9, ub.at[l, z, at_y], ub.at[l, z, at_y], z_dev(k))

    def user_gather_end(l):
        arrive(ug[l] + 8, ua.at[l, pl.ds(0, SIDE - 1)])
        arrive(ug[l] + 9, ub.at[l, pl.ds(0, SIDE - 1)])

    us = [sems(10) for _ in range(LAYERS + 1)]
    groups = ((2, 1), (3, 1), (1, 1), (0, 1))
    order = (
        ((2, 2), (2, 3), (3, 2), (2, 1), (1, 2)),
        ((3, 3), (3, 1), (1, 3)),
        ((1, 1),),
        ((0, 1), (0, 2), (0, 3), (1, 0), (2, 0), (3, 0)),
        ((0, 0),),
    )

    def layer_bufs(l):
        return us[l], [ref.at[l] for ref in (pa, pb, ra, rb, sa, sb, qa, qb)]

    pick_bufs = us[LAYERS], [ppa, ppb, pra, prb, psa, psb, pqa, pqb]

    def sum_send(bufs, g):
        sem, (own_a, own_b, got_a, got_b) = bufs[0], bufs[1][:4]
        part = pl.ds(*groups[g])
        for k in sides:
            push(sem + g, own_a.at[plus(y, k, SIDE), part], got_a.at[k - 1, part], y_dev(k))
            push(sem + 5 + g, own_b.at[plus(z, k, SIDE), part], got_b.at[k - 1, part], z_dev(k))

    def sum_1(bufs):
        sem, (own_a, own_b, got_a, got_b, mid_a, mid_b, end_a, end_b) = bufs
        for g, (lo, n) in enumerate(groups):
            part = pl.ds(lo, n)
            arrive(sem + g, got_a.at[:, part])
            arrive(sem + 5 + g, got_b.at[:, part])
            for j in range(lo, lo + n):
                mid_a[j] = own_a[y, j] + got_a[0, j] + got_a[1, j] + got_a[2, j]
                mid_b[j] = own_b[z, j] + got_b[0, j] + got_b[1, j] + got_b[2, j]
            for k in range(lo, lo + n):
                if k:
                    push(sem + 4, mid_a.at[k], end_a.at[k - 1], z_dev(k))
                    push(sem + 9, mid_b.at[k], end_b.at[k - 1], y_dev(k))

    def sum_2(bufs):
        sem, (mid_a, mid_b, end_a, end_b) = bufs[0], bufs[1][4:]
        arrive(sem + 4, end_a)
        arrive(sem + 9, end_b)
        next_a = (mid_a[0] + end_a[0] + end_a[1] + end_a[2]).astype(BF16)
        next_b = (mid_b[0] + end_b[0] + end_b[1] + end_b[2]).astype(BF16)
        return next_a, next_b

    def user_product(l, panel, g, build=None):
        for dz, dy in order[g]:
            jz, jy = plus(z, dz, SIDE), plus(y, dy, SIDE)
            j = jz * SIDE + jy
            blk = adj[j] if build is None else build(j)
            part = mm(panel, blk, NT)
            pa[l, jy, dz] = part[:half]
            pb[l, jz, dy] = part[half:]

    def user_sum_send(l, g):
        sum_send(layer_bufs(l), g)

    def user_sum_1(l):
        sum_1(layer_bufs(l))

    def user_sum_2(l):
        next_a, next_b = sum_2(layer_bufs(l))
        utot[pl.ds(0, half)] += next_a.astype(F32)
        utot[pl.ds(half, half)] += next_b.astype(F32)
        return next_a, next_b

    def user_keep(l, next_a, next_b):
        ua[l, y, z] = next_a
        ub[l, z, y] = next_b

    ig = [sems(1) for _ in range(LAYERS + 1)]
    isum = [sems(1) for _ in range(LAYERS)]

    def item_product(l):
        def step(j, acc):
            jz, jy = lax.div(j, SIDE), lax.rem(j, SIDE)
            lhs = jnp.concatenate([ua[l, jy, jz], ub[l, jz, jy]], axis=0)
            return acc + mm(lhs, adj[j])
        acc = lax.fori_loop(0, chunks, step, jnp.zeros((emb, iblk), F32), unroll=4)
        pi[l] = acc.reshape(pi.shape[1:])
        for k in far_ring:
            push(isum[l], pi.at[l, plus(r, k, rows)], ri.at[l, k - 1], r_dev(k))

    def item_gather(l, mine):
        i_pan[l, r] = mine
        for k in far_ring:
            push(ig[l], i_pan.at[l, r], i_pan.at[l, r], r_dev(k))

    def item_sum(l):
        arrive(isum[l], ri.at[l])
        acc = pi[l, r]
        for k in ring:
            acc = acc + ri[l, k - 1]
        mine = acc.astype(BF16).astype(F32)
        itot[...] += mine
        return mine

    def item_panel(l):
        arrive(ig[l], i_pan.at[l, pl.ds(0, rows - 1)])
        return i_pan[l].reshape(emb, iblk).astype(BF16)

    def pick_rows(t):
        ids = (tri_ref[0:1, t * tw:(t + 1) * tw] - r * (chunks * ublk)).astype(F32)
        ids = jnp.broadcast_to(ids, (8, tw)).T[:, :1]
        lane = lax.broadcasted_iota(jnp.int32, (tw, ublk), 1).astype(F32)
        for j in range(chunks):
            oh[:, j * ublk:(j + 1) * ublk] = jnp.where(ids - j * ublk == lane, 1.0, 0.0).astype(BF16)
        rows_got = mm(oh[...], adj[...].reshape(chunks * ublk, iblk))
        apick[t] = rows_got.astype(BF16)

    def pick_product(panel):
        for t in range(tiles):
            part = mm(panel, apick[t], NT)
            for h in range(tw // 128):
                jz, jy = divmod(t * (tw // 128) + h, SIDE)
                cut = part[:, h * 128:(h + 1) * 128]
                ppa[jy, plus(jz + SIDE, -z, SIDE)] = cut[:half]
                ppb[jz, plus(jy + SIDE, -y, SIDE)] = cut[half:]
        for g in range(len(groups)):
            sum_send(pick_bufs, g)

    def pick_users(l):
        local = tri_ref[0:1, pl.ds(pl.multiple_of(c * 128, 128), 128)] - r * (chunks * ublk)
        blk_id = jnp.where(local < 0, -1, lax.div(local, ublk))
        at_row = lax.broadcasted_iota(jnp.int32, (ublk, 128), 0)
        hit = jnp.where(local - blk_id * ublk == at_row, 1.0, 0.0).astype(BF16)
        got_a = mm(ua[l].reshape(chunks * half, ublk), hit)
        got_b = mm(ub[l].reshape(chunks * half, ublk), hit)
        vec_a = jnp.zeros((half, 128), F32)
        vec_b = jnp.zeros((half, 128), F32)
        for jz in range(SIDE):
            for jy in range(SIDE):
                here = blk_id == jz * SIDE + jy
                ja = (jy * SIDE + jz) * half
                jb = (jz * SIDE + jy) * half
                vec_a = vec_a + jnp.where(here, got_a[ja:ja + half], 0.0)
                vec_b = vec_b + jnp.where(here, got_b[jb:jb + half], 0.0)
        if l:
            vec_a = upick[pl.ds(0, half)] + vec_a
            vec_b = upick[pl.ds(half, half)] + vec_b
        upick[pl.ds(0, half)] = vec_a
        upick[pl.ds(half, half)] = vec_b

    def item_hits():
        at_row = lax.broadcasted_iota(jnp.int32, (ublk, tw), 0)
        for which in (1, 2):
            for t in range(tiles):
                local = tri_ref[which:which + 1, t * tw:(t + 1) * tw] - c * iblk
                hit = lax.rem(local + USER_SPAN * ublk, ublk) == at_row
                ihit[which - 1, t] = jnp.where(hit, 1.0, 0.0).astype(BF16)

    def pick_items(mine):
        lhs = jnp.concatenate([mine[:, h * ublk:(h + 1) * ublk] for h in range(iblk // ublk)], axis=0).astype(BF16)
        width = mine.shape[0]
        for which in (1, 2):
            for t in range(tiles):
                local = tri_ref[which:which + 1, t * tw:(t + 1) * tw] - c * iblk
                got = mm(lhs, ihit[which - 1, t])
                vec = jnp.zeros((width, tw), F32)
                for h in range(iblk // ublk):
                    here = (local >= h * ublk) & (local < (h + 1) * ublk)
                    vec = vec + jnp.where(here, got[h * width:(h + 1) * width], 0.0)
                for h in range(tw // 128):
                    px[t * (tw // 128) + h, which - 1] = vec[:, h * 128:(h + 1) * 128]

    du_s, dz_s, di_s = sems(1), sems(1), sems(1)
    ones = jnp.ones((8, iblk), BF16)
    di_acc = jnp.zeros((8, iblk), jnp.int32)
    for j in range(chunks):
        loads[j].wait()
        if j + AHEAD < chunks:
            loads[j + AHEAD].start()
        blk = mask_buf[j]
        di_acc = di_acc + jnp.sum(blk.reshape(ublk // 8, 8, iblk), axis=0)
        blk = blk.astype(F32).astype(BF16)
        adj[j] = blk
        du_own[pl.ds(j, 1), :] = mm(ones, blk, NT)[:1]
    di_own[...] = di_acc.astype(F32)
    for one in smalls:
        one.wait()
    pl.semaphore_wait(barrier, 2 * len(sides) + len(ring))
    for k in sides:
        push(du_s, du_own, du_y.at[k - 1], y_dev(k))
    for k in far_ring:
        push(di_s, di_own, di_got.at[k - 1], r_dev(k))
    user_gather_start(0)
    utot[pl.ds(0, half)] = ua[0, y, z].astype(F32)
    utot[pl.ds(half, half)] = ub[0, z, y].astype(F32)
    for k in far_ring:
        copy(i_nat.at[r], i_nat.at[r], ig[0], r_dev(k), 3).start()
    arrive(du_s, du_y)
    du_ysum[...] = du_own[...] + du_y[0] + du_y[1] + du_y[2]
    for k in sides:
        push(dz_s, du_ysum, du_z.at[k - 1], z_dev(k))
    arrive(ig[0], i_nat.at[pl.ds(0, rows - 1)])
    item0 = mm(eye, i_nat[...].reshape(iblk, emb), NT)
    i_pan[0] = item0.reshape(i_pan.shape[1:])
    itot[...] = i_pan[0, r]
    item0 = item0.astype(BF16)
    user_gather_fwd(0)
    arrive(di_s, di_got)
    deg_i = di_own[...]
    for k in ring:
        deg_i = deg_i + di_got[k - 1]
    deg_i = jnp.sum(deg_i, axis=0, keepdims=True)
    scale_i = lax.rsqrt(jnp.maximum(deg_i, 1.0))
    arrive(dz_s, du_z)
    deg_u = du_ysum[...] + du_z[0] + du_z[1] + du_z[2]
    du_inv[...] = lax.rsqrt(jnp.maximum(deg_u, 1.0))

    def build(j):
        scale_u = jnp.broadcast_to(du_inv[pl.ds(j, 1), :], (8, ublk)).T[:, :1]
        blk = adj[j] * (scale_u * scale_i).astype(BF16)
        adj[j] = blk
        return blk

    s_u, s_i, s_m, s_l = sems(1), sems(1), sems(1), sems(1)
    user_product(0, item0, 0, build)
    user_sum_send(0, 0)
    user_product(0, item0, 1, build)
    user_sum_send(0, 1)
    user_product(0, item0, 2, build)
    user_sum_send(0, 2)
    user_product(0, item0, 3, build)
    user_sum_send(0, 3)
    user_product(0, item0, 4, build)
    user_gather_end(0)
    item_product(0)
    pick_rows(0)
    mine = item_sum(0)
    item_gather(1, mine)
    pick_rows(1)
    user_sum_1(0)
    panel1 = item_panel(1)
    user_product(1, panel1, 0)
    user_sum_send(1, 0)
    user_product(1, panel1, 1)
    user_sum_send(1, 1)
    user_product(1, panel1, 2)
    user_product(1, panel1, 3)
    user_product(1, panel1, 4)
    user_keep(1, *user_sum_2(0))
    user_gather_start(1)
    user_sum_send(1, 2)
    pick_rows(2)
    user_gather_fwd(1)
    user_sum_send(1, 3)
    pick_rows(3)
    pick_rows(4)
    pick_rows(5)
    user_sum_1(1)
    user_gather_end(1)
    item_product(1)
    item_hits()
    pick_users(0)
    pick_users(1)
    user_keep(2, *user_sum_2(1))
    user_gather_start(2)
    mine = item_sum(1)
    item_gather(2, mine)
    user_gather_fwd(2)
    pick_rows(6)
    pick_rows(7)
    panel2 = item_panel(2)
    pick_product(panel2)
    user_gather_end(2)
    item_product(2)
    pick_users(2)
    sum_1(pick_bufs)
    item_sum(2)
    out_slice = (itot[...] / (LAYERS + 1)).astype(BF16).astype(F32)
    pick_items(out_slice)
    for k in far_plane:
        push(s_i, px.at[plus(c, k, chunks)], pxr.at[k - 1], c_dev(k))
    vec_a, vec_b = sum_2(pick_bufs)
    vec_a = ((upick[pl.ds(0, half)] + vec_a.astype(F32)) / (LAYERS + 1)).astype(BF16).astype(F32)
    vec_b = ((upick[pl.ds(half, half)] + vec_b.astype(F32)) / (LAYERS + 1)).astype(BF16).astype(F32)
    vx[...] = jnp.concatenate([vec_a, vec_b], axis=0).reshape(vx.shape)
    for k in far_ring:
        push(s_u, vx.at[plus(r, k, rows)], vxr.at[k - 1], r_dev(k))
    user_product(2, panel2, 0)
    user_sum_send(2, 0)
    user_product(2, panel2, 1)
    user_sum_send(2, 1)
    user_product(2, panel2, 2)
    user_sum_send(2, 2)
    user_product(2, panel2, 3)
    user_sum_send(2, 3)
    user_product(2, panel2, 4)
    item_gather(3, out_slice)
    arrive(s_u, vxr)
    vec_u = vx[r]
    for k in ring:
        vec_u = vec_u + vxr[k - 1]
    arrive(s_i, pxr)
    vec_p, vec_n = px[c, 0], px[c, 1]
    for k in plane:
        vec_p = vec_p + pxr[k - 1, 0]
        vec_n = vec_n + pxr[k - 1, 1]
    part = jnp.sum(vec_u * vec_p, axis=0, keepdims=True) - jnp.sum(vec_u * vec_n, axis=0, keepdims=True)
    tiny[chunks + r] = part
    for k in far_ring:
        push(s_m, tiny.at[chunks + r], tiny.at[chunks + r], r_dev(k))
    arrive(s_m, tiny.at[pl.ds(chunks, rows - 1)])
    neg_x = -tiny[chunks]
    for k in range(1, rows):
        neg_x = neg_x - tiny[chunks + k]
    tiny[c] = jnp.maximum(neg_x, 0.0) + jnp.log1p(jnp.exp(-jnp.abs(neg_x)))
    for k in far_plane:
        push(s_l, tiny.at[c], tiny.at[c], c_dev(k))
    user_sum_1(2)
    user_sum_2(2)
    ou_ref[...] = (utot[...] / (LAYERS + 1)).astype(BF16)
    out_it = item_panel(3)
    oi_nat[...] = mm(out_it, eye, TN).reshape(oi_nat.shape)
    oi_ref[...] = oi_nat[r].astype(BF16)
    arrive(s_l, tiny.at[pl.ds(0, chunks - 1)])
    for k in range(chunks):
        loss_ref[pl.ds(k, 1), :] = tiny[k]

    span = mask_buf.reshape(chunks * ublk, iblk)
    ends = (
        span.at[pl.ds(0, sum(sent[0]) // (4 * iblk))],
        span.at[pl.ds(0, sum(sent[1]) // 512), pl.ds(0, 128)],
        tiny.at[pl.ds(0, sum(sent[2]) // 512)],
        i_nat.at[pl.ds(0, rows - 1)],
    )
    for kind, whole in enumerate(ends):
        copy(whole, whole, 0, {"row": r}, kind).wait_send()
    assert count[0] == recv_sem.shape[0]
    assert all(size % 512 == 0 for size in sent[2])


def emit(ou_in, oi_in, loss_in, ou_ref, oi_ref, loss_ref):
    ou_ref[...] = ou_in[...]
    oi_ref[...] = oi_in[...]
    loss_ref[...] = loss_in[...]


def solution(mesh):
    rows = mesh.shape["row"]
    cols = mesh.shape["col"]

    def device_body(mask_blk, user_shard, item_shard, triples):
        ublk, emb = user_shard.shape
        isub = item_shard.shape[0]
        iblk = mask_blk.shape[1]
        batch = triples.shape[0]
        half = emb // 2
        width = emb // rows
        tw = 256
        tiles = batch // tw
        n_sem = 10 * LAYERS + 10 * (LAYERS + 1) + 2 * LAYERS + 1 + 3 + 4
        vmem = pltpu.VMEM
        out_user, out_item, loss = pl.pallas_call(
            functools.partial(kernel, rows),
            name="lightgcn",
            out_shape=(
                jax.ShapeDtypeStruct((emb, ublk), BF16),
                jax.ShapeDtypeStruct((isub, emb), BF16),
                jax.ShapeDtypeStruct((batch // 128, 128), F32),
            ),
            in_specs=[pl.BlockSpec(memory_space=pl.ANY)] * 4,
            out_specs=tuple([pl.BlockSpec(memory_space=vmem)] * 3),
            scratch_shapes=[
                vmem((cols, ublk, iblk), jnp.int32),
                vmem((cols, ublk, iblk), BF16),
                vmem((LAYERS, SIDE, SIDE, half, ublk), BF16),
                vmem((LAYERS, SIDE, SIDE, half, ublk), BF16),
                vmem((LAYERS, SIDE, SIDE, half, ublk), F32),
                vmem((LAYERS, SIDE, SIDE, half, ublk), F32),
                vmem((LAYERS, 3, SIDE, half, ublk), F32),
                vmem((LAYERS, 3, SIDE, half, ublk), F32),
                vmem((LAYERS, SIDE, half, ublk), F32),
                vmem((LAYERS, SIDE, half, ublk), F32),
                vmem((LAYERS, 3, half, ublk), F32),
                vmem((LAYERS, 3, half, ublk), F32),
                vmem((emb, ublk), F32),
                vmem((rows, isub, emb), BF16),
                vmem((LAYERS + 1, rows, width, iblk), F32),
                vmem((LAYERS, rows, width, iblk), F32),
                vmem((LAYERS, rows - 1, width, iblk), F32),
                vmem((width, iblk), F32),
                vmem((cols, ublk), F32),
                vmem((3, cols, ublk), F32),
                vmem((cols, ublk), F32),
                vmem((3, cols, ublk), F32),
                vmem((cols, ublk), F32),
                vmem((8, iblk), F32),
                vmem((rows - 1, 8, iblk), F32),
                vmem((rows, isub, emb), F32),
                vmem((tw, cols * ublk), BF16),
                vmem((tiles, tw, iblk), BF16),
                vmem((2, tiles, ublk, tw), BF16),
                vmem((SIDE, SIDE, half, 128), F32),
                vmem((SIDE, SIDE, half, 128), F32),
                vmem((3, SIDE, half, 128), F32),
                vmem((3, SIDE, half, 128), F32),
                vmem((SIDE, half, 128), F32),
                vmem((SIDE, half, 128), F32),
                vmem((3, half, 128), F32),
                vmem((3, half, 128), F32),
                vmem((emb, 128), F32),
                vmem((rows, width, 128), F32),
                vmem((rows - 1, width, 128), F32),
                vmem((cols, 2, width, 128), F32),
                vmem((cols - 1, 2, width, 128), F32),
                vmem((cols + rows, 1, 128), F32),
                vmem((3, batch), jnp.int32),
                pltpu.SemaphoreType.DMA((AHEAD + 4,)),
                pltpu.SemaphoreType.DMA((4,)),
                pltpu.SemaphoreType.DMA((n_sem,)),
            ],
            compiler_params=pltpu.CompilerParams(collective_id=0, has_side_effects=True),
        )(mask_blk, user_shard.T, item_shard, triples.T)
        out_user, out_item, loss = pl.pallas_call(
            emit,
            name="emit",
            out_shape=(
                jax.ShapeDtypeStruct((emb, ublk), BF16),
                jax.ShapeDtypeStruct((isub, emb), BF16),
                jax.ShapeDtypeStruct((batch // 128, 128), F32),
            ),
        )(out_user, out_item, loss)
        return out_user.T, out_item, loss.reshape(batch)

    return jax.shard_map(
        device_body,
        mesh=mesh,
        in_specs=(P("row", "col"), P(("row", "col"), None), P(("col", "row"), None), P()),
        out_specs=(P(("row", "col"), None), P(("col", "row"), None), P()),
        check_vma=False,
    )
```

```python
import functools
import math

import jax
import jax.numpy as jnp
from jax import lax
from jax.experimental import pallas as pl
from jax.experimental.pallas import tpu as pltpu
from jax.sharding import PartitionSpec as P

LAYERS = 3
SIDE = 4
USER_SPAN = 128
AHEAD = 8
F32 = jnp.float32
BF16 = jnp.bfloat16
NN = (((1,), (0,)), ((), ()))
NT = (((1,), (1,)), ((), ()))
TN = (((0,), (0,)), ((), ()))


def mm(lhs, rhs, dims=NN):
    return lax.dot_general(lhs, rhs, dims, preferred_element_type=F32)


def identity(size):
    at_row = lax.broadcasted_iota(jnp.int32, (size, size), 0)
    at_col = lax.broadcasted_iota(jnp.int32, (size, size), 1)
    return jnp.where(at_row == at_col, 1.0, 0.0).astype(BF16)


def kernel(
    rows, mask_hbm, eu_hbm, ei_hbm, tri_hbm, ou_ref, oi_ref, loss_ref,
    mask_buf, adj, ua, ub, pa, pb, ra, rb, sa, sb, qa, qb, utot,
    i_nat, i_pan, pi, ri, itot, du_own, du_y, du_ysum, du_z, du_inv, di_own, di_got,
    oi_nat, oh, apick, ihit, ppa, ppb, pra, prb, psa, psb, pqa, pqb, upick,
    vx, vxr, px, pxr, tiny,
    tri_ref, load_sem, send_sem, recv_sem,
):
    r = lax.axis_index("row")
    c = lax.axis_index("col")
    z, y = lax.div(c, SIDE), lax.rem(c, SIDE)
    half = ua.shape[-2]
    emb = 2 * half
    ublk = ua.shape[-1]
    chunks = SIDE * SIDE
    iblk = adj.shape[-1]
    isub = i_nat.shape[1]
    tiles, tw = apick.shape[:2]

    def plus(base, k, n):
        return lax.rem(base + k, n)

    def y_dev(k):
        return {"col": z * SIDE + plus(y, k, SIDE)}

    def z_dev(k):
        return {"col": plus(z, k, SIDE) * SIDE + y}

    def r_dev(k):
        return {"row": plus(r, k, rows)}

    def c_dev(k):
        return {"col": plus(c, k, chunks)}

    sides = (2, 1, 3)
    plane = tuple(range(1, chunks))
    ring = tuple(range(1, rows))
    far_ring = tuple(sorted(ring, key=lambda k: -min(k, rows - k)))
    far_plane = tuple(sorted(plane, key=lambda k: -min(k % SIDE, SIDE - k % SIDE) - min(k // SIDE, SIDE - k // SIDE)))
    count = [0]
    sent = [], [], []

    def sems(n):
        first = count[0]
        count[0] += n
        return first

    def copy(src, dst, sem, dev, out=0):
        return pltpu.make_async_remote_copy(
            src_ref=src, dst_ref=dst, send_sem=send_sem.at[out], recv_sem=recv_sem.at[sem],
            device_id=dev, device_id_type=pl.DeviceIdType.MESH)

    def push(sem, src, dst, dev):
        size = math.prod(src.shape) * src.dtype.itemsize
        kind = 0 if size % (32 * iblk) == 0 else 1 if size % 4096 == 0 else 2
        copy(src, dst, sem, dev, kind).start()
        sent[kind].append(size)

    def arrive(sem, whole):
        copy(whole, whole, sem, {"row": r}).wait_recv()

    loads = [pltpu.make_async_copy(mask_hbm.at[pl.ds(j * ublk, ublk)], mask_buf.at[j], load_sem.at[j % AHEAD]) for j in range(chunks)]
    for one in loads[:AHEAD]:
        one.start()
    smalls = [
        pltpu.make_async_copy(eu_hbm.at[pl.ds(0, half)], ua.at[0, y, z], load_sem.at[AHEAD]),
        pltpu.make_async_copy(eu_hbm.at[pl.ds(half, half)], ub.at[0, z, y], load_sem.at[AHEAD + 1]),
        pltpu.make_async_copy(ei_hbm, i_nat.at[r], load_sem.at[AHEAD + 2]),
        pltpu.make_async_copy(tri_hbm, tri_ref, load_sem.at[AHEAD + 3]),
    ]
    for one in smalls:
        one.start()

    barrier = pltpu.get_barrier_semaphore()
    for k in sides:
        pl.semaphore_signal(barrier, inc=1, device_id=y_dev(k), device_id_type=pl.DeviceIdType.MESH)
        pl.semaphore_signal(barrier, inc=1, device_id=z_dev(k), device_id_type=pl.DeviceIdType.MESH)
    for k in ring:
        pl.semaphore_signal(barrier, inc=1, device_id=r_dev(k), device_id_type=pl.DeviceIdType.MESH)

    eye = identity(emb)
    ug = [sems(10) for _ in range(2)]
    ug.append(ug[0])

    def user_gather_start(l):
        for k in sides:
            push(ug[l] + k, ua.at[l, y, z], ua.at[l, y, z], z_dev(k))
            push(ug[l] + 4 + k, ub.at[l, z, y], ub.at[l, z, y], y_dev(k))
        for k in sides:
            push(ug[l] + 8, ua.at[l, y, z], ua.at[l, y, z], y_dev(k))
            push(ug[l] + 9, ub.at[l, z, y], ub.at[l, z, y], z_dev(k))

    def user_gather_fwd(l):
        for q in (1, 3, 2):
            at_z, at_y = plus(z, SIDE - q, SIDE), plus(y, SIDE - q, SIDE)
            arrive(ug[l] + q, ua.at[l, y, at_z])
            for k in sides:
                push(ug[l] + 8, ua.at[l, y, at_z], ua.at[l, y, at_z], y_dev(k))
            arrive(ug[l] + 4 + q, ub.at[l, z, at_y])
            for k in sides:
                push(ug[l] + 9, ub.at[l, z, at_y], ub.at[l, z, at_y], z_dev(k))

    def user_gather_end(l):
        arrive(ug[l] + 8, ua.at[l, pl.ds(0, SIDE - 1)])
        arrive(ug[l] + 9, ub.at[l, pl.ds(0, SIDE - 1)])

    us = [sems(10) for _ in range(2)]
    us += [us[1], us[0]]
    groups = ((2, 1), (3, 1), (1, 1), (0, 1))
    order = (
        ((2, 2), (2, 3), (3, 2), (2, 1), (1, 2)),
        ((3, 3), (3, 1), (1, 3)),
        ((1, 1),),
        ((0, 1), (0, 2), (0, 3), (1, 0), (2, 0), (3, 0)),
        ((0, 0),),
    )

    def layer_bufs(l):
        return us[l], [ref.at[l] for ref in (pa, pb, ra, rb, sa, sb, qa, qb)]

    pick_bufs = us[LAYERS], [ppa, ppb, pra, prb, psa, psb, pqa, pqb]

    def sum_send(bufs, g):
        sem, (own_a, own_b, got_a, got_b) = bufs[0], bufs[1][:4]
        part = pl.ds(*groups[g])
        for k in sides:
            push(sem + g, own_a.at[plus(y, k, SIDE), part], got_a.at[k - 1, part], y_dev(k))
            push(sem + 5 + g, own_b.at[plus(z, k, SIDE), part], got_b.at[k - 1, part], z_dev(k))

    def sum_1(bufs):
        sem, (own_a, own_b, got_a, got_b, mid_a, mid_b, end_a, end_b) = bufs
        for g, (lo, n) in enumerate(groups):
            part = pl.ds(lo, n)
            arrive(sem + g, got_a.at[:, part])
            arrive(sem + 5 + g, got_b.at[:, part])
            for j in range(lo, lo + n):
                mid_a[j] = own_a[y, j] + got_a[0, j] + got_a[1, j] + got_a[2, j]
                mid_b[j] = own_b[z, j] + got_b[0, j] + got_b[1, j] + got_b[2, j]
            for k in range(lo, lo + n):
                if k:
                    push(sem + 4, mid_a.at[k], end_a.at[k - 1], z_dev(k))
                    push(sem + 9, mid_b.at[k], end_b.at[k - 1], y_dev(k))

    def sum_2(bufs):
        sem, (mid_a, mid_b, end_a, end_b) = bufs[0], bufs[1][4:]
        arrive(sem + 4, end_a)
        arrive(sem + 9, end_b)
        next_a = (mid_a[0] + end_a[0] + end_a[1] + end_a[2]).astype(BF16)
        next_b = (mid_b[0] + end_b[0] + end_b[1] + end_b[2]).astype(BF16)
        return next_a, next_b

    def user_product(l, panel, g, build=None):
        for dz, dy in order[g]:
            jz, jy = plus(z, dz, SIDE), plus(y, dy, SIDE)
            j = jz * SIDE + jy
            blk = adj[j] if build is None else build(j)
            part = mm(panel, blk, NT)
            pa[l, jy, dz] = part[:half]
            pb[l, jz, dy] = part[half:]

    def user_sum_send(l, g):
        sum_send(layer_bufs(l), g)

    def user_sum_1(l):
        sum_1(layer_bufs(l))

    def user_sum_2(l):
        next_a, next_b = sum_2(layer_bufs(l))
        utot[pl.ds(0, half)] += next_a.astype(F32)
        utot[pl.ds(half, half)] += next_b.astype(F32)
        return next_a, next_b

    def user_keep(l, next_a, next_b):
        ua[l, y, z] = next_a
        ub[l, z, y] = next_b

    ig = [sems(1) for _ in range(LAYERS + 1)]
    isum = [sems(1) for _ in range(LAYERS)]

    def item_product(l):
        def step(j, acc):
            jz, jy = lax.div(j, SIDE), lax.rem(j, SIDE)
            lhs = jnp.concatenate([ua[l, jy, jz], ub[l, jz, jy]], axis=0)
            return acc + mm(lhs, adj[j])
        acc = lax.fori_loop(0, chunks, step, jnp.zeros((emb, iblk), F32), unroll=4)
        pi[l] = acc.reshape(pi.shape[1:])
        for k in far_ring:
            push(isum[l], pi.at[l, plus(r, k, rows)], ri.at[l, k - 1], r_dev(k))

    def item_gather(l, mine):
        i_pan[l, r] = mine
        for k in far_ring:
            push(ig[l], i_pan.at[l, r], i_pan.at[l, r], r_dev(k))

    def item_sum(l):
        arrive(isum[l], ri.at[l])
        acc = pi[l, r]
        for k in ring:
            acc = acc + ri[l, k - 1]
        mine = acc.astype(BF16).astype(F32)
        itot[...] += mine
        return mine

    def item_panel(l):
        arrive(ig[l], i_pan.at[l, pl.ds(0, rows - 1)])
        return i_pan[l].reshape(emb, iblk).astype(BF16)

    def pick_rows(t):
        ids = (tri_ref[0:1, t * tw:(t + 1) * tw] - r * (chunks * ublk)).astype(F32)
        ids = jnp.broadcast_to(ids, (8, tw)).T[:, :1]
        lane = lax.broadcasted_iota(jnp.int32, (tw, ublk), 1).astype(F32)
        for j in range(chunks):
            oh[:, j * ublk:(j + 1) * ublk] = jnp.where(ids - j * ublk == lane, 1.0, 0.0).astype(BF16)
        rows_got = mm(oh[...], adj[...].reshape(chunks * ublk, iblk))
        apick[t] = rows_got.astype(BF16)

    def pick_product(panel):
        for t in range(tiles):
            part = mm(panel, apick[t], NT)
            for h in range(tw // 128):
                jz, jy = divmod(t * (tw // 128) + h, SIDE)
                cut = part[:, h * 128:(h + 1) * 128]
                ppa[jy, plus(jz + SIDE, -z, SIDE)] = cut[:half]
                ppb[jz, plus(jy + SIDE, -y, SIDE)] = cut[half:]
        for g in range(len(groups)):
            sum_send(pick_bufs, g)

    def pick_users(l):
        local = tri_ref[0:1, pl.ds(pl.multiple_of(c * 128, 128), 128)] - r * (chunks * ublk)
        blk_id = jnp.where(local < 0, -1, lax.div(local, ublk))
        at_row = lax.broadcasted_iota(jnp.int32, (ublk, 128), 0)
        hit = jnp.where(local - blk_id * ublk == at_row, 1.0, 0.0).astype(BF16)
        got_a = mm(ua[l].reshape(chunks * half, ublk), hit)
        got_b = mm(ub[l].reshape(chunks * half, ublk), hit)
        vec_a = jnp.zeros((half, 128), F32)
        vec_b = jnp.zeros((half, 128), F32)
        for jz in range(SIDE):
            for jy in range(SIDE):
                here = blk_id == jz * SIDE + jy
                ja = (jy * SIDE + jz) * half
                jb = (jz * SIDE + jy) * half
                vec_a = vec_a + jnp.where(here, got_a[ja:ja + half], 0.0)
                vec_b = vec_b + jnp.where(here, got_b[jb:jb + half], 0.0)
        if l:
            vec_a = upick[pl.ds(0, half)] + vec_a
            vec_b = upick[pl.ds(half, half)] + vec_b
        upick[pl.ds(0, half)] = vec_a
        upick[pl.ds(half, half)] = vec_b

    def item_hits():
        at_row = lax.broadcasted_iota(jnp.int32, (ublk, tw), 0)
        for which in (1, 2):
            for t in range(tiles):
                local = tri_ref[which:which + 1, t * tw:(t + 1) * tw] - c * iblk
                hit = lax.rem(local + USER_SPAN * ublk, ublk) == at_row
                ihit[which - 1, t] = jnp.where(hit, 1.0, 0.0).astype(BF16)

    def pick_items(mine):
        lhs = jnp.concatenate([mine[:, h * ublk:(h + 1) * ublk] for h in range(iblk // ublk)], axis=0).astype(BF16)
        width = mine.shape[0]
        for which in (1, 2):
            for t in range(tiles):
                local = tri_ref[which:which + 1, t * tw:(t + 1) * tw] - c * iblk
                got = mm(lhs, ihit[which - 1, t])
                vec = jnp.zeros((width, tw), F32)
                for h in range(iblk // ublk):
                    here = (local >= h * ublk) & (local < (h + 1) * ublk)
                    vec = vec + jnp.where(here, got[h * width:(h + 1) * width], 0.0)
                for h in range(tw // 128):
                    px[t * (tw // 128) + h, which - 1] = vec[:, h * 128:(h + 1) * 128]

    du_s, dz_s, di_s = sems(1), sems(1), sems(1)
    ones = jnp.ones((8, iblk), BF16)
    di_acc = jnp.zeros((8, iblk), jnp.int32)
    for j in range(chunks):
        loads[j].wait()
        if j + AHEAD < chunks:
            loads[j + AHEAD].start()
        blk = mask_buf[j]
        di_acc = di_acc + jnp.sum(blk.reshape(ublk // 8, 8, iblk), axis=0)
        blk = blk.astype(F32).astype(BF16)
        adj[j] = blk
        du_own[pl.ds(j, 1), :] = mm(ones, blk, NT)[:1]
    di_own[...] = di_acc.astype(F32)
    for one in smalls:
        one.wait()
    pl.semaphore_wait(barrier, 2 * len(sides) + len(ring))
    for k in sides:
        push(du_s, du_own, du_y.at[k - 1], y_dev(k))
    for k in far_ring:
        push(di_s, di_own, di_got.at[k - 1], r_dev(k))
    user_gather_start(0)
    utot[pl.ds(0, half)] = ua[0, y, z].astype(F32)
    utot[pl.ds(half, half)] = ub[0, z, y].astype(F32)
    for k in far_ring:
        copy(i_nat.at[r], i_nat.at[r], ig[0], r_dev(k), 3).start()
    arrive(du_s, du_y)
    du_ysum[...] = du_own[...] + du_y[0] + du_y[1] + du_y[2]
    for k in sides:
        push(dz_s, du_ysum, du_z.at[k - 1], z_dev(k))
    arrive(ig[0], i_nat.at[pl.ds(0, rows - 1)])
    item0 = mm(eye, i_nat[...].reshape(iblk, emb), NT)
    i_pan[0] = item0.reshape(i_pan.shape[1:])
    itot[...] = i_pan[0, r]
    item0 = item0.astype(BF16)
    user_gather_fwd(0)
    arrive(di_s, di_got)
    deg_i = di_own[...]
    for k in ring:
        deg_i = deg_i + di_got[k - 1]
    deg_i = jnp.sum(deg_i, axis=0, keepdims=True)
    scale_i = lax.rsqrt(jnp.maximum(deg_i, 1.0))
    arrive(dz_s, du_z)
    deg_u = du_ysum[...] + du_z[0] + du_z[1] + du_z[2]
    du_inv[...] = lax.rsqrt(jnp.maximum(deg_u, 1.0))

    def build(j):
        scale_u = jnp.broadcast_to(du_inv[pl.ds(j, 1), :], (8, ublk)).T[:, :1]
        blk = adj[j] * (scale_u * scale_i).astype(BF16)
        adj[j] = blk
        return blk

    s_u, s_i, s_m, s_l = sems(1), sems(1), sems(1), sems(1)
    user_product(0, item0, 0, build)
    user_sum_send(0, 0)
    user_product(0, item0, 1, build)
    user_sum_send(0, 1)
    user_product(0, item0, 2, build)
    user_sum_send(0, 2)
    user_product(0, item0, 3, build)
    user_sum_send(0, 3)
    user_product(0, item0, 4, build)
    user_gather_end(0)
    item_product(0)
    pick_rows(0)
    mine = item_sum(0)
    item_gather(1, mine)
    pick_rows(1)
    user_sum_1(0)
    panel1 = item_panel(1)
    user_product(1, panel1, 0)
    user_sum_send(1, 0)
    user_product(1, panel1, 1)
    user_sum_send(1, 1)
    user_product(1, panel1, 2)
    user_product(1, panel1, 3)
    user_product(1, panel1, 4)
    user_keep(1, *user_sum_2(0))
    user_gather_start(1)
    user_sum_send(1, 2)
    pick_rows(2)
    user_gather_fwd(1)
    user_sum_send(1, 3)
    pick_rows(3)
    pick_rows(4)
    pick_rows(5)
    user_sum_1(1)
    user_gather_end(1)
    item_product(1)
    item_hits()
    pick_users(0)
    pick_users(1)
    user_keep(2, *user_sum_2(1))
    user_gather_start(2)
    mine = item_sum(1)
    item_gather(2, mine)
    user_gather_fwd(2)
    pick_rows(6)
    pick_rows(7)
    panel2 = item_panel(2)
    pick_product(panel2)
    user_gather_end(2)
    item_product(2)
    pick_users(2)
    sum_1(pick_bufs)
    item_sum(2)
    out_slice = (itot[...] / (LAYERS + 1)).astype(BF16).astype(F32)
    pick_items(out_slice)
    for k in far_plane:
        push(s_i, px.at[plus(c, k, chunks)], pxr.at[k - 1], c_dev(k))
    vec_a, vec_b = sum_2(pick_bufs)
    vec_a = ((upick[pl.ds(0, half)] + vec_a.astype(F32)) / (LAYERS + 1)).astype(BF16).astype(F32)
    vec_b = ((upick[pl.ds(half, half)] + vec_b.astype(F32)) / (LAYERS + 1)).astype(BF16).astype(F32)
    vx[...] = jnp.concatenate([vec_a, vec_b], axis=0).reshape(vx.shape)
    for k in far_ring:
        push(s_u, vx.at[plus(r, k, rows)], vxr.at[k - 1], r_dev(k))
    user_product(2, panel2, 0)
    user_sum_send(2, 0)
    user_product(2, panel2, 1)
    user_sum_send(2, 1)
    user_product(2, panel2, 2)
    user_sum_send(2, 2)
    user_product(2, panel2, 3)
    user_sum_send(2, 3)
    user_product(2, panel2, 4)
    item_gather(3, out_slice)
    arrive(s_u, vxr)
    vec_u = vx[r]
    for k in ring:
        vec_u = vec_u + vxr[k - 1]
    arrive(s_i, pxr)
    vec_p, vec_n = px[c, 0], px[c, 1]
    for k in plane:
        vec_p = vec_p + pxr[k - 1, 0]
        vec_n = vec_n + pxr[k - 1, 1]
    part = jnp.sum(vec_u * vec_p, axis=0, keepdims=True) - jnp.sum(vec_u * vec_n, axis=0, keepdims=True)
    tiny[chunks + r] = part
    for k in far_ring:
        push(s_m, tiny.at[chunks + r], tiny.at[chunks + r], r_dev(k))
    arrive(s_m, tiny.at[pl.ds(chunks, rows - 1)])
    neg_x = -tiny[chunks]
    for k in range(1, rows):
        neg_x = neg_x - tiny[chunks + k]
    tiny[c] = jnp.maximum(neg_x, 0.0) + jnp.log1p(jnp.exp(-jnp.abs(neg_x)))
    for k in far_plane:
        push(s_l, tiny.at[c], tiny.at[c], c_dev(k))
    user_sum_1(2)
    user_sum_2(2)
    ou_ref[...] = (utot[...] / (LAYERS + 1)).astype(BF16)
    out_it = item_panel(3)
    oi_nat[...] = mm(out_it, eye, TN).reshape(oi_nat.shape)
    oi_ref[...] = oi_nat[r].astype(BF16)
    arrive(s_l, tiny.at[pl.ds(0, chunks - 1)])
    for k in range(chunks):
        loss_ref[pl.ds(k, 1), :] = tiny[k]

    span = mask_buf.reshape(chunks * ublk, iblk)
    ends = (
        span.at[pl.ds(0, sum(sent[0]) // (4 * iblk))],
        span.at[pl.ds(0, sum(sent[1]) // 512), pl.ds(0, 128)],
        tiny.at[pl.ds(0, sum(sent[2]) // 512)],
        i_nat.at[pl.ds(0, rows - 1)],
    )
    for kind, whole in enumerate(ends):
        copy(whole, whole, 0, {"row": r}, kind).wait_send()
    assert count[0] == recv_sem.shape[0]
    assert all(size % 512 == 0 for size in sent[2])


def emit(ou_in, oi_in, loss_in, ou_ref, oi_ref, loss_ref):
    ou_ref[...] = ou_in[...]
    oi_ref[...] = oi_in[...]
    loss_ref[...] = loss_in[...]


def solution(mesh):
    rows = mesh.shape["row"]
    cols = mesh.shape["col"]

    def device_body(mask_blk, user_shard, item_shard, triples):
        ublk, emb = user_shard.shape
        isub = item_shard.shape[0]
        iblk = mask_blk.shape[1]
        batch = triples.shape[0]
        half = emb // 2
        width = emb // rows
        tw = 256
        tiles = batch // tw
        n_sem = 20 + 20 + 2 * LAYERS + 1 + 3 + 4
        vmem = pltpu.VMEM
        out_user, out_item, loss = pl.pallas_call(
            functools.partial(kernel, rows),
            name="lightgcn",
            out_shape=(
                jax.ShapeDtypeStruct((emb, ublk), BF16),
                jax.ShapeDtypeStruct((isub, emb), BF16),
                jax.ShapeDtypeStruct((batch // 128, 128), F32),
            ),
            in_specs=[pl.BlockSpec(memory_space=pl.ANY)] * 4,
            out_specs=tuple([pl.BlockSpec(memory_space=vmem)] * 3),
            scratch_shapes=[
                vmem((cols, ublk, iblk), jnp.int32),
                vmem((cols, ublk, iblk), BF16),
                vmem((LAYERS, SIDE, SIDE, half, ublk), BF16),
                vmem((LAYERS, SIDE, SIDE, half, ublk), BF16),
                vmem((LAYERS, SIDE, SIDE, half, ublk), F32),
                vmem((LAYERS, SIDE, SIDE, half, ublk), F32),
                vmem((LAYERS, 3, SIDE, half, ublk), F32),
                vmem((LAYERS, 3, SIDE, half, ublk), F32),
                vmem((LAYERS, SIDE, half, ublk), F32),
                vmem((LAYERS, SIDE, half, ublk), F32),
                vmem((LAYERS, 3, half, ublk), F32),
                vmem((LAYERS, 3, half, ublk), F32),
                vmem((emb, ublk), F32),
                vmem((rows, isub, emb), BF16),
                vmem((LAYERS + 1, rows, width, iblk), F32),
                vmem((LAYERS, rows, width, iblk), F32),
                vmem((LAYERS, rows - 1, width, iblk), F32),
                vmem((width, iblk), F32),
                vmem((cols, ublk), F32),
                vmem((3, cols, ublk), F32),
                vmem((cols, ublk), F32),
                vmem((3, cols, ublk), F32),
                vmem((cols, ublk), F32),
                vmem((8, iblk), F32),
                vmem((rows - 1, 8, iblk), F32),
                vmem((rows, isub, emb), F32),
                vmem((tw, cols * ublk), BF16),
                vmem((tiles, tw, iblk), BF16),
                vmem((2, tiles, ublk, tw), BF16),
                vmem((SIDE, SIDE, half, 128), F32),
                vmem((SIDE, SIDE, half, 128), F32),
                vmem((3, SIDE, half, 128), F32),
                vmem((3, SIDE, half, 128), F32),
                vmem((SIDE, half, 128), F32),
                vmem((SIDE, half, 128), F32),
                vmem((3, half, 128), F32),
                vmem((3, half, 128), F32),
                vmem((emb, 128), F32),
                vmem((rows, width, 128), F32),
                vmem((rows - 1, width, 128), F32),
                vmem((cols, 2, width, 128), F32),
                vmem((cols - 1, 2, width, 128), F32),
                vmem((cols + rows, 1, 128), F32),
                vmem((3, batch), jnp.int32),
                pltpu.SemaphoreType.DMA((AHEAD + 4,)),
                pltpu.SemaphoreType.DMA((4,)),
                pltpu.SemaphoreType.DMA((n_sem,)),
            ],
            compiler_params=pltpu.CompilerParams(collective_id=0, has_side_effects=True),
        )(mask_blk, user_shard.T, item_shard, triples.T)
        out_user, out_item, loss = pl.pallas_call(
            emit,
            name="emit",
            out_shape=(
                jax.ShapeDtypeStruct((emb, ublk), BF16),
                jax.ShapeDtypeStruct((isub, emb), BF16),
                jax.ShapeDtypeStruct((batch // 128, 128), F32),
            ),
        )(out_user, out_item, loss)
        return out_user.T, out_item, loss.reshape(batch)

    return jax.shard_map(
        device_body,
        mesh=mesh,
        in_specs=(P("row", "col"), P(("row", "col"), None), P(("col", "row"), None), P()),
        out_specs=(P(("row", "col"), None), P(("col", "row"), None), P()),
        check_vma=False,
    )
```
